32 devices in a mesh: graph: 16 (over z, y, x), mp: 2 (over core).
Axes of the slice: x: 2, y: 2, z: 4, core: 2. Of those that a mesh axis runs over, the one named last changes fastest.
Arguments:
- tokens: bfloat16 [32, 256, 768], P('graph'), may hold values from -30 to 30
- token_counts: int32 [16, 2], P('graph'), may hold values from 1 to 256, 384 in all within a row
- w_qkv: bfloat16 [768, 3, 768], P(None, None, 'mp'), may hold values from -0.21875 to 0.21875
- w_out: bfloat16 [768, 768], P('mp'), may hold values from -0.21875 to 0.21875
- w_up: bfloat16 [768, 3072], P(None, 'mp'), may hold values from -0.21875 to 0.21875
- w_down: bfloat16 [3072, 768], P('mp'), may hold values from -0.109375 to 0.109375
- ln_gains: float32 [2, 768], replicated, may hold values from 0.1 to 1.9
- cache: bfloat16 [8192, 768], P('graph', 'mp'), may hold values from -6 to 6
- node_text: int32 [8192], P('graph'), may hold values from -1 to 31, as said below
- adj_tiles: int32 [64, 5], P('graph'), may hold values from -1 to 63, as said below
- adj_values: bfloat16 [64, 5, 128, 128], P('graph'), may hold values from -0.1875 to 0.1875
- w_gnn: bfloat16 [768, 768], P('mp'), may hold values from -0.21875 to 0.21875
- out_grad: bfloat16 [8192, 768], P('graph', 'mp'), may hold values from -6 to 6
Outputs:
- node_out: bfloat16 [8192, 768], P('graph', 'mp')
- w_grad: float32 [768, 768], P('mp', 'graph')
- text_grad: float32 [32, 768], P('graph', 'mp')
- node_grad: bfloat16 [8192, 768], P('graph', 'mp')
The draws below stay inside these ranges and needn't reach their ends.
Inputs may be any that keep to these rules, and one draw needn't show every extreme that they name: `token_counts`: the counts of one row sum to 384. `node_text`: every text number below 32 is held by exactly one node; every other node holds -1. `adj_tiles`: an entry names a source tile by its global number (tile j of block q is q * 4 + j) or is -1. The entries of a row tile are distinct and include the row tile itself and one other tile of its own block. A block lists at most one tile of any other block, in one entry only; a block lists tiles of at most 12 other blocks, and some block lists tiles of 12 other blocks; a tile is listed by at most 4 other blocks.
All inputs are finite; a program needn't handle non-finite values.
Results may differ from the reference program's by a relative error of at most 0.011.
Values may be sent and summed in bfloat16 or wider, within the bound.
No kernel may reach another device: no remote copies, remote signals or barrier semaphores. Data moves between devices by JAX's collectives and lax.ppermute only.
A program may use at most 192 MiB of HBM per device.

```python
import math
import jax
import jax.numpy as jnp
import numpy as np
from jax import lax

D = 768
HEADS = 12
HEAD = 64
FF = 3072
SEQ = 256
TEXTS_PER_INDEX = 2
TILE = 128
TPD = 4
PEERS_MAX = 12
K = 5
SHARDS = 16
TEXTS = 32
NODES = 8192
TILES = 64
N_MP = 2


def draw_tokens(key, part):
    key_base = jax.random.fold_in(jax.random.fold_in(key, 3), 0)
    base = jnp.clip(jax.random.normal(key_base, (TEXTS, SEQ, D), jnp.float32), -4.0, 4.0)
    return base.astype(jnp.bfloat16)


def draw_node_text(key, part):
    shuffled = jax.random.permutation(jax.random.fold_in(key, 7), NODES)
    holders = jnp.full((NODES,), -1, jnp.int32)
    return holders.at[shuffled[:TEXTS]].set(jnp.arange(TEXTS, dtype=jnp.int32))


def shuffled_rows(subkey):
    return jax.random.permutation(subkey, SHARDS)


def graph_tables(key):
    base = jax.random.fold_in(key, 1234)
    key_want, key_busy, key_order, key_reader, key_shift, key_local = jax.random.split(base, 6)
    devices = jnp.arange(SHARDS, dtype=jnp.int32)
    wanted = jax.random.randint(key_want, (SHARDS,), max(2, PEERS_MAX // 2), PEERS_MAX + 1)
    picked_four = jax.random.permutation(key_busy, SHARDS)[:4]
    busiest = picked_four[:2]
    popular = picked_four[2:]
    wanted = wanted.at[busiest].set(PEERS_MAX)
    is_popular = jnp.any(devices[:, None] == popular[None, :], axis=1)
    order_of = jax.vmap(shuffled_rows)(jax.random.split(key_order, SHARDS))
    first_rank = jnp.argsort(order_of, axis=1, stable=True).astype(jnp.int32)
    composite = first_rank + SHARDS * (1 - is_popular.astype(jnp.int32))[None, :]
    rank_of = jnp.argsort(jnp.argsort(composite, axis=1, stable=True), axis=1, stable=True).astype(jnp.int32)
    self_rank = jnp.sum(jnp.where(devices[None, :] == devices[:, None], rank_of, 0), axis=1)
    peer_rank = rank_of - (rank_of > self_rank[:, None]).astype(jnp.int32)
    not_self = devices[None, :] != devices[:, None]
    needed = not_self & (peer_rank < wanted[:, None])
    reader_order = jax.vmap(shuffled_rows)(jax.random.split(key_reader, SHARDS))
    reader_rank = jnp.argsort(reader_order, axis=1, stable=True).astype(jnp.int32).T
    earlier = needed[:, None, :] & (reader_rank[:, None, :] < reader_rank[None, :, :])
    position = jnp.sum(earlier.astype(jnp.int32), axis=0)
    shift_of = jax.random.randint(key_shift, (SHARDS,), 0, TPD)
    chosen = (position + shift_of[None, :]) % TPD
    row_slot = jnp.where(needed, peer_rank % TPD, 0)
    col_slot = jnp.where(needed, 2 + peer_rank // TPD, K)
    tile_id = devices[None, :] * TPD + chosen
    table = jnp.full((SHARDS, TPD, K + 1), -1, jnp.int32)
    owners = jnp.broadcast_to(devices[:, None], (SHARDS, SHARDS))
    table = table.at[owners, row_slot, col_slot].set(jnp.where(needed, tile_id, -1).astype(jnp.int32))
    local_rows = jnp.arange(TPD, dtype=jnp.int32)
    local_shift = jax.random.randint(key_local, (SHARDS,), 0, TPD - 1)
    table = table.at[:, :, 0].set(devices[:, None] * TPD + local_rows[None, :])
    table = table.at[:, :, 1].set(devices[:, None] * TPD + (local_rows[None, :] + 1 + local_shift[:, None]) % TPD)
    return table[:, :, :K].reshape(TILES, K)


def draw_adj_tiles(key, part):
    return graph_tables(key)


def spiked(drawn, key, source, target, blocks, factor):
    owner, partner = [(jnp.arange(drawn.shape[dim]) // (drawn.shape[dim] // blocks)).reshape([-1 if axis == dim else 1 for axis in range(drawn.ndim)]) for dim in (source, target)]
    chosen = jax.random.permutation(key, blocks)[partner]
    strong = (owner == chosen) | (owner == (partner + blocks // 2) % blocks)
    return jnp.where(strong, factor * drawn, drawn)


def levels(key, extent, shards, smallest, high):
    level = 1.0
    for dim, shards_of in shards:
        heights = jax.random.uniform(jax.random.fold_in(jax.random.fold_in(key, 6), dim), (shards_of,), jnp.float32, smallest / len(shards), high / len(shards))
        level = level * jnp.repeat(jnp.exp(heights), extent[dim] // shards_of).reshape((-1,) + (1,) * (len(extent) - 1 - dim))
    return level


def split_up(count, total, most, lean):
    weights = [(1 << 20) // math.isqrt(standing ** lean) + 1 for standing in range(2, count + 1)]
    spare, holding = total - most - (count - 1), [1] * (count - 1)
    while spare > 0:
        free = [i for i in range(count - 1) if holding[i] < most]
        whole, budget = sum([weights[i] for i in free]), spare
        for i in free:
            addition = min(most - holding[i], max(1, budget * weights[i] // whole), spare)
            holding[i] = holding[i] + addition
            spare = spare - addition
    return np.array([most] + holding)


def ragged(own_key, count, total, limit, skew):
    if count == 2:
        one = jax.random.randint(own_key, (), max(1, total - limit), min(limit, total - 1) + 1)
        return jnp.stack([one, total - one])
    sizes = jnp.asarray(split_up(count, total, limit, skew), jnp.int32)
    couples = (count - 1) // 2
    source_of, taker = sizes[1:1 + 2 * couples:2], sizes[2:2 + 2 * couples:2]
    margin = jnp.minimum(source_of - 1, limit - taker)
    shifted = jax.random.randint(jax.random.fold_in(own_key, 1), (couples,), 0, 1 << 20) % (margin + 1)
    sizes = sizes.at[1:1 + 2 * couples:2].set(source_of - shifted).at[2:2 + 2 * couples:2].set(taker + shifted)
    return sizes[jax.random.permutation(jax.random.fold_in(own_key, 2), count)]


def normal_values(own_key, extent, spread, most, pieces=(), kind=jnp.bfloat16):
    drawn = spread * jax.random.normal(own_key, extent, jnp.float32)
    if pieces:
        drawn = drawn * levels(own_key, extent, pieces, -0.22, 0.18)
    return jnp.clip(drawn, -most, most).astype(kind)


def heavy_noise(stream_key, extent, spread, reach, cuts, heavy, kind=jnp.bfloat16):
    array = spread * jax.random.normal(stream_key, extent, jnp.float32)
    if cuts:
        array = array * levels(stream_key, extent, cuts, -0.22, 0.18)
    return jnp.clip(spiked(array, jax.random.fold_in(stream_key, 3), *heavy), -reach, reach).astype(kind)


def setup_inputs(seed: int = 0) -> dict:
    arg_keys = jax.random.split(jax.random.key(seed), 14)
    return {
        "tokens": draw_tokens(jax.random.fold_in(arg_keys[13], 71), 0),
        "token_counts": jax.vmap(lambda own: ragged(own, TEXTS_PER_INDEX, SEQ + (TEXTS_PER_INDEX - 1) * SEQ // 2, SEQ, 2))(jax.random.split(arg_keys[1], SHARDS)).reshape((SHARDS, TEXTS_PER_INDEX)).astype(jnp.int32),
        "w_qkv": normal_values(arg_keys[2], (D, 3, D), D ** -0.5, 0.21875, ((2, 2),)),
        "w_out": normal_values(arg_keys[3], (D, D), D ** -0.5, 0.21875, ((0, 2),)),
        "w_up": normal_values(arg_keys[4], (D, FF), D ** -0.5, 0.21875, ((1, 2),)),
        "w_down": normal_values(arg_keys[5], (FF, D), FF ** -0.5, 0.109375, ((0, 2),)),
        "ln_gains": jnp.clip(1.0 + 0.18 * jax.random.normal(arg_keys[6], (2, D), jnp.float32), 0.1, 1.9),
        "cache": normal_values(arg_keys[7], (NODES, D), 1.0, 6.0, ((0, 16), (1, 2))),
        "node_text": draw_node_text(jax.random.fold_in(arg_keys[13], 71), 0),
        "adj_tiles": draw_adj_tiles(jax.random.fold_in(arg_keys[13], 71), 0),
        "adj_values": normal_values(arg_keys[10], (TILES, K, TILE, TILE), (TILE * 8) ** -0.5, 0.1875, ((0, 16),)),
        "w_gnn": normal_values(arg_keys[11], (D, D), D ** -0.5, 0.21875, ((0, 2),)),
        "out_grad": heavy_noise(arg_keys[12], (NODES, D), 1.0, 6.0, ((0, 16), (1, 2)), (0, 1, 16, 2.0)),
    }


norm_eps = 1e-05
masked_score = -1e+30

def layer_norm(values, scale_row):
    average = lax.optimization_barrier(jnp.mean(values, axis=-1, keepdims=True))
    centred = values - average
    variance = lax.optimization_barrier(jnp.mean(centred * centred, axis=-1, keepdims=True))
    return centred * lax.rsqrt(variance + norm_eps) * scale_row

def softmax_rows(scores):
    row_max = lax.optimization_barrier(jnp.max(scores, axis=-1, keepdims=True))
    powers = jnp.exp(scores - row_max)
    return powers / lax.optimization_barrier(jnp.sum(powers, axis=-1, keepdims=True))

def round_keep(values):
    return lax.optimization_barrier(values.astype(jnp.bfloat16)).astype(jnp.float32)

def encode_block(tokens, counts, w_qkv, w_out, w_up, w_down, ln_gains):
    text_count = tokens.shape[0]
    flat_tokens = tokens.reshape(text_count * SEQ, D)
    projected = jnp.dot(flat_tokens, w_qkv.reshape(D, 3 * D), preferred_element_type=jnp.float32)
    projected = round_keep(projected).reshape(text_count, SEQ, 3, HEADS, HEAD)
    scores = jnp.einsum('bqhe,bkhe->bhqk', projected[:, :, 0], projected[:, :, 1], precision=lax.Precision.HIGHEST) / math.sqrt(HEAD)
    valid = jnp.arange(SEQ, dtype=jnp.int32)[None, :] < counts[:, None]
    scores = jnp.where(valid[:, None, None, :], scores, masked_score)
    attn_weights = round_keep(softmax_rows(scores))
    context = jnp.einsum('bhqk,bkhe->bqhe', attn_weights, projected[:, :, 2], precision=lax.Precision.HIGHEST)
    context = context.astype(jnp.bfloat16).reshape(text_count * SEQ, D)
    half_width = D // N_MP
    ff_width = FF // N_MP
    attention_layer = jnp.zeros((text_count * SEQ, D), jnp.float32)
    for core_index in range(N_MP):
        start_col = core_index * half_width
        part_out = jnp.dot(context[:, start_col:start_col + half_width], w_out[start_col:start_col + half_width], preferred_element_type=jnp.float32)
        attention_layer = attention_layer + round_keep(part_out)
    first_norm = layer_norm(flat_tokens.astype(jnp.float32) + attention_layer, ln_gains[0]).astype(jnp.bfloat16)
    inner = jax.nn.gelu(jnp.dot(first_norm, w_up, preferred_element_type=jnp.float32)).astype(jnp.bfloat16)
    mlp_out = jnp.zeros((text_count * SEQ, D), jnp.float32)
    for core_index in range(N_MP):
        start_col = core_index * ff_width
        part_out = jnp.dot(inner[:, start_col:start_col + ff_width], w_down[start_col:start_col + ff_width], preferred_element_type=jnp.float32)
        mlp_out = mlp_out + round_keep(part_out)
    second_norm = layer_norm(first_norm.astype(jnp.float32) + mlp_out, ln_gains[1])
    second_norm = second_norm.reshape(text_count, SEQ, D)
    pooled = lax.optimization_barrier(jnp.sum(jnp.where(valid[:, :, None], second_norm, 0.0), axis=1)) / counts[:, None].astype(jnp.float32)
    return pooled.astype(jnp.bfloat16)

def reference(tokens, token_counts, w_qkv, w_out, w_up, w_down, ln_gains, cache, node_text, adj_tiles, adj_values, w_gnn, out_grad):
    blocks = tokens.reshape(TEXTS // TEXTS_PER_INDEX, TEXTS_PER_INDEX, SEQ, D)
    count_blocks = token_counts.reshape(TEXTS // TEXTS_PER_INDEX, TEXTS_PER_INDEX)
    pooled = lax.map(lambda inputs: encode_block(inputs[0], inputs[1], w_qkv, w_out, w_up, w_down, ln_gains), (blocks, count_blocks))
    pooled = pooled.reshape(TEXTS, D)
    fresh_mask = node_text >= 0
    picked = jnp.take(pooled, jnp.maximum(node_text, 0), axis=0)
    features = jnp.where(fresh_mask[:, None], picked, cache)
    feature_tiles = features.reshape(TILES, TILE, D)

    def gather_one(inputs):
        tile_ids, tile_values = inputs
        is_live = tile_ids >= 0
        source_nodes = jnp.take(feature_tiles, jnp.maximum(tile_ids, 0), axis=0).astype(jnp.float32)
        masked = jnp.where(is_live[:, None, None], tile_values, 0).astype(jnp.float32)
        summed = jnp.einsum('kab,kbd->ad', masked, source_nodes, precision=lax.Precision.HIGHEST)
        return summed.astype(jnp.bfloat16)
    neighbor_aggregate = lax.map(gather_one, (adj_tiles, adj_values)).reshape(NODES, D)
    hidden = jnp.dot(neighbor_aggregate, w_gnn, preferred_element_type=jnp.float32)
    activated, pull = jax.vjp(jax.nn.gelu, hidden)
    node_out = (features.astype(jnp.float32) + activated).astype(jnp.bfloat16)
    hidden_grad = pull(out_grad.astype(jnp.float32))[0].astype(jnp.bfloat16)
    w_grad = jnp.dot(neighbor_aggregate.T, hidden_grad, preferred_element_type=jnp.float32)
    agg_grad = jnp.dot(hidden_grad, w_gnn.T, preferred_element_type=jnp.float32).astype(jnp.bfloat16)
    gradient_tile_list = agg_grad.reshape(TILES, TILE, D)

    def spread_one(running, inputs):
        row_tile, tile_ids, tile_values = inputs
        is_live = tile_ids >= 0
        masked = jnp.where(is_live[:, None, None], tile_values, 0).astype(jnp.float32)
        neighbor_contribution = jnp.einsum('kab,ad->kbd', masked, gradient_tile_list[row_tile].astype(jnp.float32), precision=lax.Precision.HIGHEST)
        is_remote = tile_ids // TPD != row_tile // TPD
        neighbor_contribution = jnp.where(is_remote[:, None, None], round_keep(neighbor_contribution), neighbor_contribution)
        return (running.at[jnp.maximum(tile_ids, 0)].add(neighbor_contribution), None)
    running, _ = lax.scan(spread_one, jnp.zeros((TILES, TILE, D), jnp.float32), (jnp.arange(TILES, dtype=jnp.int32), adj_tiles, adj_values))
    node_grad_full = out_grad.astype(jnp.float32) + running.reshape(NODES, D)
    text_slot = jnp.where(fresh_mask, node_text, TEXTS).astype(jnp.int32)
    text_grad = jnp.zeros((TEXTS + 1, D), jnp.float32).at[text_slot].add(node_grad_full)[:TEXTS]
    return (node_out, w_grad, text_grad, node_grad_full.astype(jnp.bfloat16))
```

```python
import functools

import jax
import jax.numpy as jnp
from jax import lax
from jax.experimental import pallas as pl
from jax.experimental.pallas import tpu as pltpu
from jax.sharding import PartitionSpec as P

HEAD = 64
LANES = 128
ROWS = 16
NORM_EPS = 1e-05
MASKED = -1e30
NO_NODE = -(1 << 20)
ROOT = 0.7978845608028654
CUBE = 0.044715

VMEM = pl.BlockSpec(memory_space=pltpu.VMEM)
SMEM = pl.BlockSpec(memory_space=pltpu.SMEM)


def up_to(value, unit):
    return (value + unit - 1) // unit * unit


def call(body, outs, ins, specs, flops, scratch=(), name=None):
    moved = sum(a.size * a.dtype.itemsize for a in ins) + sum(
        o.size * o.dtype.itemsize for o in outs
    )
    many = len(outs) > 1
    return pl.pallas_call(
        body,
        out_shape=tuple(outs) if many else outs[0],
        in_specs=list(specs),
        out_specs=tuple([VMEM] * len(outs)) if many else VMEM,
        scratch_shapes=list(scratch),
        cost_estimate=pl.CostEstimate(flops=flops, bytes_accessed=moved, transcendentals=0),
        name=name,
    )(*ins)


def shape(dims, dtype=jnp.bfloat16):
    return jax.ShapeDtypeStruct(tuple(dims), dtype)


def mm(a, b, dims=(1, 0)):
    return lax.dot_general(
        a, b, (((dims[0],), (dims[1],)), ((), ())), preferred_element_type=jnp.float32
    )


def tile_of(tile_id, tiles_here):
    safe = jnp.maximum(tile_id, 0)
    owner = lax.div(safe, jnp.int32(tiles_here))
    return safe, owner, safe - owner * tiles_here


def index_body(texts_here, ids_ref, self_ref, text_ref, out_ref):
    tiles_here, entries = ids_ref.shape
    shards, lanes = out_ref.shape
    width = lanes - LANES
    texts = texts_here * shards
    me = self_ref[0]
    row = lax.broadcasted_iota(jnp.int32, (shards, LANES), 0)
    wanted = jnp.full((shards, LANES), -1, jnp.int32)
    for r in range(tiles_here):
        for k in range(entries):
            tile_id = ids_ref[r, k]
            _, owner, place = tile_of(tile_id, tiles_here)
            target = jnp.where((tile_id >= 0) & (owner != me), owner, -1)
            wanted = jnp.where(row == target, place, wanted)
    out_ref[:, width:] = wanted
    tile_rows = text_ref.shape[1]
    lane = lax.broadcasted_iota(jnp.int32, (LANES, tile_rows), 1)
    sub = lax.broadcasted_iota(jnp.int32, (LANES, LANES), 0)
    diagonal = sub == lax.broadcasted_iota(jnp.int32, (LANES, LANES), 1)
    for c in range(width // LANES):
        slot = c * LANES + lax.broadcasted_iota(jnp.int32, (LANES, 1), 0)
        part = lax.div(slot, jnp.int32(shards))
        text = jnp.where(slot < texts, (slot - part * shards) * texts_here + part, -5)
        best = jnp.full((LANES, tile_rows), NO_NODE, jnp.int32)
        for j in range(tiles_here):
            node = (me * tiles_here + j) * tile_rows + lane
            best = jnp.where(text_ref[j : j + 1, :] == text, node, best)
        column = jnp.max(best.astype(jnp.float32), axis=1, keepdims=True)
        line = jnp.max(jnp.where(diagonal, column, float(NO_NODE)), axis=0, keepdims=True)
        out_ref[:, c * LANES : (c + 1) * LANES] = jnp.broadcast_to(
            line, (shards, LANES)
        ).astype(jnp.int32)


def pack_body(asked_ref, cache_ref, out_ref):
    def one(q, carry):
        out_ref[q] = cache_ref[jnp.maximum(asked_ref[q], 0)]
        return carry

    lax.fori_loop(0, out_ref.shape[0], one, 0)


def mask_body(ids_ref, self_ref, got_ref, adj_ref, cache_ref, kept_ref, pick_ref, own_ref, base_ref):
    tiles_here, entries, tile_rows, _ = adj_ref.shape
    width = got_ref.shape[1] - LANES
    me = self_ref[0]
    table = jnp.max(got_ref[:, :width].astype(jnp.float32), axis=0, keepdims=True)
    place = lax.broadcasted_iota(jnp.int32, (tile_rows, width), 0).astype(jnp.float32)
    ones = jnp.ones((ROWS, width), jnp.bfloat16)

    def holds(tile_id):
        first = (tile_id * tile_rows).astype(jnp.float32)
        return jnp.where(table - first == place, 1.0, 0.0)

    for r in range(tiles_here):

        def one(k, total):
            tile_id = ids_ref[r, k]
            hot = holds(tile_id).astype(jnp.bfloat16)
            values = adj_ref[r, k]
            taken = mm(ones, hot, (1, 1))[0:1, :]
            keep = jnp.where(tile_id >= 0, 1.0, 0.0) * jnp.where(taken > 0.5, 0.0, 1.0)
            kept_ref[r, k] = (values.astype(jnp.float32) * keep).astype(jnp.bfloat16)
            return total + mm(values, hot)

        pick = lax.fori_loop(0, entries, one, jnp.zeros((tile_rows, width), jnp.float32))
        pick_ref[r] = pick.astype(jnp.bfloat16)
        hot = holds(me * tiles_here + r)
        own_ref[r] = hot.astype(jnp.bfloat16)
        fresh = jnp.max(hot, axis=1, keepdims=True)
        base_ref[r] = (cache_ref[r].astype(jnp.float32) * (1.0 - fresh)).astype(jnp.bfloat16)


def norm(values, gain):
    average = jnp.mean(values, axis=-1, keepdims=True)
    centred = values - average
    variance = jnp.mean(centred * centred, axis=-1, keepdims=True)
    return centred * lax.rsqrt(variance + NORM_EPS) * gain


def attend_body(seq, counts_ref, tokens_ref, w_qkv_ref, w_out_ref, out_ref, proj_ref, ctx_ref):
    half = w_out_ref.shape[0]
    texts_here = tokens_ref.shape[0] // seq
    for c in range(3):
        proj_ref[:, c * half : (c + 1) * half] = mm(
            tokens_ref[...], w_qkv_ref[:, c * half : (c + 1) * half]
        ).astype(jnp.bfloat16)
    left = lax.broadcasted_iota(jnp.int32, (seq, LANES), 1) < HEAD
    key_at = lax.broadcasted_iota(jnp.int32, (seq, seq), 1)
    for t in range(texts_here):
        rows = slice(t * seq, (t + 1) * seq)
        live = key_at < counts_ref[0, t]
        for pair in range(half // LANES):
            first = pair * LANES
            query = proj_ref[rows, first : first + LANES].astype(jnp.float32) * (HEAD**-0.5)
            key = proj_ref[rows, half + first : half + first + LANES]
            value = proj_ref[rows, 2 * half + first : 2 * half + first + LANES]
            sides = []
            for side in (left, jnp.logical_not(left)):
                scores = mm(jnp.where(side, query, 0.0).astype(jnp.bfloat16), key, (1, 1))
                scores = jnp.where(live, scores, MASKED)
                powers = jnp.exp(scores - jnp.max(scores, axis=-1, keepdims=True))
                total = jnp.sum(powers, axis=-1, keepdims=True)
                sides.append(mm((powers / total).astype(jnp.bfloat16), value))
            ctx_ref[rows, first : first + LANES] = jnp.where(left, sides[0], sides[1]).astype(
                jnp.bfloat16
            )
    out_ref[...] = mm(ctx_ref[...], w_out_ref[...]).astype(jnp.bfloat16)


def inner_body(tokens_ref, mine_ref, other_ref, up_ref, down_ref, gains_ref, first_ref, out_ref, inner_ref):
    added = mine_ref[...].astype(jnp.float32) + other_ref[...].astype(jnp.float32)
    first = norm(tokens_ref[...].astype(jnp.float32) + added, gains_ref[0:1, :])
    first_ref[...] = first.astype(jnp.bfloat16)
    hidden_units = up_ref.shape[1]
    step = hidden_units // 4
    for c in range(4):
        cols = slice(c * step, (c + 1) * step)
        value = mm(first_ref[...], up_ref[:, cols])
        gate = jnp.tanh(ROOT * (value + CUBE * (value * value * value)))
        inner_ref[:, cols] = (0.5 * value * (1.0 + gate)).astype(jnp.bfloat16)
    out_ref[...] = mm(inner_ref[...], down_ref[...]).astype(jnp.bfloat16)


def pool_body(seq, counts_ref, core_ref, first_ref, mine_ref, other_ref, gains_ref, out_ref, pooled_ref):
    shards, lanes = out_ref.shape
    texts_here = first_ref.shape[0] // seq
    half = lanes // texts_here
    for t in range(texts_here):
        rows = slice(t * seq, (t + 1) * seq)
        added = mine_ref[rows, :].astype(jnp.float32) + other_ref[rows, :].astype(jnp.float32)
        second = norm(first_ref[rows, :].astype(jnp.float32) + added, gains_ref[1:2, :])
        count = counts_ref[0, t]
        live = lax.broadcasted_iota(jnp.int32, (seq, 1), 0) < count
        total = jnp.sum(jnp.where(live, second, 0.0), axis=0, keepdims=True)
        pooled_ref[...] = jnp.broadcast_to(
            total / count.astype(jnp.float32), pooled_ref.shape
        )
        start = pl.multiple_of(core_ref[0] * half, LANES)
        own = pooled_ref[:, pl.ds(start, half)][0:1, :]
        out_ref[:, t * half : (t + 1) * half] = jnp.broadcast_to(own, (shards, half)).astype(
            jnp.bfloat16
        )


def pooled_rows(pooled_ref, half):
    parts = pooled_ref.shape[1] // half
    return jnp.concatenate([pooled_ref[:, i * half : (i + 1) * half] for i in range(parts)], axis=0)


def gather_body(ids_ref, self_ref, kept_ref, pick_ref, pooled_ref, cache_ref, remote_ref, out_ref, source_ref):
    tiles_here, entries, tile_rows, _ = kept_ref.shape
    half = cache_ref.shape[2]
    me = self_ref[0]
    pooled = pooled_rows(pooled_ref, half)
    texts = pooled.shape[0]
    for r in range(tiles_here):

        def fetch(k, carry):
            tile_id = ids_ref[r, k]
            _, owner, place = tile_of(tile_id, tiles_here)
            local = (owner == me) | (tile_id < 0)

            @pl.when(local)
            def _():
                source_ref[k] = cache_ref[place]

            @pl.when(jnp.logical_not(local))
            def _():
                source_ref[k] = remote_ref[owner]

            return carry

        lax.fori_loop(0, entries, fetch, 0)
        total = mm(pick_ref[r][:, :texts], pooled)
        for k in range(entries):
            total = total + mm(kept_ref[r, k], source_ref[k])
        out_ref[r] = total.astype(jnp.bfloat16)


def forward_body(core_ref, mine_ref, other_ref, w_own_ref, w_other_ref, grad_ref, own_ref, base_ref, pooled_ref, node_ref, slope_ref):
    rows, half = mine_ref.shape
    start = pl.multiple_of(core_ref[0] * half, LANES)
    hidden = mm(mine_ref[...], w_own_ref[:, pl.ds(start, half)]) + mm(
        other_ref[...], w_other_ref[...]
    )
    square = hidden * hidden
    gate = jnp.tanh(ROOT * hidden * (1.0 + CUBE * square))
    lifted = 0.5 * (1.0 + gate)
    slope = lifted + 0.5 * hidden * (1.0 - gate * gate) * (ROOT * (1.0 + 3.0 * CUBE * square))
    slope_ref[...] = (grad_ref[...].astype(jnp.float32) * slope).astype(jnp.bfloat16)
    pooled = pooled_rows(pooled_ref, half)
    fresh = mm(own_ref[:, : pooled.shape[0]], pooled)
    node_ref[...] = (base_ref[...].astype(jnp.float32) + fresh + hidden * lifted).astype(
        jnp.bfloat16
    )


def backward_body(
    per, texts_here, ids_ref, self_ref, core_ref, mine_ref, other_ref, agg_ref, w_own_ref, adj_ref,
    pick_ref, own_ref, grad_ref, send_ref, local_ref, down_ref, w_ref, text_ref
):
    tiles_here, entries, tile_rows, _ = adj_ref.shape
    half = agg_ref.shape[1]
    shards = send_ref.shape[0]
    me = self_ref[0]
    core = core_ref[0]
    own = pl.multiple_of(core * half, LANES)
    far = pl.multiple_of((1 - core) * half, LANES)
    down = mm(mine_ref[...], w_own_ref[:, pl.ds(own, half)], (1, 1)) + mm(
        other_ref[...], w_own_ref[:, pl.ds(far, half)], (1, 1)
    )
    down_ref[...] = down.astype(jnp.bfloat16)
    local_ref[...] = grad_ref[...].astype(jnp.float32)
    for r in range(tiles_here):
        rows = slice(r * tile_rows, (r + 1) * tile_rows)

        def one(k, carry):
            tile_id = ids_ref[r, k]
            _, owner, place = tile_of(tile_id, tiles_here)

            @pl.when((tile_id >= 0) & (owner == me))
            def _():
                local_ref[place] += mm(adj_ref[r, k], down_ref[rows, :], (0, 0))

            @pl.when((tile_id >= 0) & (owner != me))
            def _():
                send_ref[owner, :tile_rows, :] = mm(
                    adj_ref[r, k], down_ref[rows, :], (0, 0)
                ).astype(jnp.bfloat16)

            return carry

        lax.fori_loop(0, entries, one, 0)
    text_ref[...] = mm(pick_ref[...], down_ref[...], (0, 0)) + mm(
        own_ref[...], grad_ref[...].reshape(tiles_here * tile_rows, half), (0, 0)
    )
    columns = 2 * half
    w_ref[pl.ds(own, half), :] = mm(mine_ref[...], agg_ref[...], (0, 0))
    w_ref[pl.ds(far, half), :] = mm(other_ref[...], agg_ref[...], (0, 0))
    w_ref[columns:, :] = jnp.zeros((w_ref.shape[0] - columns, half), jnp.float32)
    deep = up_to(per, ROWS)
    row = lax.broadcasted_iota(jnp.int32, (ROWS, half), 0)
    for q in range(shards):
        send_ref[q, tile_rows : tile_rows + deep, :] = w_ref[q * per : q * per + deep, :].astype(
            jnp.bfloat16
        )
        block = jnp.zeros((ROWS, half), jnp.float32)
        for i in range(texts_here):
            line = text_ref[i * shards + q : i * shards + q + 1, :]
            high = line.astype(jnp.bfloat16).astype(jnp.float32)
            block = jnp.where(row == 2 * i, high, block)
            block = jnp.where(row == 2 * i + 1, line - high, block)
        send_ref[q, tile_rows + deep :, :] = block.astype(jnp.bfloat16)


def finish_body(per, texts_here, asked_ref, local_ref, got_ref, node_ref, w_ref, text_ref, sum_ref):
    tiles_here, tile_rows, half = local_ref.shape
    shards = got_ref.shape[0]
    sum_ref[...] = local_ref[...]
    deep = up_to(per, ROWS)

    def one(q, carry):
        w_sum, text_sum = carry
        asked = asked_ref[q]

        @pl.when(asked >= 0)
        def _():
            sum_ref[asked] += got_ref[q, :tile_rows, :].astype(jnp.float32)

        w_sum = w_sum + got_ref[q, tile_rows : tile_rows + deep, :].astype(jnp.float32)
        text_sum = text_sum + got_ref[q, tile_rows + deep :, :].astype(jnp.float32)
        return w_sum, text_sum

    w_sum, text_sum = lax.fori_loop(
        0,
        shards,
        one,
        (jnp.zeros((deep, half), jnp.float32), jnp.zeros((ROWS, half), jnp.float32)),
    )
    w_ref[...] = w_sum
    node_ref[...] = sum_ref[...].astype(jnp.bfloat16)
    for i in range(texts_here):
        text_ref[i : i + 1, :] = text_sum[2 * i : 2 * i + 1, :] + text_sum[2 * i + 1 : 2 * i + 2, :]


def on_device(
    tokens, token_counts, w_qkv, w_out, w_up, w_down, ln_gains, cache, node_text, adj_tiles,
    adj_values, w_gnn, out_grad
):
    shards = lax.axis_size("graph")
    cores = lax.axis_size("mp")
    me = lax.axis_index("graph").astype(jnp.int32).reshape(1)
    core_at = lax.axis_index("mp")
    core = core_at.astype(jnp.int32).reshape(1)
    texts_here, seq, width = tokens.shape
    nodes_here, half = cache.shape
    tiles_here, entries, tile_rows = adj_values.shape[:3]
    texts = texts_here * shards
    slots = up_to(texts, LANES)
    per = width // shards
    deep = up_to(per, ROWS)
    count = texts_here * seq
    inner = w_up.shape[1]

    def swap(values):
        return lax.ppermute(values, "mp", [(i, cores - 1 - i) for i in range(cores)])

    def spread(values):
        return lax.all_to_all(values, "graph", split_axis=0, concat_axis=0, tiled=True)

    index = call(
        functools.partial(index_body, texts_here),
        [shape((shards, slots + LANES), jnp.int32)],
        [adj_tiles, me, node_text.reshape(tiles_here, tile_rows)],
        [SMEM, SMEM, VMEM],
        flops=1000,
        name="index",
    )
    got = spread(index)
    asked = got[:, slots]
    cache_tiles = cache.reshape(tiles_here, tile_rows, half)
    packed = call(
        pack_body,
        [shape((shards, tile_rows, half))],
        [asked, cache_tiles],
        [SMEM, VMEM],
        flops=1000,
        name="pack",
    )
    remote = spread(packed)

    w_other = swap(lax.dynamic_slice_in_dim(w_gnn, (1 - core_at) * half, half, 1))

    flat_tokens = tokens.reshape(count, width)
    partial = call(
        functools.partial(attend_body, seq),
        [shape((count, width))],
        [token_counts, flat_tokens, w_qkv.reshape(width, 3 * half), w_out],
        [SMEM, VMEM, VMEM, VMEM],
        flops=2 * count * (width * 3 * half + half * width + 2 * seq * half * 2),
        scratch=[pltpu.VMEM((count, 3 * half), jnp.bfloat16), pltpu.VMEM((count, half), jnp.bfloat16)],
        name="attend",
    )
    first, mlp = call(
        inner_body,
        [shape((count, width)), shape((count, width))],
        [flat_tokens, partial, swap(partial), w_up, w_down, ln_gains],
        [VMEM] * 6,
        flops=4 * count * width * inner,
        scratch=[pltpu.VMEM((count, inner), jnp.bfloat16)],
        name="inner",
    )
    pooled = call(
        functools.partial(pool_body, seq),
        [shape((shards, texts_here * half))],
        [token_counts, core, first, mlp, swap(mlp), ln_gains],
        [SMEM, SMEM, VMEM, VMEM, VMEM, VMEM],
        flops=20 * count * width,
        scratch=[pltpu.VMEM((8, width), jnp.float32)],
        name="pool",
    )
    pooled = spread(pooled)

    kept, pick, own, base = call(
        mask_body,
        [
            shape(adj_values.shape),
            shape((tiles_here, tile_rows, slots)),
            shape((tiles_here, tile_rows, slots)),
            shape(cache_tiles.shape),
        ],
        [adj_tiles, me, got, adj_values, cache_tiles],
        [SMEM, SMEM, VMEM, VMEM, VMEM],
        flops=2 * adj_values.size * slots,
        name="mask",
    )
    gathered = call(
        gather_body,
        [shape((tiles_here, tile_rows, half))],
        [adj_tiles, me, kept, pick, pooled, cache_tiles, remote],
        [SMEM, SMEM] + [VMEM] * 5,
        flops=2 * adj_values.size * half,
        scratch=[pltpu.VMEM((entries, tile_rows, half), jnp.bfloat16)],
        name="gather",
    ).reshape(nodes_here, half)
    node_out, slope = call(
        forward_body,
        [shape((nodes_here, half)), shape((nodes_here, half))],
        [
            core, gathered, swap(gathered), w_gnn, w_other, out_grad, own.reshape(nodes_here, slots),
            base.reshape(nodes_here, half), pooled,
        ],
        [SMEM] + [VMEM] * 8,
        flops=4 * nodes_here * half * half,
        name="forward",
    )
    grad_tiles = out_grad.reshape(tiles_here, tile_rows, half)
    send, local = call(
        functools.partial(backward_body, per, texts_here),
        [
            shape((shards, tile_rows + deep + ROWS, half)),
            shape((tiles_here, tile_rows, half), jnp.float32),
        ],
        [
            adj_tiles, me, core, slope, swap(slope), gathered, w_gnn, adj_values,
            pick.reshape(nodes_here, slots), own.reshape(nodes_here, slots), grad_tiles,
        ],
        [SMEM, SMEM, SMEM] + [VMEM] * 8,
        flops=8 * nodes_here * half * half,
        scratch=[
            pltpu.VMEM((nodes_here, half), jnp.bfloat16),
            pltpu.VMEM((width + ROWS, half), jnp.float32),
            pltpu.VMEM((slots, half), jnp.float32),
        ],
        name="backward",
    )
    returned = spread(send)
    node_grad, w_part, text_grad = call(
        functools.partial(finish_body, per, texts_here),
        [
            shape((tiles_here, tile_rows, half)),
            shape((deep, half), jnp.float32),
            shape((texts_here, half), jnp.float32),
        ],
        [asked, local, returned],
        [SMEM, VMEM, VMEM],
        flops=1000,
        scratch=[pltpu.VMEM((tiles_here, tile_rows, half), jnp.float32)],
        name="finish",
    )
    return (node_out, w_part[:per].T, text_grad, node_grad.reshape(nodes_here, half))


def solution(mesh):
    placed = (
        P("graph", None, None),
        P("graph", None),
        P(None, None, "mp"),
        P("mp", None),
        P(None, "mp"),
        P("mp", None),
        P(),
        P("graph", "mp"),
        P("graph"),
        P("graph", None),
        P("graph", None, None, None),
        P("mp", None),
        P("graph", "mp"),
    )
    return jax.shard_map(
        on_device,
        mesh=mesh,
        in_specs=placed,
        out_specs=(P("graph", "mp"), P("mp", "graph"), P("graph", "mp"), P("graph", "mp")),
        check_vma=False,
    )
```

```python
import functools
import math

import jax
import jax.numpy as jnp
from jax import lax
from jax.experimental import pallas as pl
from jax.experimental.pallas import tpu as pltpu
from jax.sharding import PartitionSpec as P


HEAD = 64
LANES = 128
ROWS = 16
SPARE = 6 << 20
NORM_EPS = 1e-05
MASKED = -1e30
NO_NODE = -(1 << 20)
ROOT = 0.7978845608028654
CUBE = 0.044715

VMEM = pl.BlockSpec(memory_space=pltpu.VMEM)
SMEM = pl.BlockSpec(memory_space=pltpu.SMEM)


def up_to(value, unit):
    return (value + unit - 1) // unit * unit


def call(body, outs, ins, specs, flops, scratch=()):
    moved = sum(a.size * a.dtype.itemsize for a in ins) + sum(
        o.size * o.dtype.itemsize for o in outs
    )
    many = len(outs) > 1
    held = sum(math.prod(s.shape) * jnp.dtype(s.dtype).itemsize for s in scratch)
    return pl.pallas_call(
        body,
        out_shape=tuple(outs) if many else outs[0],
        in_specs=list(specs),
        out_specs=tuple([VMEM] * len(outs)) if many else VMEM,
        scratch_shapes=list(scratch),
        compiler_params=pltpu.CompilerParams(vmem_limit_bytes=moved + moved // 8 + held + SPARE),
        cost_estimate=pl.CostEstimate(flops=flops, bytes_accessed=moved, transcendentals=0),
    )(*ins)


def shape(dims, dtype=jnp.bfloat16):
    return jax.ShapeDtypeStruct(tuple(dims), dtype)


def mm(a, b, dims=(1, 0)):
    return lax.dot_general(
        a, b, (((dims[0],), (dims[1],)), ((), ())), preferred_element_type=jnp.float32
    )


def tile_of(tile_id, tiles_here):
    safe = jnp.maximum(tile_id, 0)
    owner = lax.div(safe, jnp.int32(tiles_here))
    return safe, owner, safe - owner * tiles_here


def index_body(texts_here, ids_ref, self_ref, text_ref, out_ref):
    tiles_here, entries = ids_ref.shape
    shards, _, lanes = out_ref.shape
    width = lanes - LANES
    texts = texts_here * shards
    me = self_ref[0]
    row = lax.broadcasted_iota(jnp.int32, (shards, LANES), 0)
    wanted = jnp.full((shards, LANES), -1, jnp.int32)
    for r in range(tiles_here):
        for k in range(entries):
            tile_id = ids_ref[r, k]
            _, owner, place = tile_of(tile_id, tiles_here)
            target = jnp.where((tile_id >= 0) & (owner != me), owner, -1)
            wanted = jnp.where(row == target, place, wanted)
    out_ref[:, :, width:] = wanted.reshape(shards, 1, LANES)
    tile_rows = text_ref.shape[1]
    lane = lax.broadcasted_iota(jnp.int32, (LANES, tile_rows), 1)
    sub = lax.broadcasted_iota(jnp.int32, (LANES, LANES), 0)
    diagonal = sub == lax.broadcasted_iota(jnp.int32, (LANES, LANES), 1)
    for c in range(width // LANES):
        slot = c * LANES + lax.broadcasted_iota(jnp.int32, (LANES, 1), 0)
        part = lax.div(slot, jnp.int32(shards))
        text = jnp.where(slot < texts, (slot - part * shards) * texts_here + part, -5)
        best = jnp.full((LANES, tile_rows), NO_NODE, jnp.int32)
        for j in range(tiles_here):
            node = (me * tiles_here + j) * tile_rows + lane
            best = jnp.where(text_ref[j : j + 1, :] == text, node, best)
        column = jnp.max(best.astype(jnp.float32), axis=1, keepdims=True)
        line = jnp.max(jnp.where(diagonal, column, float(NO_NODE)), axis=0, keepdims=True)
        out_ref[:, :, c * LANES : (c + 1) * LANES] = (
            jnp.broadcast_to(line, (shards, LANES)).astype(jnp.int32).reshape(shards, 1, LANES)
        )


def pack_body(asked_ref, cache_ref, out_ref):
    def one(q, carry):
        out_ref[q] = cache_ref[jnp.maximum(asked_ref[q], 0)]
        return carry

    lax.fori_loop(0, out_ref.shape[0], one, 0)


def mask_body(ids_ref, self_ref, got_ref, adj_ref, cache_ref, kept_ref, pick_ref, own_ref, base_ref):
    tiles_here, entries, tile_rows, _ = adj_ref.shape
    shards, _, lanes = got_ref.shape
    width = lanes - LANES
    me = self_ref[0]
    table = jnp.max(
        got_ref[:, :, :width].reshape(shards, width).astype(jnp.float32), axis=0, keepdims=True
    )
    place = lax.broadcasted_iota(jnp.int32, (tile_rows, width), 0).astype(jnp.float32)
    ones = jnp.ones((ROWS, width), jnp.bfloat16)

    def holds(tile_id):
        first = (tile_id * tile_rows).astype(jnp.float32)
        return jnp.where(table - first == place, 1.0, 0.0)

    for r in range(tiles_here):

        def one(k, total):
            tile_id = ids_ref[r, k]
            hot = holds(tile_id).astype(jnp.bfloat16)
            values = adj_ref[r, k]
            taken = mm(ones, hot, (1, 1))[0:1, :]
            keep = jnp.where(tile_id >= 0, 1.0, 0.0) * jnp.where(taken > 0.5, 0.0, 1.0)
            kept_ref[r, k] = (values.astype(jnp.float32) * keep).astype(jnp.bfloat16)
            return total + mm(values, hot)

        pick = lax.fori_loop(0, entries, one, jnp.zeros((tile_rows, width), jnp.float32))
        pick_ref[r] = pick.astype(jnp.bfloat16)
        hot = holds(me * tiles_here + r)
        own_ref[r] = hot.astype(jnp.bfloat16)
        fresh = jnp.max(hot, axis=1, keepdims=True)
        base_ref[r] = (cache_ref[r].astype(jnp.float32) * (1.0 - fresh)).astype(jnp.bfloat16)


def norm(values, gain):
    average = jnp.mean(values, axis=-1, keepdims=True)
    centred = values - average
    variance = jnp.mean(centred * centred, axis=-1, keepdims=True)
    return centred * lax.rsqrt(variance + NORM_EPS) * gain


def attend_body(seq, counts_ref, tokens_ref, w_qkv_ref, w_out_ref, out_ref, proj_ref, ctx_ref):
    half = w_out_ref.shape[0]
    texts_here = tokens_ref.shape[0] // seq
    for c in range(3):
        proj_ref[:, c * half : (c + 1) * half] = mm(
            tokens_ref[...], w_qkv_ref[:, c * half : (c + 1) * half]
        ).astype(jnp.bfloat16)
    left = lax.broadcasted_iota(jnp.int32, (seq, LANES), 1) < HEAD
    key_at = lax.broadcasted_iota(jnp.int32, (seq, seq), 1)
    for t in range(texts_here):
        rows = slice(t * seq, (t + 1) * seq)
        live = key_at < counts_ref[0, t]
        for pair in range(half // LANES):
            first = pair * LANES
            query = proj_ref[rows, first : first + LANES].astype(jnp.float32) * (HEAD**-0.5)
            key = proj_ref[rows, half + first : half + first + LANES]
            value = proj_ref[rows, 2 * half + first : 2 * half + first + LANES]
            sides = []
            for side in (left, jnp.logical_not(left)):
                scores = mm(jnp.where(side, query, 0.0).astype(jnp.bfloat16), key, (1, 1))
                scores = jnp.where(live, scores, MASKED)
                powers = jnp.exp(scores - jnp.max(scores, axis=-1, keepdims=True))
                total = jnp.sum(powers, axis=-1, keepdims=True)
                sides.append(mm((powers / total).astype(jnp.bfloat16), value))
            ctx_ref[rows, first : first + LANES] = jnp.where(left, sides[0], sides[1]).astype(
                jnp.bfloat16
            )
    out_ref[...] = mm(ctx_ref[...], w_out_ref[...]).astype(jnp.bfloat16)


def inner_body(tokens_ref, mine_ref, other_ref, up_ref, down_ref, gains_ref, first_ref, out_ref, inner_ref):
    added = mine_ref[...].astype(jnp.float32) + other_ref[...].astype(jnp.float32)
    first = norm(tokens_ref[...].astype(jnp.float32) + added, gains_ref[0:1, :])
    first_ref[...] = first.astype(jnp.bfloat16)
    hidden_units = up_ref.shape[1]
    step = hidden_units // 4
    for c in range(4):
        cols = slice(c * step, (c + 1) * step)
        value = mm(first_ref[...], up_ref[:, cols])
        gate = jnp.tanh(ROOT * (value + CUBE * (value * value * value)))
        inner_ref[:, cols] = (0.5 * value * (1.0 + gate)).astype(jnp.bfloat16)
    out_ref[...] = mm(inner_ref[...], down_ref[...]).astype(jnp.bfloat16)


def pool_body(seq, counts_ref, core_ref, first_ref, mine_ref, other_ref, gains_ref, out_ref, pooled_ref):
    _, _, lanes = out_ref.shape
    texts_here = first_ref.shape[0] // seq
    half = lanes // texts_here
    for t in range(texts_here):
        rows = slice(t * seq, (t + 1) * seq)
        added = mine_ref[rows, :].astype(jnp.float32) + other_ref[rows, :].astype(jnp.float32)
        second = norm(first_ref[rows, :].astype(jnp.float32) + added, gains_ref[1:2, :])
        count = counts_ref[0, t]
        live = lax.broadcasted_iota(jnp.int32, (seq, 1), 0) < count
        total = jnp.sum(jnp.where(live, second, 0.0), axis=0, keepdims=True)
        pooled_ref[...] = jnp.broadcast_to(
            total / count.astype(jnp.float32), pooled_ref.shape
        )
        start = pl.multiple_of(core_ref[0] * half, LANES)
        own = pooled_ref[:, pl.ds(start, half)][0:1, :]
        own = own.astype(jnp.bfloat16).astype(jnp.float32)
        out_ref[:, :, t * half : (t + 1) * half] = own.reshape(1, 1, half)


def pooled_rows(me, near_ref, far_ref, half):
    shards = 2 * near_ref.shape[0]
    parts = []
    for first in range(0, near_ref.shape[2], half):
        for ref in (near_ref, far_ref):
            part = ref[:, :, first : first + half].reshape(shards // 2, half)
            parts.append(part.astype(jnp.bfloat16))
    stacked = jnp.concatenate(parts, axis=0)
    texts = stacked.shape[0]
    row = lax.broadcasted_iota(jnp.int32, (texts, texts), 0)
    column = lax.broadcasted_iota(jnp.int32, (texts, texts), 1)
    order = jnp.where(row == (column ^ me), 1.0, 0.0).astype(jnp.bfloat16)
    return mm(order, stacked).astype(jnp.bfloat16)


def fresh_body(self_ref, near_ref, far_ref, pick_ref, own_ref, base_ref, start_ref, feature_ref):
    half = base_ref.shape[2]
    pooled = pooled_rows(self_ref[0], near_ref, far_ref, half)
    texts = pooled.shape[0]
    for r in range(pick_ref.shape[0]):
        start_ref[r] = mm(pick_ref[r][:, :texts], pooled)
        feature_ref[r] = (
            base_ref[r].astype(jnp.float32) + mm(own_ref[r][:, :texts], pooled)
        ).astype(jnp.bfloat16)


def gather_body(ids_ref, self_ref, kept_ref, start_ref, cache_ref, remote_ref, out_ref, source_ref):
    tiles_here, entries, _, _ = kept_ref.shape
    me = self_ref[0]
    for r in range(tiles_here):

        def fetch(k, carry):
            tile_id = ids_ref[r, k]
            _, owner, place = tile_of(tile_id, tiles_here)
            local = (owner == me) | (tile_id < 0)

            @pl.when(local)
            def _():
                source_ref[k] = cache_ref[place]

            @pl.when(jnp.logical_not(local))
            def _():
                source_ref[k] = remote_ref[owner]

            return carry

        lax.fori_loop(0, entries, fetch, 0)
        total = start_ref[r]
        for k in range(entries):
            total = total + mm(kept_ref[r, k], source_ref[k])
        out_ref[r] = total.astype(jnp.bfloat16)


def forward_body(core_ref, mine_ref, other_ref, w_own_ref, w_other_ref, grad_ref, feature_ref, node_ref, slope_ref):
    _, half = mine_ref.shape
    start = pl.multiple_of(core_ref[0] * half, LANES)
    hidden = mm(mine_ref[...], w_own_ref[:, pl.ds(start, half)]) + mm(
        other_ref[...], w_other_ref[...]
    )
    square = hidden * hidden
    gate = jnp.tanh(ROOT * hidden * (1.0 + CUBE * square))
    lifted = 0.5 * (1.0 + gate)
    slope = lifted + 0.5 * hidden * (1.0 - gate * gate) * (ROOT * (1.0 + 3.0 * CUBE * square))
    slope_ref[...] = (grad_ref[...].astype(jnp.float32) * slope).astype(jnp.bfloat16)
    node_ref[...] = (feature_ref[...].astype(jnp.float32) + hidden * lifted).astype(jnp.bfloat16)


def backward_body(
    ids_ref, self_ref, core_ref, mine_ref, other_ref, w_own_ref, adj_ref, send_ref, down_ref
):
    tiles_here, entries, tile_rows, _ = adj_ref.shape
    half = send_ref.shape[2]
    me = self_ref[0]
    core = core_ref[0]
    own = pl.multiple_of(core * half, LANES)
    far = pl.multiple_of((1 - core) * half, LANES)
    down = mm(mine_ref[...], w_own_ref[:, pl.ds(own, half)], (1, 1)) + mm(
        other_ref[...], w_own_ref[:, pl.ds(far, half)], (1, 1)
    )
    down_ref[...] = down.astype(jnp.bfloat16)
    for r in range(tiles_here):
        rows = slice(r * tile_rows, (r + 1) * tile_rows)

        def one(k, carry):
            tile_id = ids_ref[r, k]
            _, owner, _ = tile_of(tile_id, tiles_here)

            @pl.when((tile_id >= 0) & (owner != me))
            def _():
                send_ref[owner] = mm(adj_ref[r, k], down_ref[rows, :], (0, 0)).astype(jnp.bfloat16)

            return carry

        lax.fori_loop(0, entries, one, 0)


def chunk_body(
    per, texts_here, self_ref, core_ref, mine_ref, other_ref, agg_ref, down_ref, pick_ref, own_ref,
    grad_ref, keep_ref, give_ref, w_ref, text_ref
):
    kept, _, half = keep_ref.shape
    shards = 2 * kept
    me = self_ref[0]
    core = core_ref[0]
    own = pl.multiple_of(core * half, LANES)
    far = pl.multiple_of((1 - core) * half, LANES)
    text_ref[...] = mm(pick_ref[...], down_ref[...], (0, 0)) + mm(
        own_ref[...], grad_ref[...], (0, 0)
    )
    columns = 2 * half
    w_ref[pl.ds(own, half), :] = mm(mine_ref[...], agg_ref[...], (0, 0))
    w_ref[pl.ds(far, half), :] = mm(other_ref[...], agg_ref[...], (0, 0))
    w_ref[columns:, :] = jnp.zeros((w_ref.shape[0] - columns, half), jnp.float32)
    deep = up_to(per, ROWS)
    row = lax.broadcasted_iota(jnp.int32, (ROWS, half), 0)
    for q in range(shards):
        piece = w_ref[q * per : q * per + deep, :].astype(jnp.bfloat16)
        block = jnp.zeros((ROWS, half), jnp.float32)
        for i in range(texts_here):
            line = text_ref[i * shards + q : i * shards + q + 1, :]
            high = line.astype(jnp.bfloat16).astype(jnp.float32)
            block = jnp.where(row == i, high, block)
            block = jnp.where(row == ROWS // 2 + i, line - high, block)
        block = block.astype(jnp.bfloat16)
        step = q ^ me
        turned = step * 0
        reach = 1
        while reach < shards:
            turned = 2 * turned + ((step // reach) & 1)
            reach *= 2

        @pl.when(turned < kept)
        def _():
            keep_ref[turned, :deep, :] = piece
            keep_ref[turned, deep:, :] = block

        @pl.when(turned >= kept)
        def _():
            give_ref[turned - kept, :deep, :] = piece
            give_ref[turned - kept, deep:, :] = block


def fold(mine, theirs, deep):
    total = mine.astype(jnp.float32) + theirs.astype(jnp.float32)
    text = total[deep : deep + ROWS // 2, :] + total[deep + ROWS // 2 :, :]
    return total[:deep, :], text


def fold_body(deep, mine_ref, theirs_ref, keep_ref, give_ref):
    kept = keep_ref.shape[0]
    for s in range(2 * kept):
        w_sum, text = fold(mine_ref[s], theirs_ref[s], deep)
        high = text.astype(jnp.bfloat16).astype(jnp.float32)
        out_ref = (keep_ref if s < kept else give_ref).at[s % kept]
        out_ref[:deep, :] = w_sum.astype(jnp.bfloat16)
        out_ref[deep:, :] = jnp.concatenate([high, text - high], axis=0).astype(jnp.bfloat16)


def close_body(deep, mine_ref, theirs_ref, w_ref, text_ref):
    w_sum, text = fold(mine_ref[0], theirs_ref[0], deep)
    w_ref[...] = w_sum
    text_ref[...] = text[: text_ref.shape[0], :]


def local_body(ids_ref, self_ref, down_ref, adj_ref, grad_ref, local_ref):
    tiles_here, entries, _, _ = adj_ref.shape
    me = self_ref[0]
    local_ref[...] = grad_ref[...].astype(jnp.float32)
    for r in range(tiles_here):

        def one(k, carry):
            tile_id = ids_ref[r, k]
            _, owner, place = tile_of(tile_id, tiles_here)

            @pl.when((tile_id >= 0) & (owner == me))
            def _():
                local_ref[place] += mm(adj_ref[r, k], down_ref[r], (0, 0))

            return carry

        lax.fori_loop(0, entries, one, 0)


def finish_body(asked_ref, local_ref, got_ref, node_ref, sum_ref):
    sum_ref[...] = local_ref[...]

    def one(q, carry):
        asked = asked_ref[q]

        @pl.when(asked >= 0)
        def _():
            sum_ref[asked] += got_ref[q].astype(jnp.float32)

        return carry

    lax.fori_loop(0, got_ref.shape[0], one, 0)
    node_ref[...] = sum_ref[...].astype(jnp.bfloat16)


def step(
    tokens, token_counts, w_qkv, w_out, w_up, w_down, ln_gains, cache, node_text, adj_tiles,
    adj_values, w_gnn, out_grad
):
    shards = lax.axis_size("graph")
    cores = lax.axis_size("mp")
    me = lax.axis_index("graph").astype(jnp.int32).reshape(1)
    core_at = lax.axis_index("mp")
    core = core_at.astype(jnp.int32).reshape(1)
    texts_here, seq, width = tokens.shape
    nodes_here, half = cache.shape
    tiles_here, entries, tile_rows = adj_values.shape[:3]
    texts = texts_here * shards
    slots = up_to(texts, LANES)
    per = width // shards
    deep = up_to(per, ROWS)
    count = texts_here * seq
    inner = w_up.shape[1]

    def swap(values):
        return lax.ppermute(values, "mp", [(i, cores - 1 - i) for i in range(cores)])

    def toward(values, reach):
        return lax.ppermute(values, "graph", [(i, i ^ reach) for i in range(shards)])

    def spread(values):
        return lax.all_to_all(values, "graph", split_axis=0, concat_axis=0, tiled=True)

    index = call(
        functools.partial(index_body, texts_here),
        [shape((shards, 1, slots + LANES), jnp.int32)],
        [adj_tiles, me, node_text.reshape(tiles_here, tile_rows)],
        [SMEM, SMEM, VMEM],
        flops=1000,
    )
    got = spread(index)
    asked = got[:, 0, slots]
    cache_tiles = cache.reshape(tiles_here, tile_rows, half)
    packed = call(
        pack_body,
        [shape((shards, tile_rows, half))],
        [asked, cache_tiles],
        [SMEM, VMEM],
        flops=1000,
    )
    remote = spread(packed)

    w_other = swap(lax.dynamic_slice_in_dim(w_gnn, (1 - core_at) * half, half, 1))

    flat_tokens = tokens.reshape(count, width)
    partial = call(
        functools.partial(attend_body, seq),
        [shape((count, width))],
        [token_counts, flat_tokens, w_qkv.reshape(width, 3 * half), w_out],
        [SMEM, VMEM, VMEM, VMEM],
        flops=2 * count * (width * 3 * half + half * width + 2 * seq * half * 2),
        scratch=[pltpu.VMEM((count, 3 * half), jnp.bfloat16), pltpu.VMEM((count, half), jnp.bfloat16)],
    )
    first, mlp = call(
        inner_body,
        [shape((count, width)), shape((count, width))],
        [flat_tokens, partial, swap(partial), w_up, w_down, ln_gains],
        [VMEM] * 6,
        flops=4 * count * width * inner,
        scratch=[pltpu.VMEM((count, inner), jnp.bfloat16)],
    )
    pooled = call(
        functools.partial(pool_body, seq),
        [shape((1, 1, texts_here * half), jnp.float32)],
        [token_counts, core, first, mlp, swap(mlp), ln_gains],
        [SMEM, SMEM, VMEM, VMEM, VMEM, VMEM],
        flops=20 * count * width,
        scratch=[pltpu.VMEM((8, width), jnp.float32)],
    )
    near = pooled
    reach = 1
    far = toward(near, reach)
    while 4 * reach <= shards:
        reach *= 2
        near = jnp.concatenate([near, far], axis=0)
        far = toward(near, reach)

    kept, pick, own, base = call(
        mask_body,
        [
            shape(adj_values.shape),
            shape((tiles_here, tile_rows, slots)),
            shape((tiles_here, tile_rows, slots)),
            shape(cache_tiles.shape),
        ],
        [adj_tiles, me, got, adj_values, cache_tiles],
        [SMEM, SMEM, VMEM, VMEM, VMEM],
        flops=2 * adj_values.size * slots,
    )
    start, features = call(
        fresh_body,
        [shape((tiles_here, tile_rows, half), jnp.float32), shape((tiles_here, tile_rows, half))],
        [me, near, far, pick, own, base],
        [SMEM] + [VMEM] * 5,
        flops=4 * nodes_here * texts * half,
    )
    gathered = call(
        gather_body,
        [shape((tiles_here, tile_rows, half))],
        [adj_tiles, me, kept, start, cache_tiles, remote],
        [SMEM, SMEM] + [VMEM] * 4,
        flops=2 * adj_values.size * half,
        scratch=[pltpu.VMEM((entries, tile_rows, half), jnp.bfloat16)],
    ).reshape(nodes_here, half)
    node_out, slope = call(
        forward_body,
        [shape((nodes_here, half)), shape((nodes_here, half))],
        [
            core, gathered, swap(gathered), w_gnn, w_other, out_grad,
            features.reshape(nodes_here, half),
        ],
        [SMEM] + [VMEM] * 6,
        flops=4 * nodes_here * half * half,
    )
    grad_tiles = out_grad.reshape(tiles_here, tile_rows, half)
    slope_other = swap(slope)
    send, down = call(
        backward_body,
        [shape((shards, tile_rows, half)), shape((nodes_here, half))],
        [adj_tiles, me, core, slope, slope_other, w_gnn, adj_values],
        [SMEM, SMEM, SMEM] + [VMEM] * 4,
        flops=4 * nodes_here * half * half + 2 * adj_values.size * half,
    )
    returned = spread(send)
    keep, give = call(
        functools.partial(chunk_body, per, texts_here),
        [shape((shards // 2, deep + ROWS, half)), shape((shards // 2, deep + ROWS, half))],
        [
            me, core, slope, slope_other, gathered, down, pick.reshape(nodes_here, slots),
            own.reshape(nodes_here, slots), out_grad,
        ],
        [SMEM, SMEM] + [VMEM] * 7,
        flops=4 * nodes_here * half * (half + slots),
        scratch=[
            pltpu.VMEM((width + ROWS, half), jnp.float32),
            pltpu.VMEM((slots, half), jnp.float32),
        ],
    )
    local = call(
        local_body,
        [shape((tiles_here, tile_rows, half), jnp.float32)],
        [adj_tiles, me, down.reshape(tiles_here, tile_rows, half), adj_values, grad_tiles],
        [SMEM, SMEM] + [VMEM] * 3,
        flops=2 * adj_values.size * half,
    )
    reach = 1
    given = toward(give, reach)
    while 2 * reach < shards:
        part = (shards // (4 * reach), deep + ROWS, half)
        keep, give = call(
            functools.partial(fold_body, deep),
            [shape(part), shape(part)],
            [keep, given],
            [VMEM] * 2,
            flops=4 * math.prod(part),
        )
        reach *= 2
        given = toward(give, reach)
    w_part, text_grad = call(
        functools.partial(close_body, deep),
        [shape((deep, half), jnp.float32), shape((texts_here, half), jnp.float32)],
        [keep, given],
        [VMEM] * 2,
        flops=1000,
    )
    node_grad = call(
        finish_body,
        [shape((tiles_here, tile_rows, half))],
        [asked, local, returned],
        [SMEM, VMEM, VMEM],
        flops=1000,
        scratch=[pltpu.VMEM((tiles_here, tile_rows, half), jnp.float32)],
    )
    return (node_out, w_part[:per].T, text_grad, node_grad.reshape(nodes_here, half))


def solution(mesh):
    placed = (
        P("graph", None, None),
        P("graph", None),
        P(None, None, "mp"),
        P("mp", None),
        P(None, "mp"),
        P("mp", None),
        P(),
        P("graph", "mp"),
        P("graph"),
        P("graph", None),
        P("graph", None, None, None),
        P("mp", None),
        P("graph", "mp"),
    )
    return jax.shard_map(
        step,
        mesh=mesh,
        in_specs=placed,
        out_specs=(P("graph", "mp"), P("mp", "graph"), P("graph", "mp"), P("graph", "mp")),
        check_vma=False,
    )
```

```python
import functools
import math

import jax
import jax.numpy as jnp
from jax import lax
from jax.experimental import pallas as pl
from jax.experimental.pallas import tpu as pltpu
from jax.sharding import PartitionSpec as P


HEAD = 64
LANES = 128
ROWS = 16
SPARE = 6 << 20
NORM_EPS = 1e-05
MASKED = -1e30
NO_NODE = -(1 << 20)
ROOT = 0.7978845608028654
CUBE = 0.044715

VMEM = pl.BlockSpec(memory_space=pltpu.VMEM)
HBM = pl.BlockSpec(memory_space=pltpu.HBM)
SMEM = pl.BlockSpec(memory_space=pltpu.SMEM)


def up_to(value, unit):
    return (value + unit - 1) // unit * unit


def call(body, outs, ins, specs, flops, scratch=(), out_specs=None):
    moved = sum(a.size * a.dtype.itemsize for a in ins) + sum(
        o.size * o.dtype.itemsize for o in outs
    )
    many = len(outs) > 1
    ins = [
        pltpu.with_memory_space_constraint(a, pltpu.HBM) if s is HBM else a
        for a, s in zip(ins, specs, strict=True)
    ]
    held = sum(math.prod(s.shape) * jnp.dtype(s.dtype).itemsize for s in scratch if counted(s))
    out_specs = out_specs or [VMEM] * len(outs)
    outs = [
        pltpu.HBM(o.shape, o.dtype) if s is HBM else o for o, s in zip(outs, out_specs, strict=True)
    ]
    return pl.pallas_call(
        body,
        out_shape=tuple(outs) if many else outs[0],
        in_specs=list(specs),
        out_specs=tuple(out_specs) if many else out_specs[0],
        scratch_shapes=list(scratch),
        compiler_params=pltpu.CompilerParams(vmem_limit_bytes=moved + moved // 8 + held + SPARE),
        cost_estimate=pl.CostEstimate(flops=flops, bytes_accessed=moved, transcendentals=0),
    )(*ins)


def counted(scratch):
    return jnp.issubdtype(scratch.dtype, jnp.number)


def copies(pairs, sems):
    started = [pltpu.make_async_copy(a, b, sems.at[i]) for i, (a, b) in enumerate(pairs)]
    for copy in started:
        copy.start()
    return started


def unroll(steps):
    return steps if steps <= 8 else 1


def shape(dims, dtype=jnp.bfloat16):
    return jax.ShapeDtypeStruct(tuple(dims), dtype)


def mm(a, b, dims=(1, 0)):
    return lax.dot_general(
        a, b, (((dims[0],), (dims[1],)), ((), ())), preferred_element_type=jnp.float32
    )


def tile_of(tile_id, tiles_here):
    safe = jnp.maximum(tile_id, 0)
    owner = lax.div(safe, jnp.int32(tiles_here))
    return safe, owner, safe - owner * tiles_here


def index_body(texts_here, ids_hbm, self_ref, text_hbm, out_ref, ids_ref, text_ref, sems):
    for copy in copies([(ids_hbm, ids_ref), (text_hbm, text_ref)], sems):
        copy.wait()
    tiles_here, entries = ids_ref.shape
    shards, _, lanes = out_ref.shape
    width = lanes - LANES
    texts = texts_here * shards
    me = self_ref[0]
    row = lax.broadcasted_iota(jnp.int32, (shards, LANES), 0)
    wanted = jnp.full((shards, LANES), -1, jnp.int32)
    for r in range(tiles_here):
        for k in range(entries):
            tile_id = ids_ref[r, k]
            _, owner, place = tile_of(tile_id, tiles_here)
            target = jnp.where((tile_id >= 0) & (owner != me), owner, -1)
            wanted = jnp.where(row == target, place, wanted)
    out_ref[:, :, width:] = wanted.reshape(shards, 1, LANES)
    tile_rows = text_ref.shape[1]
    lane = lax.broadcasted_iota(jnp.int32, (LANES, tile_rows), 1)
    sub = lax.broadcasted_iota(jnp.int32, (LANES, LANES), 0)
    diagonal = sub == lax.broadcasted_iota(jnp.int32, (LANES, LANES), 1)
    for c in range(width // LANES):
        slot = c * LANES + lax.broadcasted_iota(jnp.int32, (LANES, 1), 0)
        part = lax.div(slot, jnp.int32(shards))
        text = jnp.where(slot < texts, (slot - part * shards) * texts_here + part, -5)
        best = jnp.full((LANES, tile_rows), NO_NODE, jnp.int32)
        for j in range(tiles_here):
            node = (me * tiles_here + j) * tile_rows + lane
            best = jnp.where(text_ref[j : j + 1, :] == text, node, best)
        column = jnp.max(best.astype(jnp.float32), axis=1, keepdims=True)
        line = jnp.max(jnp.where(diagonal, column, float(NO_NODE)), axis=0, keepdims=True)
        out_ref[:, :, c * LANES : (c + 1) * LANES] = (
            jnp.broadcast_to(line, (shards, LANES)).astype(jnp.int32).reshape(shards, 1, LANES)
        )


def pack_body(asked_ref, cache_hbm, out_hbm, tile_ref, in_sems, out_sems):
    tiles_here = tile_ref.shape[0]
    for copy in copies([(cache_hbm.at[j], tile_ref.at[j]) for j in range(tiles_here)], in_sems):
        copy.wait()

    def slot(q):
        place = jnp.maximum(asked_ref[q], 0)
        return pltpu.make_async_copy(tile_ref.at[place], out_hbm.at[q], out_sems.at[q])

    shards = out_hbm.shape[0]
    lax.fori_loop(0, shards, lambda q, c: (slot(q).start(), c)[1], 0)
    lax.fori_loop(0, shards, lambda q, c: (slot(q).wait(), c)[1], 0)


def mask_body(ids_ref, self_ref, got_ref, adj_ref, cache_ref, kept_ref, pick_ref, own_ref, base_ref):
    tiles_here, entries, tile_rows, _ = adj_ref.shape
    shards, _, lanes = got_ref.shape
    width = lanes - LANES
    me = self_ref[0]
    table = jnp.max(
        got_ref[:, :, :width].reshape(shards, width).astype(jnp.float32), axis=0, keepdims=True
    )
    place = lax.broadcasted_iota(jnp.int32, (tile_rows, width), 0).astype(jnp.float32)
    ones = jnp.ones((ROWS, width), jnp.bfloat16)

    def holds(tile_id):
        first = (tile_id * tile_rows).astype(jnp.float32)
        return jnp.where(table - first == place, 1.0, 0.0)

    for r in range(tiles_here):

        def one(k, total):
            tile_id = ids_ref[r, k]
            hot = holds(tile_id).astype(jnp.bfloat16)
            values = adj_ref[r, k]
            taken = mm(ones, hot, (1, 1))[0:1, :]
            keep = jnp.where(tile_id >= 0, 1.0, 0.0) * jnp.where(taken > 0.5, 0.0, 1.0)
            kept_ref[r, k] = (values.astype(jnp.float32) * keep).astype(jnp.bfloat16)
            return total + mm(values, hot)

        pick = lax.fori_loop(
            0, entries, one, jnp.zeros((tile_rows, width), jnp.float32), unroll=unroll(entries)
        )
        pick_ref[r] = pick.astype(jnp.bfloat16)
        hot = holds(me * tiles_here + r)
        own_ref[r] = hot.astype(jnp.bfloat16)
        fresh = jnp.max(hot, axis=1, keepdims=True)
        base_ref[r] = (cache_ref[r].astype(jnp.float32) * (1.0 - fresh)).astype(jnp.bfloat16)


def norm(values, gain):
    average = jnp.mean(values, axis=-1, keepdims=True)
    centred = values - average
    variance = jnp.mean(centred * centred, axis=-1, keepdims=True)
    return centred * lax.rsqrt(variance + NORM_EPS) * gain


def attend_body(seq, counts_ref, tokens_ref, w_qkv_ref, w_out_ref, out_ref, proj_ref, ctx_ref):
    half = w_out_ref.shape[0]
    texts_here = tokens_ref.shape[0] // seq
    for c in range(3):
        proj_ref[:, c * half : (c + 1) * half] = mm(tokens_ref[...], w_qkv_ref[c]).astype(
            jnp.bfloat16
        )
    left = lax.broadcasted_iota(jnp.int32, (seq, LANES), 1) < HEAD
    key_at = lax.broadcasted_iota(jnp.int32, (seq, seq), 1)
    for t in range(texts_here):
        rows = slice(t * seq, (t + 1) * seq)
        live = key_at < counts_ref[0, t]
        for pair in range(half // LANES):
            first = pair * LANES
            query = proj_ref[rows, first : first + LANES].astype(jnp.float32) * (HEAD**-0.5)
            key = proj_ref[rows, half + first : half + first + LANES]
            value = proj_ref[rows, 2 * half + first : 2 * half + first + LANES]
            sides = []
            for side in (left, jnp.logical_not(left)):
                scores = mm(jnp.where(side, query, 0.0).astype(jnp.bfloat16), key, (1, 1))
                scores = jnp.where(live, scores, MASKED)
                powers = jnp.exp(scores - jnp.max(scores, axis=-1, keepdims=True))
                total = jnp.sum(powers, axis=-1, keepdims=True)
                sides.append(mm((powers / total).astype(jnp.bfloat16), value))
            ctx_ref[rows, first : first + LANES] = jnp.where(left, sides[0], sides[1]).astype(
                jnp.bfloat16
            )
    out_ref[...] = mm(ctx_ref[...], w_out_ref[...]).astype(jnp.bfloat16)


def inner_body(tokens_ref, mine_ref, other_ref, up_ref, down_ref, gains_ref, first_ref, out_ref, inner_ref):
    added = mine_ref[...].astype(jnp.float32) + other_ref[...].astype(jnp.float32)
    first = norm(tokens_ref[...].astype(jnp.float32) + added, gains_ref[0:1, :])
    first_ref[...] = first.astype(jnp.bfloat16)
    hidden_units = up_ref.shape[1]
    step = hidden_units // 4
    for c in range(4):
        cols = slice(c * step, (c + 1) * step)
        value = mm(first_ref[...], up_ref[:, cols])
        gate = jnp.tanh(ROOT * (value + CUBE * (value * value * value)))
        inner_ref[:, cols] = (0.5 * value * (1.0 + gate)).astype(jnp.bfloat16)
    out_ref[...] = mm(inner_ref[...], down_ref[...]).astype(jnp.bfloat16)


def pool_body(seq, counts_ref, core_ref, first_ref, mine_ref, other_ref, gains_ref, out_ref, pooled_ref):
    _, _, lanes = out_ref.shape
    texts_here = first_ref.shape[0] // seq
    half = lanes // texts_here
    for t in range(texts_here):
        rows = slice(t * seq, (t + 1) * seq)
        added = mine_ref[rows, :].astype(jnp.float32) + other_ref[rows, :].astype(jnp.float32)
        second = norm(first_ref[rows, :].astype(jnp.float32) + added, gains_ref[1:2, :])
        count = counts_ref[0, t]
        live = lax.broadcasted_iota(jnp.int32, (seq, 1), 0) < count
        total = jnp.sum(jnp.where(live, second, 0.0), axis=0, keepdims=True)
        pooled_ref[...] = jnp.broadcast_to(
            total / count.astype(jnp.float32), pooled_ref.shape
        )
        start = pl.multiple_of(core_ref[0] * half, LANES)
        own = pooled_ref[:, pl.ds(start, half)][0:1, :]
        own = own.astype(jnp.bfloat16).astype(jnp.float32)
        out_ref[:, :, t * half : (t + 1) * half] = own.reshape(1, 1, half)


def pooled_rows(me, near_ref, far_ref, half):
    shards = 2 * near_ref.shape[0]
    parts = []
    for first in range(0, near_ref.shape[2], half):
        for ref in (near_ref, far_ref):
            part = ref[:, :, first : first + half].reshape(shards // 2, half)
            parts.append(part.astype(jnp.bfloat16))
    stacked = jnp.concatenate(parts, axis=0)
    texts = stacked.shape[0]
    row = lax.broadcasted_iota(jnp.int32, (texts, texts), 0)
    column = lax.broadcasted_iota(jnp.int32, (texts, texts), 1)
    order = jnp.where(row == (column ^ me), 1.0, 0.0).astype(jnp.bfloat16)
    return mm(order, stacked).astype(jnp.bfloat16)


def gather_body(
    ids_hbm, self_ref, kept_hbm, pick_hbm, near_hbm, far_hbm, cache_hbm, remote_ref, out_ref,
    pooled_ref, ids_ref, kept_ref, pick_ref, near_ref, far_ref, cache_ref, source_ref, sems
):
    started = copies(
        [
            (near_hbm, near_ref), (far_hbm, far_ref), (ids_hbm, ids_ref), (cache_hbm, cache_ref),
            (pick_hbm, pick_ref), (kept_hbm, kept_ref),
        ],
        sems,
    )
    tiles_here, entries, _, _ = kept_ref.shape
    half = cache_ref.shape[2]
    me = self_ref[0]
    for copy in started:
        copy.wait()
    pooled = pooled_rows(me, near_ref, far_ref, half)
    pooled_ref[...] = pooled
    texts = pooled.shape[0]

    def fetch(r, k):
        tile_id = ids_ref[r, k]
        _, owner, place = tile_of(tile_id, tiles_here)
        local = (owner == me) | (tile_id < 0)

        @pl.when(local)
        def _():
            source_ref[r % 2, k] = cache_ref[place]

        @pl.when(jnp.logical_not(local))
        def _():
            source_ref[r % 2, k] = remote_ref[owner]

    for r in range(tiles_here):
        lax.fori_loop(
            0, entries, lambda k, c: (fetch(r, k), c)[1], 0, unroll=unroll(entries)
        )
        total = mm(pick_ref[r][:, :texts], pooled)
        for k in range(entries):
            total = total + mm(kept_ref[r, k], source_ref[r % 2, k])
        out_ref[r] = total.astype(jnp.bfloat16)


def forward_body(core_ref, mine_ref, other_ref, w_own_ref, w_other_ref, grad_ref, own_ref, base_ref, pooled_ref, node_ref, slope_ref):
    _, half = mine_ref.shape
    start = pl.multiple_of(core_ref[0] * half, LANES)
    hidden = mm(mine_ref[...], w_own_ref[:, pl.ds(start, half)]) + mm(
        other_ref[...], w_other_ref[...]
    )
    square = hidden * hidden
    gate = jnp.tanh(ROOT * hidden * (1.0 + CUBE * square))
    lifted = 0.5 * (1.0 + gate)
    slope = lifted + 0.5 * hidden * (1.0 - gate * gate) * (ROOT * (1.0 + 3.0 * CUBE * square))
    slope_ref[...] = (grad_ref[...].astype(jnp.float32) * slope).astype(jnp.bfloat16)
    fresh = mm(own_ref[:, : pooled_ref.shape[0]], pooled_ref[...])
    node_ref[...] = (base_ref[...].astype(jnp.float32) + fresh + hidden * lifted).astype(
        jnp.bfloat16
    )


def backward_body(
    per, texts_here, ids_ref, self_ref, core_ref, mine_ref, other_ref, agg_ref, w_own_ref, adj_ref,
    pick_ref, own_ref, grad_ref, send_hbm, keep_hbm, give_hbm, down_hbm,
    down_ref, w_ref, text_ref, send_ref, rows_ref, half_ref, sems, slot_sems, row_sems
):
    tiles_here, entries, tile_rows, _ = adj_ref.shape
    shards, text_rows, half = rows_ref.shape
    kept = shards // 2
    me = self_ref[0]
    core = core_ref[0]
    own = pl.multiple_of(core * half, LANES)
    far = pl.multiple_of((1 - core) * half, LANES)
    down = mm(mine_ref[...], w_own_ref[:, pl.ds(own, half)], (1, 1)) + mm(
        other_ref[...], w_own_ref[:, pl.ds(far, half)], (1, 1)
    )
    down_ref[...] = down.astype(jnp.bfloat16)
    down_copy = pltpu.make_async_copy(down_ref, down_hbm, sems.at[0])
    down_copy.start()

    def remote(r, k):
        tile_id = ids_ref[r, k]
        _, owner, _ = tile_of(tile_id, tiles_here)
        slot = pltpu.make_async_copy(
            send_ref.at[owner], send_hbm.at[owner, pl.ds(0, tile_rows), :], slot_sems.at[owner]
        )
        return (tile_id >= 0) & (owner != me), owner, slot

    for r in range(tiles_here):
        rows = slice(r * tile_rows, (r + 1) * tile_rows)

        def give_one(k, carry):
            away, owner, slot = remote(r, k)

            @pl.when(away)
            def _():
                send_ref[owner] = mm(adj_ref[r, k], down_ref[rows, :], (0, 0)).astype(jnp.bfloat16)
                slot.start()

            return carry

        lax.fori_loop(0, entries, give_one, 0, unroll=unroll(entries))

    text_ref[...] = mm(pick_ref[...], down_ref[...], (0, 0)) + mm(
        own_ref[...], grad_ref[...], (0, 0)
    )
    row = lax.broadcasted_iota(jnp.int32, (text_rows, half), 0)
    for q in range(shards):
        block = jnp.zeros((text_rows, half), jnp.float32)
        for i in range(texts_here):
            line = text_ref[i * shards + q : i * shards + q + 1, :]
            high = line.astype(jnp.bfloat16).astype(jnp.float32)
            block = jnp.where(row == i, high, block)
            block = jnp.where(row == text_rows // 2 + i, line - high, block)
        rows_ref[q] = block.astype(jnp.bfloat16)
    row_copy = pltpu.make_async_copy(
        rows_ref, send_hbm.at[:, pl.ds(tile_rows, text_rows), :], row_sems.at[0]
    )
    row_copy.start()

    columns = 2 * half
    w_ref[pl.ds(own, half), :] = mm(mine_ref[...], agg_ref[...], (0, 0))
    w_ref[pl.ds(far, half), :] = mm(other_ref[...], agg_ref[...], (0, 0))
    w_ref[columns:, :] = jnp.zeros((w_ref.shape[0] - columns, half), jnp.float32)
    deep = half_ref.shape[1]
    for q in range(shards):
        step = q ^ me
        turned = step * 0
        reach = 1
        while reach < shards:
            turned = 2 * turned + ((step // reach) & 1)
            reach *= 2
        half_ref[turned] = w_ref[q * per : q * per + deep, :].astype(jnp.bfloat16)
    ends = copies(
        [(half_ref.at[pl.ds(kept, kept)], give_hbm), (half_ref.at[pl.ds(0, kept)], keep_hbm)],
        sems.at[pl.ds(1, 2)],
    )

    for r in range(tiles_here):

        def wait_one(k, carry):
            away, _, slot = remote(r, k)

            @pl.when(away)
            def _():
                slot.wait()

            return carry

        lax.fori_loop(0, entries, wait_one, 0)
    down_copy.wait()
    row_copy.wait()
    for copy in ends:
        copy.wait()


def fold_body(mine_ref, theirs_ref, keep_ref, give_ref):
    kept = keep_ref.shape[0]
    for s in range(2 * kept):
        total = mine_ref[s].astype(jnp.float32) + theirs_ref[s].astype(jnp.float32)
        (keep_ref if s < kept else give_ref)[s % kept] = total.astype(jnp.bfloat16)


def close_body(mine_ref, theirs_ref, w_ref):
    w_ref[...] = mine_ref[0].astype(jnp.float32) + theirs_ref[0].astype(jnp.float32)


def local_body(ids_ref, self_ref, down_ref, adj_ref, grad_ref, local_ref):
    tiles_here, entries, _, _ = adj_ref.shape
    me = self_ref[0]
    local_ref[...] = grad_ref[...].astype(jnp.float32)
    for r in range(tiles_here):

        def one(k, carry):
            tile_id = ids_ref[r, k]
            _, owner, place = tile_of(tile_id, tiles_here)

            @pl.when((tile_id >= 0) & (owner == me))
            def _():
                local_ref[place] += mm(adj_ref[r, k], down_ref[r], (0, 0))

            return carry

        lax.fori_loop(0, entries, one, 0, unroll=unroll(entries))


def finish_body(asked_ref, local_hbm, got_ref, node_ref, text_ref, sum_ref, sems):
    local = pltpu.make_async_copy(local_hbm, sum_ref, sems.at[0])
    local.start()
    _, tile_rows, half = sum_ref.shape
    shards, rows, _ = got_ref.shape
    total = jnp.zeros((rows - tile_rows, half), jnp.float32)
    for q in range(shards):
        total = total + got_ref[q, tile_rows:, :].astype(jnp.float32)
    text_ref[...] = (total[: (rows - tile_rows) // 2] + total[(rows - tile_rows) // 2 :])[
        : text_ref.shape[0]
    ]
    local.wait()

    def one(q, carry):
        asked = asked_ref[q]

        @pl.when(asked >= 0)
        def _():
            sum_ref[asked] += got_ref[q, :tile_rows, :].astype(jnp.float32)

        return carry

    lax.fori_loop(0, shards, one, 0)
    node_ref[...] = sum_ref[...].astype(jnp.bfloat16)


def step(
    tokens, token_counts, w_qkv, w_out, w_up, w_down, ln_gains, cache, node_text, adj_tiles,
    adj_values, w_gnn, out_grad
):
    shards = lax.axis_size("graph")
    cores = lax.axis_size("mp")
    me = lax.axis_index("graph").astype(jnp.int32).reshape(1)
    core_at = lax.axis_index("mp")
    core = core_at.astype(jnp.int32).reshape(1)
    texts_here, seq, width = tokens.shape
    nodes_here, half = cache.shape
    tiles_here, entries, tile_rows = adj_values.shape[:3]
    texts = texts_here * shards
    slots = up_to(texts, LANES)
    per = width // shards
    deep = up_to(per, ROWS)
    count = texts_here * seq
    inner = w_up.shape[1]

    def swap(values):
        return lax.ppermute(values, "mp", [(i, cores - 1 - i) for i in range(cores)])

    def toward(values, reach):
        return lax.ppermute(values, "graph", [(i, i ^ reach) for i in range(shards)])

    def spread(values):
        return lax.all_to_all(values, "graph", split_axis=0, concat_axis=0, tiled=True)

    index = call(
        functools.partial(index_body, texts_here),
        [shape((shards, 1, slots + LANES), jnp.int32)],
        [adj_tiles, me, node_text.reshape(tiles_here, tile_rows)],
        [HBM, SMEM, HBM],
        flops=1000,
        scratch=[
            pltpu.SMEM(adj_tiles.shape, jnp.int32),
            pltpu.VMEM((tiles_here, tile_rows), jnp.int32),
            pltpu.SemaphoreType.DMA((2,)),
        ],
    )
    got = spread(index)
    asked = got[:, 0, slots]
    cache_tiles = cache.reshape(tiles_here, tile_rows, half)
    packed = call(
        pack_body,
        [shape((shards, tile_rows, half))],
        [asked, cache_tiles],
        [SMEM, HBM],
        flops=1000,
        scratch=[
            pltpu.VMEM(cache_tiles.shape, jnp.bfloat16),
            pltpu.SemaphoreType.DMA((tiles_here,)),
            pltpu.SemaphoreType.DMA((shards,)),
        ],
        out_specs=[HBM],
    )
    remote = spread(packed)

    w_other = swap(lax.dynamic_slice_in_dim(w_gnn, (1 - core_at) * half, half, 1))

    flat_tokens = tokens.reshape(count, width)
    partial = call(
        functools.partial(attend_body, seq),
        [shape((count, width))],
        [token_counts, flat_tokens, jnp.transpose(w_qkv, (1, 0, 2)), w_out],
        [SMEM, VMEM, VMEM, VMEM],
        flops=2 * count * (width * 3 * half + half * width + 2 * seq * half * 2),
        scratch=[pltpu.VMEM((count, 3 * half), jnp.bfloat16), pltpu.VMEM((count, half), jnp.bfloat16)],
    )
    first, mlp = call(
        inner_body,
        [shape((count, width)), shape((count, width))],
        [flat_tokens, partial, swap(partial), w_up, w_down, ln_gains],
        [VMEM] * 6,
        flops=4 * count * width * inner,
        scratch=[pltpu.VMEM((count, inner), jnp.bfloat16)],
    )
    pooled = call(
        functools.partial(pool_body, seq),
        [shape((1, 1, texts_here * half), jnp.float32)],
        [token_counts, core, first, mlp, swap(mlp), ln_gains],
        [SMEM, SMEM, VMEM, VMEM, VMEM, VMEM],
        flops=20 * count * width,
        scratch=[pltpu.VMEM((8, width), jnp.float32)],
    )
    near = pooled
    reach = 1
    far = toward(near, reach)
    while 4 * reach <= shards:
        reach *= 2
        near = jnp.concatenate([near, far], axis=0)
        far = toward(near, reach)

    kept, pick, own, base = call(
        mask_body,
        [
            shape(adj_values.shape),
            shape((tiles_here, tile_rows, slots)),
            shape((tiles_here, tile_rows, slots)),
            shape(cache_tiles.shape),
        ],
        [adj_tiles, me, got, adj_values, cache_tiles],
        [SMEM, SMEM, VMEM, VMEM, VMEM],
        flops=2 * adj_values.size * slots,
    )
    gathered, pooled = call(
        gather_body,
        [shape((tiles_here, tile_rows, half)), shape((texts, half))],
        [adj_tiles, me, kept, pick, near, far, cache_tiles, remote],
        [HBM, SMEM, HBM, HBM, HBM, HBM, HBM, VMEM],
        flops=2 * adj_values.size * half,
        scratch=[
            pltpu.SMEM(adj_tiles.shape, jnp.int32),
            pltpu.VMEM(kept.shape, jnp.bfloat16),
            pltpu.VMEM(pick.shape, jnp.bfloat16),
            pltpu.VMEM(near.shape, jnp.float32),
            pltpu.VMEM(far.shape, jnp.float32),
            pltpu.VMEM(cache_tiles.shape, jnp.bfloat16),
            pltpu.VMEM((2, entries, tile_rows, half), jnp.bfloat16),
            pltpu.SemaphoreType.DMA((6,)),
        ],
    )
    gathered = gathered.reshape(nodes_here, half)
    node_out, slope = call(
        forward_body,
        [shape((nodes_here, half)), shape((nodes_here, half))],
        [
            core, gathered, swap(gathered), w_gnn, w_other, out_grad,
            own.reshape(nodes_here, slots), base.reshape(nodes_here, half), pooled,
        ],
        [SMEM] + [VMEM] * 8,
        flops=4 * nodes_here * half * half,
    )
    grad_tiles = out_grad.reshape(tiles_here, tile_rows, half)
    slope_other = swap(slope)
    text_rows = up_to(2 * texts_here, 8)
    halves = (shards // 2, deep, half)
    send, keep, give, down = call(
        functools.partial(backward_body, per, texts_here),
        [
            shape((shards, tile_rows + text_rows, half)),
            shape(halves),
            shape(halves),
            shape((nodes_here, half)),
        ],
        [
            adj_tiles, me, core, slope, slope_other, gathered, w_gnn, adj_values,
            pick.reshape(nodes_here, slots), own.reshape(nodes_here, slots), out_grad,
        ],
        [SMEM, SMEM, SMEM] + [VMEM] * 8,
        flops=8 * nodes_here * half * half + 2 * adj_values.size * half,
        scratch=[
            pltpu.VMEM((nodes_here, half), jnp.bfloat16),
            pltpu.VMEM((width + ROWS, half), jnp.float32),
            pltpu.VMEM((slots, half), jnp.float32),
            pltpu.VMEM((shards, tile_rows, half), jnp.bfloat16),
            pltpu.VMEM((shards, text_rows, half), jnp.bfloat16),
            pltpu.VMEM((shards, deep, half), jnp.bfloat16),
            pltpu.SemaphoreType.DMA((3,)),
            pltpu.SemaphoreType.DMA((shards,)),
            pltpu.SemaphoreType.DMA((1,)),
        ],
        out_specs=[HBM] * 4,
    )
    returned = spread(send)
    local = call(
        local_body,
        [shape((tiles_here, tile_rows, half), jnp.float32)],
        [adj_tiles, me, down.reshape(tiles_here, tile_rows, half), adj_values, grad_tiles],
        [SMEM, SMEM] + [VMEM] * 3,
        flops=2 * adj_values.size * half,
    )
    reach = 1
    given = toward(give, reach)
    while 2 * reach < shards:
        part = (shards // (4 * reach), deep, half)
        keep, give = call(
            fold_body,
            [shape(part), shape(part)],
            [keep, given],
            [VMEM] * 2,
            flops=4 * math.prod(part),
        )
        reach *= 2
        given = toward(give, reach)
    w_part = call(
        close_body, [shape((deep, half), jnp.float32)], [keep, given], [VMEM] * 2, flops=1000
    )
    node_grad, text_grad = call(
        finish_body,
        [shape((tiles_here, tile_rows, half)), shape((texts_here, half), jnp.float32)],
        [asked, local, returned],
        [SMEM, HBM, VMEM],
        flops=1000,
        scratch=[
            pltpu.VMEM((tiles_here, tile_rows, half), jnp.float32),
            pltpu.SemaphoreType.DMA((1,)),
        ],
    )
    return (node_out, w_part[:per].T, text_grad, node_grad.reshape(nodes_here, half))


def solution(mesh):
    placed = (
        P("graph", None, None),
        P("graph", None),
        P(None, None, "mp"),
        P("mp", None),
        P(None, "mp"),
        P("mp", None),
        P(),
        P("graph", "mp"),
        P("graph"),
        P("graph", None),
        P("graph", None, None, None),
        P("mp", None),
        P("graph", "mp"),
    )
    return jax.shard_map(
        step,
        mesh=mesh,
        in_specs=placed,
        out_specs=(P("graph", "mp"), P("mp", "graph"), P("graph", "mp"), P("graph", "mp")),
        check_vma=False,
    )
```

```python
import functools
import math

import jax
import jax.numpy as jnp
from jax import lax
from jax.experimental import pallas as pl
from jax.experimental.pallas import tpu as pltpu
from jax.sharding import PartitionSpec as P


HEAD = 64
LANES = 128
ROWS = 16
SPARE = 6 << 20
NORM_EPS = 1e-05
MASKED = -1e30
NO_NODE = -(1 << 20)
ROOT = 0.7978845608028654
CUBE = 0.044715

VMEM = pl.BlockSpec(memory_space=pltpu.VMEM)
HBM = pl.BlockSpec(memory_space=pltpu.HBM)
SMEM = pl.BlockSpec(memory_space=pltpu.SMEM)


def up_to(value, unit):
    return (value + unit - 1) // unit * unit


def call(body, outs, ins, specs, flops, scratch=(), out_specs=None):
    moved = sum(a.size * a.dtype.itemsize for a in ins) + sum(
        o.size * o.dtype.itemsize for o in outs
    )
    many = len(outs) > 1
    ins = [
        pltpu.with_memory_space_constraint(a, pltpu.HBM) if s is HBM else a
        for a, s in zip(ins, specs, strict=True)
    ]
    held = sum(math.prod(s.shape) * jnp.dtype(s.dtype).itemsize for s in scratch if counted(s))
    out_specs = out_specs or [VMEM] * len(outs)
    outs = [
        pltpu.HBM(o.shape, o.dtype) if s is HBM else o for o, s in zip(outs, out_specs, strict=True)
    ]
    return pl.pallas_call(
        body,
        out_shape=tuple(outs) if many else outs[0],
        in_specs=list(specs),
        out_specs=tuple(out_specs) if many else out_specs[0],
        scratch_shapes=list(scratch),
        compiler_params=pltpu.CompilerParams(vmem_limit_bytes=moved + moved // 8 + held + SPARE),
        cost_estimate=pl.CostEstimate(flops=flops, bytes_accessed=moved, transcendentals=0),
    )(*ins)


def counted(scratch):
    return jnp.issubdtype(scratch.dtype, jnp.number)


def copies(pairs, sems):
    started = [pltpu.make_async_copy(a, b, sems.at[i]) for i, (a, b) in enumerate(pairs)]
    for copy in started:
        copy.start()
    return started


def unroll(steps):
    return steps if steps <= 8 else 1


def shape(dims, dtype=jnp.bfloat16):
    return jax.ShapeDtypeStruct(tuple(dims), dtype)


def mm(a, b, dims=(1, 0)):
    return lax.dot_general(
        a, b, (((dims[0],), (dims[1],)), ((), ())), preferred_element_type=jnp.float32
    )


def tile_of(tile_id, tiles_here):
    safe = jnp.maximum(tile_id, 0)
    owner = lax.div(safe, jnp.int32(tiles_here))
    return safe, owner, safe - owner * tiles_here


def side_of(owner, me, peers):
    half = lax.div(owner, jnp.int32(peers))
    mine = lax.div(me, jnp.int32(peers))
    return jnp.where(half == mine, 0, 1), owner - half * peers


def index_body(texts_here, ids_hbm, self_ref, text_hbm, out_ref, ids_ref, text_ref, sems):
    for copy in copies([(ids_hbm, ids_ref), (text_hbm, text_ref)], sems):
        copy.wait()
    tiles_here, entries = ids_ref.shape
    peers, _, lanes = out_ref.shape
    shards = 2 * peers
    width = lanes - 2 * LANES
    texts = texts_here * shards
    me = self_ref[0]
    row = lax.broadcasted_iota(jnp.int32, (peers, LANES), 0)
    near = jnp.full((peers, LANES), -1, jnp.int32)
    far = near
    for r in range(tiles_here):
        for k in range(entries):
            tile_id = ids_ref[r, k]
            _, owner, place = tile_of(tile_id, tiles_here)
            side, spot = side_of(owner, me, peers)
            wanted = (tile_id >= 0) & (owner != me)
            near = jnp.where(row == jnp.where(wanted & (side == 0), spot, -1), place, near)
            far = jnp.where(row == jnp.where(wanted & (side == 1), spot, -1), place, far)
    out_ref[:, :, width : width + LANES] = near.reshape(peers, 1, LANES)
    out_ref[:, :, width + LANES :] = far.reshape(peers, 1, LANES)
    tile_rows = text_ref.shape[1]
    lane = lax.broadcasted_iota(jnp.int32, (LANES, tile_rows), 1)
    sub = lax.broadcasted_iota(jnp.int32, (LANES, LANES), 0)
    diagonal = sub == lax.broadcasted_iota(jnp.int32, (LANES, LANES), 1)
    for c in range(width // LANES):
        slot = c * LANES + lax.broadcasted_iota(jnp.int32, (LANES, 1), 0)
        part = lax.div(slot, jnp.int32(shards))
        text = jnp.where(slot < texts, (slot - part * shards) * texts_here + part, -5)
        best = jnp.full((LANES, tile_rows), NO_NODE, jnp.int32)
        for j in range(tiles_here):
            node = (me * tiles_here + j) * tile_rows + lane
            best = jnp.where(text_ref[j : j + 1, :] == text, node, best)
        column = jnp.max(best.astype(jnp.float32), axis=1, keepdims=True)
        line = jnp.max(jnp.where(diagonal, column, float(NO_NODE)), axis=0, keepdims=True)
        out_ref[:, :, c * LANES : (c + 1) * LANES] = (
            jnp.broadcast_to(line, (peers, LANES)).astype(jnp.int32).reshape(peers, 1, LANES)
        )


def pack_body(asked_ref, cache_hbm, mate_hbm, out_hbm, tile_ref, in_sems, out_sems):
    _, _, tile_rows, _ = tile_ref.shape
    started = copies([(cache_hbm, tile_ref.at[0]), (mate_hbm, tile_ref.at[1])], in_sems)
    peers = out_hbm.shape[0]

    def slot(p, side):
        place = jnp.maximum(asked_ref[p, side], 0)
        target = out_hbm.at[p, pl.ds(side * tile_rows, tile_rows), :]
        return pltpu.make_async_copy(tile_ref.at[side, place], target, out_sems.at[side, p])

    for side in range(2):
        started[side].wait()
        lax.fori_loop(0, peers, lambda p, c: (slot(p, side).start(), c)[1], 0)
    for side in range(2):
        lax.fori_loop(0, peers, lambda p, c: (slot(p, side).wait(), c)[1], 0)


def mask_body(ids_ref, self_ref, got_ref, mate_ref, adj_ref, cache_ref, kept_ref, pick_ref, own_ref, base_ref):
    tiles_here, entries, tile_rows, _ = adj_ref.shape
    peers, _, lanes = got_ref.shape
    width = lanes - 2 * LANES
    me = self_ref[0]
    both = jnp.maximum(got_ref[:, :, :width], mate_ref[:, :, :width])
    table = jnp.max(both.reshape(peers, width).astype(jnp.float32), axis=0, keepdims=True)
    place = lax.broadcasted_iota(jnp.int32, (tile_rows, width), 0).astype(jnp.float32)
    ones = jnp.ones((ROWS, width), jnp.bfloat16)

    def holds(tile_id):
        first = (tile_id * tile_rows).astype(jnp.float32)
        return jnp.where(table - first == place, 1.0, 0.0)

    for r in range(tiles_here):

        def one(k, total):
            tile_id = ids_ref[r, k]
            hot = holds(tile_id).astype(jnp.bfloat16)
            values = adj_ref[r, k]
            taken = mm(ones, hot, (1, 1))[0:1, :]
            keep = jnp.where(tile_id >= 0, 1.0, 0.0) * jnp.where(taken > 0.5, 0.0, 1.0)
            kept_ref[r, k] = (values.astype(jnp.float32) * keep).astype(jnp.bfloat16)
            return total + mm(values, hot)

        pick = lax.fori_loop(
            0, entries, one, jnp.zeros((tile_rows, width), jnp.float32), unroll=unroll(entries)
        )
        pick_ref[r] = pick.astype(jnp.bfloat16)
        hot = holds(me * tiles_here + r)
        own_ref[r] = hot.astype(jnp.bfloat16)
        fresh = jnp.max(hot, axis=1, keepdims=True)
        base_ref[r] = (cache_ref[r].astype(jnp.float32) * (1.0 - fresh)).astype(jnp.bfloat16)


def norm(values, gain):
    average = jnp.mean(values, axis=-1, keepdims=True)
    centred = values - average
    variance = jnp.mean(centred * centred, axis=-1, keepdims=True)
    return centred * lax.rsqrt(variance + NORM_EPS) * gain


def attend_body(seq, counts_ref, tokens_ref, w_qkv_ref, w_out_ref, out_ref, proj_ref, ctx_ref):
    half = w_out_ref.shape[0]
    texts_here = tokens_ref.shape[0] // seq
    for c in range(3):
        proj_ref[:, c * half : (c + 1) * half] = mm(tokens_ref[...], w_qkv_ref[c]).astype(
            jnp.bfloat16
        )
    left = lax.broadcasted_iota(jnp.int32, (seq, LANES), 1) < HEAD
    key_at = lax.broadcasted_iota(jnp.int32, (seq, seq), 1)
    for t in range(texts_here):
        rows = slice(t * seq, (t + 1) * seq)
        live = key_at < counts_ref[0, t]
        for pair in range(half // LANES):
            first = pair * LANES
            query = proj_ref[rows, first : first + LANES].astype(jnp.float32) * (HEAD**-0.5)
            key = proj_ref[rows, half + first : half + first + LANES]
            value = proj_ref[rows, 2 * half + first : 2 * half + first + LANES]
            sides = []
            for side in (left, jnp.logical_not(left)):
                scores = mm(jnp.where(side, query, 0.0).astype(jnp.bfloat16), key, (1, 1))
                scores = jnp.where(live, scores, MASKED)
                powers = jnp.exp(scores - jnp.max(scores, axis=-1, keepdims=True))
                total = jnp.sum(powers, axis=-1, keepdims=True)
                sides.append(mm((powers / total).astype(jnp.bfloat16), value))
            ctx_ref[rows, first : first + LANES] = jnp.where(left, sides[0], sides[1]).astype(
                jnp.bfloat16
            )
    out_ref[...] = mm(ctx_ref[...], w_out_ref[...]).astype(jnp.bfloat16)


def inner_body(tokens_ref, mine_ref, other_ref, up_ref, down_ref, gains_ref, first_ref, out_ref, inner_ref):
    added = mine_ref[...].astype(jnp.float32) + other_ref[...].astype(jnp.float32)
    first = norm(tokens_ref[...].astype(jnp.float32) + added, gains_ref[0:1, :])
    first_ref[...] = first.astype(jnp.bfloat16)
    hidden_units = up_ref.shape[1]
    step = hidden_units // 4
    for c in range(4):
        cols = slice(c * step, (c + 1) * step)
        value = mm(first_ref[...], up_ref[:, cols])
        gate = jnp.tanh(ROOT * (value + CUBE * (value * value * value)))
        inner_ref[:, cols] = (0.5 * value * (1.0 + gate)).astype(jnp.bfloat16)
    out_ref[...] = mm(inner_ref[...], down_ref[...]).astype(jnp.bfloat16)


def pool_body(seq, counts_ref, core_ref, first_ref, mine_ref, other_ref, gains_ref, out_ref, pooled_ref):
    _, _, lanes = out_ref.shape
    texts_here = first_ref.shape[0] // seq
    half = lanes // texts_here
    for t in range(texts_here):
        rows = slice(t * seq, (t + 1) * seq)
        added = mine_ref[rows, :].astype(jnp.float32) + other_ref[rows, :].astype(jnp.float32)
        second = norm(first_ref[rows, :].astype(jnp.float32) + added, gains_ref[1:2, :])
        count = counts_ref[0, t]
        live = lax.broadcasted_iota(jnp.int32, (seq, 1), 0) < count
        total = jnp.sum(jnp.where(live, second, 0.0), axis=0, keepdims=True)
        pooled_ref[...] = jnp.broadcast_to(
            total / count.astype(jnp.float32), pooled_ref.shape
        )
        start = pl.multiple_of(core_ref[0] * half, LANES)
        own = pooled_ref[:, pl.ds(start, half)][0:1, :]
        own = own.astype(jnp.bfloat16).astype(jnp.float32)
        out_ref[:, :, t * half : (t + 1) * half] = own.reshape(1, 1, half)


def pooled_rows(me, near_ref, far_ref, half):
    shards = 2 * near_ref.shape[0]
    parts = []
    for first in range(0, near_ref.shape[2], half):
        for ref in (near_ref, far_ref):
            part = ref[:, :, first : first + half].reshape(shards // 2, half)
            parts.append(part.astype(jnp.bfloat16))
    stacked = jnp.concatenate(parts, axis=0)
    texts = stacked.shape[0]
    row = lax.broadcasted_iota(jnp.int32, (texts, texts), 0)
    column = lax.broadcasted_iota(jnp.int32, (texts, texts), 1)
    order = jnp.where(row == (column ^ me), 1.0, 0.0).astype(jnp.bfloat16)
    return mm(order, stacked).astype(jnp.bfloat16)


def gather_body(
    ids_hbm, self_ref, kept_hbm, pick_hbm, near_hbm, far_hbm, cache_hbm, remote_ref, out_ref,
    pooled_ref, ids_ref, kept_ref, pick_ref, near_ref, far_ref, cache_ref, source_ref, sems
):
    started = copies(
        [
            (near_hbm, near_ref), (far_hbm, far_ref), (ids_hbm, ids_ref), (cache_hbm, cache_ref),
            (pick_hbm, pick_ref), (kept_hbm, kept_ref),
        ],
        sems,
    )
    tiles_here, entries, tile_rows, _ = kept_ref.shape
    half = cache_ref.shape[2]
    me = self_ref[0]
    for copy in started:
        copy.wait()
    pooled = pooled_rows(me, near_ref, far_ref, half)
    pooled_ref[...] = pooled
    texts = pooled.shape[0]

    def fetch(r, k):
        tile_id = ids_ref[r, k]
        _, owner, place = tile_of(tile_id, tiles_here)
        local = (owner == me) | (tile_id < 0)

        @pl.when(local)
        def _():
            source_ref[r % 2, k] = cache_ref[place]

        @pl.when(jnp.logical_not(local))
        def _():
            side, spot = side_of(owner, me, remote_ref.shape[0])
            first = pl.multiple_of(side * tile_rows, tile_rows)
            source_ref[r % 2, k] = remote_ref[spot, pl.ds(first, tile_rows), :]

    for r in range(tiles_here):
        lax.fori_loop(
            0, entries, lambda k, c: (fetch(r, k), c)[1], 0, unroll=unroll(entries)
        )
        total = mm(pick_ref[r][:, :texts], pooled)
        for k in range(entries):
            total = total + mm(kept_ref[r, k], source_ref[r % 2, k])
        out_ref[r] = total.astype(jnp.bfloat16)


def forward_body(core_ref, mine_ref, other_ref, w_own_ref, w_other_ref, grad_ref, own_ref, base_ref, pooled_ref, node_ref, slope_ref):
    _, half = mine_ref.shape
    start = pl.multiple_of(core_ref[0] * half, LANES)
    hidden = mm(mine_ref[...], w_own_ref[:, pl.ds(start, half)]) + mm(
        other_ref[...], w_other_ref[...]
    )
    square = hidden * hidden
    gate = jnp.tanh(ROOT * hidden * (1.0 + CUBE * square))
    lifted = 0.5 * (1.0 + gate)
    slope = lifted + 0.5 * hidden * (1.0 - gate * gate) * (ROOT * (1.0 + 3.0 * CUBE * square))
    slope_ref[...] = (grad_ref[...].astype(jnp.float32) * slope).astype(jnp.bfloat16)
    fresh = mm(own_ref[:, : pooled_ref.shape[0]], pooled_ref[...])
    node_ref[...] = (base_ref[...].astype(jnp.float32) + fresh + hidden * lifted).astype(
        jnp.bfloat16
    )


def weight_body(
    per, self_ref, core_ref, mine_ref, other_ref, agg_ref, keep_hbm, give_hbm, w_ref, half_ref, sems
):
    shards, deep, half = half_ref.shape
    kept = shards // 2
    me = self_ref[0]
    own = pl.multiple_of(core_ref[0] * half, LANES)
    far = pl.multiple_of((1 - core_ref[0]) * half, LANES)
    columns = 2 * half
    w_ref[pl.ds(own, half), :] = mm(mine_ref[...], agg_ref[...], (0, 0))
    w_ref[pl.ds(far, half), :] = mm(other_ref[...], agg_ref[...], (0, 0))
    w_ref[columns:, :] = jnp.zeros((w_ref.shape[0] - columns, half), jnp.float32)
    for q in range(shards):
        step = q ^ me
        turned = step * 0
        reach = 1
        while reach < shards:
            turned = 2 * turned + ((step // reach) & 1)
            reach *= 2
        half_ref[turned] = w_ref[q * per : q * per + deep, :].astype(jnp.bfloat16)
    ends = copies(
        [(half_ref.at[pl.ds(kept, kept)], give_hbm), (half_ref.at[pl.ds(0, kept)], keep_hbm)], sems
    )
    for copy in ends:
        copy.wait()


def backward_body(
    texts_here, ids_ref, self_ref, core_ref, mine_ref, other_ref, w_own_ref, adj_ref,
    pick_ref, own_ref, grad_ref, send_hbm, down_hbm,
    down_ref, text_ref, send_ref, rows_ref, sems, slot_sems
):
    tiles_here, entries, tile_rows, _ = adj_ref.shape
    shards, text_rows, half = rows_ref.shape
    me = self_ref[0]
    core = core_ref[0]
    own = pl.multiple_of(core * half, LANES)
    far = pl.multiple_of((1 - core) * half, LANES)
    down = mm(mine_ref[...], w_own_ref[:, pl.ds(own, half)], (1, 1)) + mm(
        other_ref[...], w_own_ref[:, pl.ds(far, half)], (1, 1)
    )
    down_ref[...] = down.astype(jnp.bfloat16)
    down_copy = pltpu.make_async_copy(down_ref, down_hbm, sems.at[0])
    down_copy.start()
    for r in range(tiles_here):
        rows = slice(r * tile_rows, (r + 1) * tile_rows)
        for first in range(0, entries, 6):
            group = range(first, min(first + 6, entries))
            side_by_side = jnp.concatenate([adj_ref[r, k] for k in group], axis=1)
            product = mm(side_by_side, down_ref[rows, :], (0, 0)).astype(jnp.bfloat16)
            for k in group:
                tile_id = ids_ref[r, k]
                _, owner, _ = tile_of(tile_id, tiles_here)
                slot = jnp.where((tile_id >= 0) & (owner != me), owner, shards)
                send_ref[slot] = product[(k - first) * tile_rows : (k - first + 1) * tile_rows]
    slots = copies(
        [(send_ref.at[q], send_hbm.at[q, pl.ds(0, tile_rows), :]) for q in range(shards)], slot_sems
    )
    text_ref[...] = mm(pick_ref[...], down_ref[...], (0, 0)) + mm(
        own_ref[...], grad_ref[...], (0, 0)
    )
    row = lax.broadcasted_iota(jnp.int32, (text_rows, half), 0)
    for q in range(shards):
        block = jnp.zeros((text_rows, half), jnp.float32)
        for i in range(texts_here):
            line = text_ref[i * shards + q : i * shards + q + 1, :]
            high = line.astype(jnp.bfloat16).astype(jnp.float32)
            block = jnp.where(row == i, high, block)
            block = jnp.where(row == text_rows // 2 + i, line - high, block)
        rows_ref[q] = block.astype(jnp.bfloat16)
    row_copy = pltpu.make_async_copy(
        rows_ref, send_hbm.at[:, pl.ds(tile_rows, text_rows), :], sems.at[1]
    )
    row_copy.start()
    for copy in slots:
        copy.wait()
    down_copy.wait()
    row_copy.wait()


def fold_body(mine_ref, theirs_ref, keep_ref, give_ref):
    kept = keep_ref.shape[0]
    for s in range(2 * kept):
        total = mine_ref[s].astype(jnp.float32) + theirs_ref[s].astype(jnp.float32)
        (keep_ref if s < kept else give_ref)[s % kept] = total.astype(jnp.bfloat16)


def close_body(mine_ref, theirs_ref, w_ref):
    w_ref[...] = mine_ref[0].astype(jnp.float32) + theirs_ref[0].astype(jnp.float32)


def local_body(ids_ref, self_ref, down_ref, adj_ref, grad_ref, local_ref):
    tiles_here, entries, _, _ = adj_ref.shape
    me = self_ref[0]
    local_ref[...] = grad_ref[...].astype(jnp.float32)
    for r in range(tiles_here):

        def one(k, carry):
            tile_id = ids_ref[r, k]
            _, owner, place = tile_of(tile_id, tiles_here)

            @pl.when((tile_id >= 0) & (owner == me))
            def _():
                local_ref[place] += mm(adj_ref[r, k], down_ref[r], (0, 0))

            return carry

        lax.fori_loop(0, entries, one, 0, unroll=unroll(entries))


def finish_body(
    self_ref, asked_ref, mate_ref, local_hbm, got_ref, node_ref, text_ref, sum_ref, sems
):
    local = pltpu.make_async_copy(local_hbm, sum_ref, sems.at[0])
    local.start()
    _, tile_rows, half = sum_ref.shape
    shards, rows, _ = got_ref.shape
    total = jnp.zeros((rows - tile_rows, half), jnp.float32)
    for q in range(shards):
        total = total + got_ref[q, tile_rows:, :].astype(jnp.float32)
    text_ref[...] = (total[: (rows - tile_rows) // 2] + total[(rows - tile_rows) // 2 :])[
        : text_ref.shape[0]
    ]
    local.wait()

    me = self_ref[0]

    def one(q, carry):
        side, spot = side_of(q, me, shards // 2)
        asked = jnp.where(side == 0, asked_ref[spot, 0], mate_ref[spot, 1])

        @pl.when(asked >= 0)
        def _():
            sum_ref[asked] += got_ref[q, :tile_rows, :].astype(jnp.float32)

        return carry

    lax.fori_loop(0, shards, one, 0)
    node_ref[...] = sum_ref[...].astype(jnp.bfloat16)


def step(
    tokens, token_counts, w_qkv, w_out, w_up, w_down, ln_gains, cache, node_text, adj_tiles,
    adj_values, w_gnn, out_grad
):
    shards = lax.axis_size("graph")
    cores = lax.axis_size("mp")
    me = lax.axis_index("graph").astype(jnp.int32).reshape(1)
    core_at = lax.axis_index("mp")
    core = core_at.astype(jnp.int32).reshape(1)
    texts_here, seq, width = tokens.shape
    nodes_here, half = cache.shape
    tiles_here, entries, tile_rows = adj_values.shape[:3]
    texts = texts_here * shards
    slots = up_to(texts, LANES)
    per = width // shards
    deep = up_to(per, ROWS)
    count = texts_here * seq
    inner = w_up.shape[1]

    def swap(values):
        return lax.ppermute(values, "mp", [(i, cores - 1 - i) for i in range(cores)])

    def toward(values, reach):
        return lax.ppermute(values, "graph", [(i, i ^ reach) for i in range(shards)])

    peers = shards // 2

    def spread(values, groups=None):
        return lax.all_to_all(
            values, "graph", split_axis=0, concat_axis=0, tiled=True, axis_index_groups=groups
        )

    halves_of = [list(range(peers)), list(range(peers, shards))]

    cache_tiles = cache.reshape(tiles_here, tile_rows, half)
    mate_tiles = toward(cache_tiles, peers)
    index = call(
        functools.partial(index_body, texts_here),
        [shape((peers, 1, slots + 2 * LANES), jnp.int32)],
        [adj_tiles, me, node_text.reshape(tiles_here, tile_rows)],
        [HBM, SMEM, HBM],
        flops=1000,
        scratch=[
            pltpu.SMEM(adj_tiles.shape, jnp.int32),
            pltpu.VMEM((tiles_here, tile_rows), jnp.int32),
            pltpu.SemaphoreType.DMA((2,)),
        ],
    )
    got = spread(index, halves_of)
    mate_got = toward(got, peers)

    def places(table):
        return table[:, 0, slots:].reshape(peers, 2, LANES)[:, :, 0]

    asked = places(got)
    packed = call(
        pack_body,
        [shape((peers, 2 * tile_rows, half))],
        [asked, cache_tiles, mate_tiles],
        [SMEM, HBM, HBM],
        flops=1000,
        scratch=[
            pltpu.VMEM((2,) + cache_tiles.shape, jnp.bfloat16),
            pltpu.SemaphoreType.DMA((2,)),
            pltpu.SemaphoreType.DMA((2, peers)),
        ],
        out_specs=[HBM],
    )
    remote = spread(packed, halves_of)

    w_other = swap(lax.dynamic_slice_in_dim(w_gnn, (1 - core_at) * half, half, 1))

    flat_tokens = tokens.reshape(count, width)
    partial = call(
        functools.partial(attend_body, seq),
        [shape((count, width))],
        [token_counts, flat_tokens, jnp.transpose(w_qkv, (1, 0, 2)), w_out],
        [SMEM, VMEM, VMEM, VMEM],
        flops=2 * count * (width * 3 * half + half * width + 2 * seq * half * 2),
        scratch=[pltpu.VMEM((count, 3 * half), jnp.bfloat16), pltpu.VMEM((count, half), jnp.bfloat16)],
    )
    first, mlp = call(
        inner_body,
        [shape((count, width)), shape((count, width))],
        [flat_tokens, partial, swap(partial), w_up, w_down, ln_gains],
        [VMEM] * 6,
        flops=4 * count * width * inner,
        scratch=[pltpu.VMEM((count, inner), jnp.bfloat16)],
    )
    pooled = call(
        functools.partial(pool_body, seq),
        [shape((1, 1, texts_here * half), jnp.float32)],
        [token_counts, core, first, mlp, swap(mlp), ln_gains],
        [SMEM, SMEM, VMEM, VMEM, VMEM, VMEM],
        flops=20 * count * width,
        scratch=[pltpu.VMEM((8, width), jnp.float32)],
    )
    near = pooled
    reach = 1
    far = toward(near, reach)
    while 4 * reach <= shards:
        reach *= 2
        near = jnp.concatenate([near, far], axis=0)
        far = toward(near, reach)

    kept, pick, own, base = call(
        mask_body,
        [
            shape(adj_values.shape),
            shape((tiles_here, tile_rows, slots)),
            shape((tiles_here, tile_rows, slots)),
            shape(cache_tiles.shape),
        ],
        [adj_tiles, me, got, mate_got, adj_values, cache_tiles],
        [SMEM, SMEM, VMEM, VMEM, VMEM, VMEM],
        flops=2 * adj_values.size * slots,
    )
    gathered, pooled = call(
        gather_body,
        [shape((tiles_here, tile_rows, half)), shape((texts, half))],
        [adj_tiles, me, kept, pick, near, far, cache_tiles, remote],
        [HBM, SMEM, HBM, HBM, HBM, HBM, HBM, VMEM],
        flops=2 * adj_values.size * half,
        scratch=[
            pltpu.SMEM(adj_tiles.shape, jnp.int32),
            pltpu.VMEM(kept.shape, jnp.bfloat16),
            pltpu.VMEM(pick.shape, jnp.bfloat16),
            pltpu.VMEM(near.shape, jnp.float32),
            pltpu.VMEM(far.shape, jnp.float32),
            pltpu.VMEM(cache_tiles.shape, jnp.bfloat16),
            pltpu.VMEM((2, entries, tile_rows, half), jnp.bfloat16),
            pltpu.SemaphoreType.DMA((6,)),
        ],
    )
    gathered = gathered.reshape(nodes_here, half)
    node_out, slope = call(
        forward_body,
        [shape((nodes_here, half)), shape((nodes_here, half))],
        [
            core, gathered, swap(gathered), w_gnn, w_other, out_grad,
            own.reshape(nodes_here, slots), base.reshape(nodes_here, half), pooled,
        ],
        [SMEM] + [VMEM] * 8,
        flops=4 * nodes_here * half * half,
    )
    grad_tiles = out_grad.reshape(tiles_here, tile_rows, half)
    slope_other = swap(slope)
    text_rows = up_to(2 * texts_here, 8)
    halves = (shards // 2, deep, half)
    keep, give = call(
        functools.partial(weight_body, per),
        [shape(halves), shape(halves)],
        [me, core, slope, slope_other, gathered],
        [SMEM, SMEM] + [VMEM] * 3,
        flops=4 * nodes_here * half * half,
        scratch=[
            pltpu.VMEM((width + ROWS, half), jnp.float32),
            pltpu.VMEM((shards, deep, half), jnp.bfloat16),
            pltpu.SemaphoreType.DMA((2,)),
        ],
        out_specs=[HBM] * 2,
    )
    given = toward(give, 1)
    send, down = call(
        functools.partial(backward_body, texts_here),
        [shape((shards, tile_rows + text_rows, half)), shape((nodes_here, half))],
        [
            adj_tiles, me, core, slope, slope_other, w_gnn, adj_values,
            pick.reshape(nodes_here, slots), own.reshape(nodes_here, slots), out_grad,
        ],
        [SMEM, SMEM, SMEM] + [VMEM] * 7,
        flops=4 * nodes_here * half * half + 2 * adj_values.size * half,
        scratch=[
            pltpu.VMEM((nodes_here, half), jnp.bfloat16),
            pltpu.VMEM((slots, half), jnp.float32),
            pltpu.VMEM((shards + 1, tile_rows, half), jnp.bfloat16),
            pltpu.VMEM((shards, text_rows, half), jnp.bfloat16),
            pltpu.SemaphoreType.DMA((2,)),
            pltpu.SemaphoreType.DMA((shards,)),
        ],
        out_specs=[HBM] * 2,
    )
    returned = spread(send)
    local = call(
        local_body,
        [shape((tiles_here, tile_rows, half), jnp.float32)],
        [adj_tiles, me, down.reshape(tiles_here, tile_rows, half), adj_values, grad_tiles],
        [SMEM, SMEM] + [VMEM] * 3,
        flops=2 * adj_values.size * half,
    )
    reach = 1
    while 2 * reach < shards:
        part = (shards // (4 * reach), deep, half)
        keep, give = call(
            fold_body,
            [shape(part), shape(part)],
            [keep, given],
            [VMEM] * 2,
            flops=4 * math.prod(part),
        )
        reach *= 2
        given = toward(give, reach)
    w_part = call(
        close_body, [shape((deep, half), jnp.float32)], [keep, given], [VMEM] * 2, flops=1000
    )
    node_grad, text_grad = call(
        finish_body,
        [shape((tiles_here, tile_rows, half)), shape((texts_here, half), jnp.float32)],
        [me, asked, places(mate_got), local, returned],
        [SMEM, SMEM, SMEM, HBM, VMEM],
        flops=1000,
        scratch=[
            pltpu.VMEM((tiles_here, tile_rows, half), jnp.float32),
            pltpu.SemaphoreType.DMA((1,)),
        ],
    )
    return (node_out, w_part[:per].T, text_grad, node_grad.reshape(nodes_here, half))


def solution(mesh):
    placed = (
        P("graph", None, None),
        P("graph", None),
        P(None, None, "mp"),
        P("mp", None),
        P(None, "mp"),
        P("mp", None),
        P(),
        P("graph", "mp"),
        P("graph"),
        P("graph", None),
        P("graph", None, None, None),
        P("mp", None),
        P("graph", "mp"),
    )
    return jax.shard_map(
        step,
        mesh=mesh,
        in_specs=placed,
        out_specs=(P("graph", "mp"), P("mp", "graph"), P("graph", "mp"), P("graph", "mp")),
        check_vma=False,
    )
```

```python
import functools
import math

import jax
import jax.numpy as jnp
from jax import lax
from jax.experimental import pallas as pl
from jax.experimental.pallas import tpu as pltpu
from jax.sharding import PartitionSpec as P


HEAD = 64
LANES = 128
ROWS = 16
SPARE = 6 << 20
NORM_EPS = 1e-05
MASKED = -1e30
NO_NODE = -(1 << 20)
ROOT = 0.7978845608028654
CUBE = 0.044715

VMEM = pl.BlockSpec(memory_space=pltpu.VMEM)
HBM = pl.BlockSpec(memory_space=pltpu.HBM)
PULL = pl.BlockSpec(memory_space=pltpu.HBM)
SMEM = pl.BlockSpec(memory_space=pltpu.SMEM)


def up_to(value, unit):
    return (value + unit - 1) // unit * unit


def call(body, outs, ins, specs, flops, scratch=(), out_specs=None):
    moved = sum(a.size * a.dtype.itemsize for a in ins) + sum(
        o.size * o.dtype.itemsize for o in outs
    )
    many = len(outs) > 1
    ins = [
        pltpu.with_memory_space_constraint(a, pltpu.HBM) if s is HBM or s is PULL else a
        for a, s in zip(ins, specs, strict=True)
    ]
    pulled = [i for i, s in enumerate(specs) if s is PULL]
    if pulled:
        body = pulling(body, pulled)
        scratch = list(scratch) + [pltpu.VMEM(ins[i].shape, ins[i].dtype) for i in pulled]
        scratch.append(pltpu.SemaphoreType.DMA((len(pulled),)))
    held = sum(math.prod(s.shape) * jnp.dtype(s.dtype).itemsize for s in scratch if counted(s))
    out_specs = out_specs or [VMEM] * len(outs)
    outs = [
        pltpu.HBM(o.shape, o.dtype) if s is HBM else o for o, s in zip(outs, out_specs, strict=True)
    ]
    return pl.pallas_call(
        body,
        out_shape=tuple(outs) if many else outs[0],
        in_specs=list(specs),
        out_specs=tuple(out_specs) if many else out_specs[0],
        scratch_shapes=list(scratch),
        compiler_params=pltpu.CompilerParams(vmem_limit_bytes=moved + moved // 8 + held + SPARE),
        cost_estimate=pl.CostEstimate(flops=flops, bytes_accessed=moved, transcendentals=0),
    )(*ins)


def counted(scratch):
    return jnp.issubdtype(scratch.dtype, jnp.number)


def copies(pairs, sems):
    started = [pltpu.make_async_copy(a, b, sems.at[i]) for i, (a, b) in enumerate(pairs)]
    for copy in started:
        copy.start()
    return started


def pulling(body, pulled):
    def wrapped(*refs):
        buffers, sems = refs[-len(pulled) - 1 : -1], refs[-1]
        held = list(refs[: -len(pulled) - 1])
        started = copies([(held[i], b) for i, b in zip(pulled, buffers)], sems)
        for i, buffer in zip(pulled, buffers):
            held[i] = buffer
        for copy in started:
            copy.wait()
        body(*held)

    return wrapped


def unroll(steps):
    return steps if steps <= 8 else 1


def shape(dims, dtype=jnp.bfloat16):
    return jax.ShapeDtypeStruct(tuple(dims), dtype)


def mm(a, b, dims=(1, 0)):
    return lax.dot_general(
        a, b, (((dims[0],), (dims[1],)), ((), ())), preferred_element_type=jnp.float32
    )


def tile_of(tile_id, tiles_here):
    safe = jnp.maximum(tile_id, 0)
    owner = lax.div(safe, jnp.int32(tiles_here))
    return safe, owner, safe - owner * tiles_here


def side_of(owner, me, peers):
    half = lax.div(owner, jnp.int32(peers))
    mine = lax.div(me, jnp.int32(peers))
    return jnp.where(half == mine, 0, 1), owner - half * peers


def index_body(texts_here, ids_hbm, self_ref, text_hbm, out_ref, ids_ref, text_ref, sems):
    for copy in copies([(ids_hbm, ids_ref), (text_hbm, text_ref)], sems):
        copy.wait()
    tiles_here, entries = ids_ref.shape
    peers, _, lanes = out_ref.shape
    shards = 2 * peers
    width = lanes - 2 * LANES
    texts = texts_here * shards
    me = self_ref[0]
    row = lax.broadcasted_iota(jnp.int32, (peers, LANES), 0)
    near = jnp.full((peers, LANES), -1, jnp.int32)
    far = near
    for r in range(tiles_here):
        for k in range(entries):
            tile_id = ids_ref[r, k]
            _, owner, place = tile_of(tile_id, tiles_here)
            side, spot = side_of(owner, me, peers)
            wanted = (tile_id >= 0) & (owner != me)
            near = jnp.where(row == jnp.where(wanted & (side == 0), spot, -1), place, near)
            far = jnp.where(row == jnp.where(wanted & (side == 1), spot, -1), place, far)
    out_ref[:, :, width : width + LANES] = near.reshape(peers, 1, LANES)
    out_ref[:, :, width + LANES :] = far.reshape(peers, 1, LANES)
    tile_rows = text_ref.shape[1]
    lane = lax.broadcasted_iota(jnp.int32, (LANES, tile_rows), 1)
    sub = lax.broadcasted_iota(jnp.int32, (LANES, LANES), 0)
    diagonal = sub == lax.broadcasted_iota(jnp.int32, (LANES, LANES), 1)
    for c in range(width // LANES):
        slot = c * LANES + lax.broadcasted_iota(jnp.int32, (LANES, 1), 0)
        part = lax.div(slot, jnp.int32(shards))
        text = jnp.where(slot < texts, (slot - part * shards) * texts_here + part, -5)
        best = jnp.full((LANES, tile_rows), NO_NODE, jnp.int32)
        for j in range(tiles_here):
            node = (me * tiles_here + j) * tile_rows + lane
            best = jnp.where(text_ref[j : j + 1, :] == text, node, best)
        column = jnp.max(best.astype(jnp.float32), axis=1, keepdims=True)
        line = jnp.max(jnp.where(diagonal, column, float(NO_NODE)), axis=0, keepdims=True)
        out_ref[:, :, c * LANES : (c + 1) * LANES] = (
            jnp.broadcast_to(line, (peers, LANES)).astype(jnp.int32).reshape(peers, 1, LANES)
        )


def pack_body(asked_ref, cache_hbm, mate_hbm, out_hbm, tile_ref, in_sems, out_sems):
    _, _, tile_rows, _ = tile_ref.shape
    started = copies([(cache_hbm, tile_ref.at[0]), (mate_hbm, tile_ref.at[1])], in_sems)
    peers = out_hbm.shape[0]

    def slot(p, side):
        place = jnp.maximum(asked_ref[p, side], 0)
        target = out_hbm.at[p, pl.ds(side * tile_rows, tile_rows), :]
        return pltpu.make_async_copy(tile_ref.at[side, place], target, out_sems.at[side, p])

    for side in range(2):
        started[side].wait()
        lax.fori_loop(0, peers, lambda p, c: (slot(p, side).start(), c)[1], 0)
    for side in range(2):
        lax.fori_loop(0, peers, lambda p, c: (slot(p, side).wait(), c)[1], 0)


def mask_body(
    ids_ref, self_ref, got_ref, mate_ref, adj_ref, cache_ref, *refs
):
    outs, (kept_ref, pick_ref, own_ref, base_ref, sems) = refs[:4], refs[4:]
    tiles_here, entries, tile_rows, _ = adj_ref.shape
    peers, _, lanes = got_ref.shape
    width = lanes - 2 * LANES
    me = self_ref[0]
    both = jnp.maximum(got_ref[:, :, :width], mate_ref[:, :, :width])
    table = jnp.max(both.reshape(peers, width).astype(jnp.float32), axis=0, keepdims=True)
    place = lax.broadcasted_iota(jnp.int32, (tile_rows, width), 0).astype(jnp.float32)
    ones = jnp.ones((ROWS, width), jnp.bfloat16)
    sent = []

    def holds(tile_id):
        first = (tile_id * tile_rows).astype(jnp.float32)
        return jnp.where(table - first == place, 1.0, 0.0)

    for r in range(tiles_here):

        def one(k, total):
            tile_id = ids_ref[r, k]
            hot = holds(tile_id).astype(jnp.bfloat16)
            values = adj_ref[r, k]
            taken = mm(ones, hot, (1, 1))[0:1, :]
            keep = jnp.where(tile_id >= 0, 1.0, 0.0) * jnp.where(taken > 0.5, 0.0, 1.0)
            kept_ref[r, k] = (values.astype(jnp.float32) * keep).astype(jnp.bfloat16)
            return total + mm(values, hot)

        pick = lax.fori_loop(
            0, entries, one, jnp.zeros((tile_rows, width), jnp.float32), unroll=unroll(entries)
        )
        pick_ref[r] = pick.astype(jnp.bfloat16)
        hot = holds(me * tiles_here + r)
        own_ref[r] = hot.astype(jnp.bfloat16)
        fresh = jnp.max(hot, axis=1, keepdims=True)
        base_ref[r] = (cache_ref[r].astype(jnp.float32) * (1.0 - fresh)).astype(jnp.bfloat16)
        row = [(ref.at[r], out.at[r]) for ref, out in zip((kept_ref, pick_ref, own_ref, base_ref), outs)]
        sent = sent + copies(row, sems.at[r])
    for copy in sent:
        copy.wait()


def norm(values, gain):
    average = jnp.mean(values, axis=-1, keepdims=True)
    centred = values - average
    variance = jnp.mean(centred * centred, axis=-1, keepdims=True)
    return centred * lax.rsqrt(variance + NORM_EPS) * gain


def attend_body(
    seq, counts_ref, tokens_hbm, w_qkv_hbm, w_out_hbm, out_hbm,
    tokens_ref, w_qkv_ref, w_out_ref, out_ref, proj_ref, ctx_ref, in_sems, out_sems
):
    half = w_out_ref.shape[0]
    texts_here = tokens_ref.shape[0] // seq
    started = copies(
        [(tokens_hbm, tokens_ref)]
        + [(w_qkv_hbm.at[c], w_qkv_ref.at[c]) for c in range(3)]
        + [(w_out_hbm, w_out_ref)],
        in_sems,
    )
    started[0].wait()
    for c in range(3):
        started[1 + c].wait()
        proj_ref[:, c * half : (c + 1) * half] = mm(tokens_ref[...], w_qkv_ref[c]).astype(
            jnp.bfloat16
        )
    started[4].wait()
    sent = []
    left = lax.broadcasted_iota(jnp.int32, (seq, LANES), 1) < HEAD
    key_at = lax.broadcasted_iota(jnp.int32, (seq, seq), 1)
    for t in range(texts_here):
        rows = pl.ds(t * seq, seq)
        live = key_at < counts_ref[0, t]
        for pair in range(half // LANES):
            first = pair * LANES
            query = proj_ref[rows, first : first + LANES].astype(jnp.float32) * (HEAD**-0.5)
            key = proj_ref[rows, half + first : half + first + LANES]
            value = proj_ref[rows, 2 * half + first : 2 * half + first + LANES]
            sides = []
            for side in (left, jnp.logical_not(left)):
                scores = mm(jnp.where(side, query, 0.0).astype(jnp.bfloat16), key, (1, 1))
                scores = jnp.where(live, scores, MASKED)
                powers = jnp.exp(scores - jnp.max(scores, axis=-1, keepdims=True))
                total = jnp.sum(powers, axis=-1, keepdims=True)
                sides.append(mm((powers / total).astype(jnp.bfloat16), value))
            ctx_ref[rows, first : first + LANES] = jnp.where(left, sides[0], sides[1]).astype(
                jnp.bfloat16
            )
        out_ref[rows, :] = mm(ctx_ref[rows, :], w_out_ref[...]).astype(jnp.bfloat16)
        sent.append(pltpu.make_async_copy(out_ref.at[rows, :], out_hbm.at[rows, :], out_sems.at[t]))
        sent[-1].start()
    for copy in sent:
        copy.wait()


def inner_body(
    tokens_hbm, mine_hbm, other_hbm, up_hbm, down_hbm, gains_ref, first_ref, out_ref,
    inner_ref, tokens_ref, mine_ref, other_ref, up_ref, down_ref, sems
):
    started = copies(
        [
            (tokens_hbm, tokens_ref), (mine_hbm, mine_ref), (other_hbm, other_ref),
            (up_hbm, up_ref), (down_hbm, down_ref),
        ],
        sems,
    )
    for copy in started[:3]:
        copy.wait()
    added = mine_ref[...].astype(jnp.float32) + other_ref[...].astype(jnp.float32)
    first = norm(tokens_ref[...].astype(jnp.float32) + added, gains_ref[0:1, :])
    first_ref[...] = first.astype(jnp.bfloat16)
    started[3].wait()
    hidden_units = up_ref.shape[1]
    step = hidden_units // 4
    for c in range(4):
        cols = slice(c * step, (c + 1) * step)
        value = mm(first_ref[...], up_ref[:, cols])
        gate = jnp.tanh(ROOT * (value + CUBE * (value * value * value)))
        inner_ref[:, cols] = (0.5 * value * (1.0 + gate)).astype(jnp.bfloat16)
    started[4].wait()
    out_ref[...] = mm(inner_ref[...], down_ref[...]).astype(jnp.bfloat16)


def pool_body(seq, counts_ref, core_ref, first_ref, mine_ref, other_ref, gains_ref, out_ref, pooled_ref):
    _, _, lanes = out_ref.shape
    texts_here = first_ref.shape[0] // seq
    half = lanes // texts_here
    for t in range(texts_here):
        rows = slice(t * seq, (t + 1) * seq)
        added = mine_ref[rows, :].astype(jnp.float32) + other_ref[rows, :].astype(jnp.float32)
        second = norm(first_ref[rows, :].astype(jnp.float32) + added, gains_ref[1:2, :])
        count = counts_ref[0, t]
        live = lax.broadcasted_iota(jnp.int32, (seq, 1), 0) < count
        total = jnp.sum(jnp.where(live, second, 0.0), axis=0, keepdims=True)
        pooled_ref[...] = jnp.broadcast_to(
            total / count.astype(jnp.float32), pooled_ref.shape
        )
        start = pl.multiple_of(core_ref[0] * half, LANES)
        own = pooled_ref[:, pl.ds(start, half)][0:1, :]
        own = own.astype(jnp.bfloat16).astype(jnp.float32)
        out_ref[:, :, t * half : (t + 1) * half] = own.reshape(1, 1, half)


def pooled_rows(me, near_ref, far_ref, half):
    shards = 2 * near_ref.shape[0]
    parts = []
    for first in range(0, near_ref.shape[2], half):
        for ref in (near_ref, far_ref):
            part = ref[:, :, first : first + half].reshape(shards // 2, half)
            parts.append(part.astype(jnp.bfloat16))
    stacked = jnp.concatenate(parts, axis=0)
    texts = stacked.shape[0]
    row = lax.broadcasted_iota(jnp.int32, (texts, texts), 0)
    column = lax.broadcasted_iota(jnp.int32, (texts, texts), 1)
    place = column & (shards - 1)
    offset = jnp.zeros_like(place)
    reach = 1
    while reach < shards:
        offset = 2 * offset + (place & 1)
        place = lax.shift_right_logical(place, 1)
        reach *= 2
    source = column - (column & (shards - 1)) + (offset ^ me)
    order = jnp.where(row == source, 1.0, 0.0).astype(jnp.bfloat16)
    return mm(order, stacked).astype(jnp.bfloat16)


def gather_body(
    ids_hbm, self_ref, kept_hbm, pick_hbm, near_hbm, far_hbm, cache_hbm, remote_ref, out_ref,
    pooled_ref, ids_ref, kept_ref, pick_ref, near_ref, far_ref, cache_ref, source_ref, sems
):
    started = copies(
        [
            (near_hbm, near_ref), (far_hbm, far_ref), (ids_hbm, ids_ref), (cache_hbm, cache_ref),
            (pick_hbm, pick_ref), (kept_hbm, kept_ref),
        ],
        sems,
    )
    tiles_here, entries, tile_rows, _ = kept_ref.shape
    half = cache_ref.shape[2]
    me = self_ref[0]
    for copy in started:
        copy.wait()
    pooled = pooled_rows(me, near_ref, far_ref, half)
    pooled_ref[...] = pooled
    texts = pooled.shape[0]

    def fetch(r, k):
        tile_id = ids_ref[r, k]
        _, owner, place = tile_of(tile_id, tiles_here)
        local = (owner == me) | (tile_id < 0)

        @pl.when(local)
        def _():
            source_ref[r % 2, k] = cache_ref[place]

        @pl.when(jnp.logical_not(local))
        def _():
            side, spot = side_of(owner, me, remote_ref.shape[0])
            first = pl.multiple_of(side * tile_rows, tile_rows)
            source_ref[r % 2, k] = remote_ref[spot, pl.ds(first, tile_rows), :]

    for r in range(tiles_here):
        lax.fori_loop(
            0, entries, lambda k, c: (fetch(r, k), c)[1], 0, unroll=unroll(entries)
        )
        total = mm(pick_ref[r][:, :texts], pooled)
        for k in range(entries):
            total = total + mm(kept_ref[r, k], source_ref[r % 2, k])
        out_ref[r] = total.astype(jnp.bfloat16)


def forward_body(core_ref, mine_ref, other_ref, w_own_ref, w_other_ref, grad_ref, own_ref, base_ref, pooled_ref, node_ref, slope_ref):
    _, half = mine_ref.shape
    start = pl.multiple_of(core_ref[0] * half, LANES)
    hidden = mm(mine_ref[...], w_own_ref[:, pl.ds(start, half)]) + mm(
        other_ref[...], w_other_ref[:, pl.ds(start, half)]
    )
    square = hidden * hidden
    gate = jnp.tanh(ROOT * hidden * (1.0 + CUBE * square))
    lifted = 0.5 * (1.0 + gate)
    slope = lifted + 0.5 * hidden * (1.0 - gate * gate) * (ROOT * (1.0 + 3.0 * CUBE * square))
    slope_ref[...] = (grad_ref[...].astype(jnp.float32) * slope).astype(jnp.bfloat16)
    fresh = mm(own_ref[:, : pooled_ref.shape[0]], pooled_ref[...])
    node_ref[...] = (base_ref[...].astype(jnp.float32) + fresh + hidden * lifted).astype(
        jnp.bfloat16
    )


def chunk_body(
    per, texts_here, self_ref, core_ref, mine_ref, other_ref, agg_ref, down_ref, pick_ref, own_ref,
    grad_ref, keep_ref, give_ref, w_ref, text_ref
):
    kept, _, half = keep_ref.shape
    shards = 2 * kept
    deep = up_to(per, ROWS)
    text_rows = keep_ref.shape[1] - deep
    me = self_ref[0]
    own = pl.multiple_of(core_ref[0] * half, LANES)
    far = pl.multiple_of((1 - core_ref[0]) * half, LANES)
    columns = 2 * half
    text_ref[...] = mm(pick_ref[...], down_ref[...], (0, 0)) + mm(
        own_ref[...], grad_ref[...], (0, 0)
    )
    w_ref[pl.ds(own, half), :] = mm(mine_ref[...], agg_ref[...], (0, 0))
    w_ref[pl.ds(far, half), :] = mm(other_ref[...], agg_ref[...], (0, 0))
    w_ref[columns:, :] = jnp.zeros((w_ref.shape[0] - columns, half), jnp.float32)
    row = lax.broadcasted_iota(jnp.int32, (text_rows, half), 0)
    for q in range(shards):
        piece = w_ref[q * per : q * per + deep, :].astype(jnp.bfloat16)
        block = jnp.zeros((text_rows, half), jnp.float32)
        for i in range(texts_here):
            line = text_ref[i * shards + q : i * shards + q + 1, :]
            high = line.astype(jnp.bfloat16).astype(jnp.float32)
            block = jnp.where(row == i, high, block)
            block = jnp.where(row == text_rows // 2 + i, line - high, block)
        block = block.astype(jnp.bfloat16)
        step = q ^ me
        turned = step * 0
        reach = 1
        while reach < shards:
            turned = 2 * turned + ((step // reach) & 1)
            reach *= 2

        @pl.when(turned < kept)
        def _():
            keep_ref[turned, :deep, :] = piece
            keep_ref[turned, deep:, :] = block

        @pl.when(turned >= kept)
        def _():
            give_ref[turned - kept, :deep, :] = piece
            give_ref[turned - kept, deep:, :] = block


def backward_body(
    ids_ref, self_ref, core_ref, mine_ref, other_ref, w_own_ref, adj_ref, send_hbm, down_hbm,
    down_ref, send_ref, sems, slot_sems
):
    tiles_here, entries, tile_rows, _ = adj_ref.shape
    shards, _, half = send_hbm.shape
    me = self_ref[0]
    core = core_ref[0]
    own = pl.multiple_of(core * half, LANES)
    far = pl.multiple_of((1 - core) * half, LANES)
    down = mm(mine_ref[...], w_own_ref[:, pl.ds(own, half)], (1, 1)) + mm(
        other_ref[...], w_own_ref[:, pl.ds(far, half)], (1, 1)
    )
    down_ref[...] = down.astype(jnp.bfloat16)
    down_copy = pltpu.make_async_copy(down_ref, down_hbm, sems.at[0])
    down_copy.start()
    for r in range(tiles_here):
        rows = slice(r * tile_rows, (r + 1) * tile_rows)
        for first in range(0, entries, 6):
            group = range(first, min(first + 6, entries))
            side_by_side = jnp.concatenate([adj_ref[r, k] for k in group], axis=1)
            product = mm(side_by_side, down_ref[rows, :], (0, 0)).astype(jnp.bfloat16)
            for k in group:
                tile_id = ids_ref[r, k]
                _, owner, _ = tile_of(tile_id, tiles_here)
                slot = jnp.where((tile_id >= 0) & (owner != me), owner, shards)
                send_ref[slot] = product[(k - first) * tile_rows : (k - first + 1) * tile_rows]
    for copy in copies([(send_ref.at[q], send_hbm.at[q]) for q in range(shards)], slot_sems):
        copy.wait()
    down_copy.wait()


def fold(mine, theirs, deep):
    total = mine.astype(jnp.float32) + theirs.astype(jnp.float32)
    lines = (total.shape[0] - deep) // 2
    return total[:deep, :], total[deep : deep + lines, :] + total[deep + lines :, :]


def fold_body(deep, mine_ref, theirs_ref, keep_ref, give_ref):
    kept = keep_ref.shape[0]
    for s in range(2 * kept):
        w_sum, text = fold(mine_ref[s], theirs_ref[s], deep)
        high = text.astype(jnp.bfloat16).astype(jnp.float32)
        out_ref = (keep_ref if s < kept else give_ref).at[s % kept]
        out_ref[:deep, :] = w_sum.astype(jnp.bfloat16)
        out_ref[deep:, :] = jnp.concatenate([high, text - high], axis=0).astype(jnp.bfloat16)


def close_body(deep, mine_ref, theirs_ref, w_ref, text_ref):
    w_sum, text = fold(mine_ref[0], theirs_ref[0], deep)
    w_ref[...] = w_sum
    text_ref[...] = text[: text_ref.shape[0], :]


def local_body(ids_ref, self_ref, down_ref, adj_ref, grad_ref, local_ref):
    tiles_here, entries, _, _ = adj_ref.shape
    me = self_ref[0]
    local_ref[...] = grad_ref[...].astype(jnp.float32)
    for r in range(tiles_here):

        def one(k, carry):
            tile_id = ids_ref[r, k]
            _, owner, place = tile_of(tile_id, tiles_here)

            @pl.when((tile_id >= 0) & (owner == me))
            def _():
                local_ref[place] += mm(adj_ref[r, k], down_ref[r], (0, 0))

            return carry

        lax.fori_loop(0, entries, one, 0, unroll=unroll(entries))


def finish_body(self_ref, asked_ref, mate_ref, local_hbm, got_ref, node_ref, sum_ref, sems):
    local = pltpu.make_async_copy(local_hbm, sum_ref, sems.at[0])
    local.start()
    shards = got_ref.shape[0]
    me = self_ref[0]
    local.wait()

    def one(q, carry):
        side, spot = side_of(q, me, shards // 2)
        asked = jnp.where(side == 0, asked_ref[spot, 0], mate_ref[spot, 1])

        @pl.when(asked >= 0)
        def _():
            sum_ref[asked] += got_ref[q].astype(jnp.float32)

        return carry

    lax.fori_loop(0, shards, one, 0)
    node_ref[...] = sum_ref[...].astype(jnp.bfloat16)


def step(
    tokens, token_counts, w_qkv, w_out, w_up, w_down, ln_gains, cache, node_text, adj_tiles,
    adj_values, w_gnn, out_grad
):
    shards = lax.axis_size("graph")
    cores = lax.axis_size("mp")
    me = lax.axis_index("graph").astype(jnp.int32).reshape(1)
    core_at = lax.axis_index("mp")
    core = core_at.astype(jnp.int32).reshape(1)
    texts_here, seq, width = tokens.shape
    nodes_here, half = cache.shape
    tiles_here, entries, tile_rows = adj_values.shape[:3]
    texts = texts_here * shards
    slots = up_to(texts, LANES)
    per = width // shards
    deep = up_to(per, ROWS)
    count = texts_here * seq
    inner = w_up.shape[1]

    def swap(values):
        return lax.ppermute(values, "mp", [(i, cores - 1 - i) for i in range(cores)])

    def toward(values, reach):
        return lax.ppermute(values, "graph", [(i, i ^ reach) for i in range(shards)])

    peers = shards // 2

    def spread(values, groups=None):
        return lax.all_to_all(
            values, "graph", split_axis=0, concat_axis=0, tiled=True, axis_index_groups=groups
        )

    halves_of = [list(range(peers)), list(range(peers, shards))]

    cache_tiles = cache.reshape(tiles_here, tile_rows, half)
    mate_tiles = toward(cache_tiles, peers)
    index = call(
        functools.partial(index_body, texts_here),
        [shape((peers, 1, slots + 2 * LANES), jnp.int32)],
        [adj_tiles, me, node_text.reshape(tiles_here, tile_rows)],
        [HBM, SMEM, HBM],
        flops=1000,
        scratch=[
            pltpu.SMEM(adj_tiles.shape, jnp.int32),
            pltpu.VMEM((tiles_here, tile_rows), jnp.int32),
            pltpu.SemaphoreType.DMA((2,)),
        ],
    )
    got = spread(index, halves_of)
    mate_got = toward(got, peers)

    def places(table):
        return table[:, 0, slots:].reshape(peers, 2, LANES)[:, :, 0]

    asked = places(got)
    packed = call(
        pack_body,
        [shape((peers, 2 * tile_rows, half))],
        [asked, cache_tiles, mate_tiles],
        [SMEM, HBM, HBM],
        flops=1000,
        scratch=[
            pltpu.VMEM((2,) + cache_tiles.shape, jnp.bfloat16),
            pltpu.SemaphoreType.DMA((2,)),
            pltpu.SemaphoreType.DMA((2, peers)),
        ],
        out_specs=[HBM],
    )
    remote = spread(packed, halves_of)

    w_other = swap(w_gnn)

    flat_tokens = tokens.reshape(count, width)
    partial = call(
        functools.partial(attend_body, seq),
        [shape((count, width))],
        [token_counts, flat_tokens, jnp.transpose(w_qkv, (1, 0, 2)), w_out],
        [SMEM, HBM, HBM, HBM],
        flops=2 * count * (width * 3 * half + half * width + 2 * seq * half * 2),
        scratch=[
            pltpu.VMEM((count, width), jnp.bfloat16),
            pltpu.VMEM((3, width, half), jnp.bfloat16),
            pltpu.VMEM((half, width), jnp.bfloat16),
            pltpu.VMEM((count, width), jnp.bfloat16),
            pltpu.VMEM((count, 3 * half), jnp.bfloat16),
            pltpu.VMEM((count, half), jnp.bfloat16),
            pltpu.SemaphoreType.DMA((5,)),
            pltpu.SemaphoreType.DMA((texts_here,)),
        ],
        out_specs=[HBM],
    )
    first, mlp = call(
        inner_body,
        [shape((count, width)), shape((count, width))],
        [flat_tokens, partial, swap(partial), w_up, w_down, ln_gains],
        [HBM] * 5 + [VMEM],
        flops=4 * count * width * inner,
        scratch=[
            pltpu.VMEM((count, inner), jnp.bfloat16),
            pltpu.VMEM((count, width), jnp.bfloat16),
            pltpu.VMEM((count, width), jnp.bfloat16),
            pltpu.VMEM((count, width), jnp.bfloat16),
            pltpu.VMEM((width, inner), jnp.bfloat16),
            pltpu.VMEM((inner, width), jnp.bfloat16),
            pltpu.SemaphoreType.DMA((5,)),
        ],
    )
    pooled = call(
        functools.partial(pool_body, seq),
        [shape((1, 1, texts_here * half), jnp.float32)],
        [token_counts, core, first, mlp, swap(mlp), ln_gains],
        [SMEM, SMEM, VMEM, VMEM, VMEM, VMEM],
        flops=20 * count * width,
        scratch=[pltpu.VMEM((8, width), jnp.float32)],
    )
    near = pooled
    reach = peers
    far = toward(near, reach)
    while reach > 1:
        reach = reach // 2
        near = jnp.concatenate([near, far], axis=0)
        far = toward(near, reach)

    kept, pick, own, base = call(
        mask_body,
        [
            shape(adj_values.shape),
            shape((tiles_here, tile_rows, slots)),
            shape((tiles_here, tile_rows, slots)),
            shape(cache_tiles.shape),
        ],
        [adj_tiles, me, got, mate_got, adj_values, cache_tiles],
        [SMEM, SMEM, VMEM, VMEM, VMEM, VMEM],
        flops=2 * adj_values.size * slots,
        scratch=[
            pltpu.VMEM(adj_values.shape, jnp.bfloat16),
            pltpu.VMEM((tiles_here, tile_rows, slots), jnp.bfloat16),
            pltpu.VMEM((tiles_here, tile_rows, slots), jnp.bfloat16),
            pltpu.VMEM(cache_tiles.shape, jnp.bfloat16),
            pltpu.SemaphoreType.DMA((tiles_here, 4)),
        ],
        out_specs=[HBM] * 4,
    )
    gathered, pooled = call(
        gather_body,
        [shape((tiles_here, tile_rows, half)), shape((texts, half))],
        [adj_tiles, me, kept, pick, near, far, cache_tiles, remote],
        [HBM, SMEM, HBM, HBM, HBM, HBM, HBM, VMEM],
        flops=2 * adj_values.size * half,
        scratch=[
            pltpu.SMEM(adj_tiles.shape, jnp.int32),
            pltpu.VMEM(kept.shape, jnp.bfloat16),
            pltpu.VMEM(pick.shape, jnp.bfloat16),
            pltpu.VMEM(near.shape, jnp.float32),
            pltpu.VMEM(far.shape, jnp.float32),
            pltpu.VMEM(cache_tiles.shape, jnp.bfloat16),
            pltpu.VMEM((2, entries, tile_rows, half), jnp.bfloat16),
            pltpu.SemaphoreType.DMA((6,)),
        ],
    )
    gathered = gathered.reshape(nodes_here, half)
    node_out, slope = call(
        forward_body,
        [shape((nodes_here, half)), shape((nodes_here, half))],
        [
            core, gathered, swap(gathered), w_gnn, w_other, out_grad,
            own.reshape(nodes_here, slots), base.reshape(nodes_here, half), pooled,
        ],
        [SMEM] + [VMEM] * 8,
        flops=4 * nodes_here * half * half,
    )
    grad_tiles = out_grad.reshape(tiles_here, tile_rows, half)
    slope_other = swap(slope)
    text_rows = up_to(2 * texts_here, 8)
    halves = (shards // 2, deep + text_rows, half)
    send, down = call(
        backward_body,
        [shape((shards, tile_rows, half)), shape((nodes_here, half))],
        [adj_tiles, me, core, slope, slope_other, w_gnn, adj_values],
        [SMEM, SMEM, SMEM] + [VMEM] * 4,
        flops=4 * nodes_here * half * half + 2 * adj_values.size * half,
        scratch=[
            pltpu.VMEM((nodes_here, half), jnp.bfloat16),
            pltpu.VMEM((shards + 1, tile_rows, half), jnp.bfloat16),
            pltpu.SemaphoreType.DMA((1,)),
            pltpu.SemaphoreType.DMA((shards,)),
        ],
        out_specs=[HBM] * 2,
    )
    returned = spread(send)
    keep, give = call(
        functools.partial(chunk_body, per, texts_here),
        [shape(halves), shape(halves)],
        [
            me, core, slope, slope_other, gathered, down, pick.reshape(nodes_here, slots),
            own.reshape(nodes_here, slots), out_grad,
        ],
        [SMEM, SMEM] + [PULL] * 7,
        flops=4 * nodes_here * half * (half + slots),
        scratch=[
            pltpu.VMEM((width + ROWS, half), jnp.float32),
            pltpu.VMEM((slots, half), jnp.float32),
        ],
    )
    local = call(
        local_body,
        [shape((tiles_here, tile_rows, half), jnp.float32)],
        [adj_tiles, me, down.reshape(tiles_here, tile_rows, half), adj_values, grad_tiles],
        [SMEM, SMEM] + [VMEM] * 3,
        flops=2 * adj_values.size * half,
    )
    reach = 1
    given = toward(give, reach)
    while 2 * reach < shards:
        part = (shards // (4 * reach), deep + text_rows, half)
        keep, give = call(
            functools.partial(fold_body, deep),
            [shape(part), shape(part)],
            [keep, given],
            [VMEM] * 2,
            flops=4 * math.prod(part),
        )
        reach = 2 * reach
        given = toward(give, reach)
    w_part, text_grad = call(
        functools.partial(close_body, deep),
        [shape((deep, half), jnp.float32), shape((texts_here, half), jnp.float32)],
        [keep, given],
        [VMEM] * 2,
        flops=1000,
    )
    node_grad = call(
        finish_body,
        [shape((tiles_here, tile_rows, half))],
        [me, asked, places(mate_got), local, returned],
        [SMEM, SMEM, SMEM, HBM, VMEM],
        flops=1000,
        scratch=[
            pltpu.VMEM((tiles_here, tile_rows, half), jnp.float32),
            pltpu.SemaphoreType.DMA((1,)),
        ],
    )
    return (node_out, w_part[:per].T, text_grad, node_grad.reshape(nodes_here, half))


def solution(mesh):
    placed = (
        P("graph", None, None),
        P("graph", None),
        P(None, None, "mp"),
        P("mp", None),
        P(None, "mp"),
        P("mp", None),
        P(),
        P("graph", "mp"),
        P("graph"),
        P("graph", None),
        P("graph", None, None, None),
        P("mp", None),
        P("graph", "mp"),
    )
    return jax.shard_map(
        step,
        mesh=mesh,
        in_specs=placed,
        out_specs=(P("graph", "mp"), P("mp", "graph"), P("graph", "mp"), P("graph", "mp")),
        check_vma=False,
    )
```

```python
import functools
import math

import jax
import jax.numpy as jnp
from jax import lax
from jax.experimental import pallas as pl
from jax.experimental.pallas import tpu as pltpu
from jax.sharding import PartitionSpec as P


HEAD = 64
LANES = 128
ROWS = 16
SPARE = 6 << 20
NORM_EPS = 1e-05
MASKED = -1e30
NO_NODE = -(1 << 20)
ROOT = 0.7978845608028654
CUBE = 0.044715

VMEM = pl.BlockSpec(memory_space=pltpu.VMEM)
HBM = pl.BlockSpec(memory_space=pltpu.HBM)
PULL = pl.BlockSpec(memory_space=pltpu.HBM)
SMEM = pl.BlockSpec(memory_space=pltpu.SMEM)


def up_to(value, unit):
    return (value + unit - 1) // unit * unit


def call(body, outs, ins, specs, flops, scratch=(), out_specs=None):
    moved = sum(a.size * a.dtype.itemsize for a in ins) + sum(
        o.size * o.dtype.itemsize for o in outs
    )
    many = len(outs) > 1
    ins = [
        pltpu.with_memory_space_constraint(a, pltpu.HBM) if s is HBM or s is PULL else a
        for a, s in zip(ins, specs, strict=True)
    ]
    pulled = [i for i, s in enumerate(specs) if s is PULL]
    if pulled:
        body = pulling(body, pulled)
        scratch = list(scratch) + [pltpu.VMEM(ins[i].shape, ins[i].dtype) for i in pulled]
        scratch.append(pltpu.SemaphoreType.DMA((len(pulled),)))
    held = sum(math.prod(s.shape) * jnp.dtype(s.dtype).itemsize for s in scratch if counted(s))
    out_specs = out_specs or [VMEM] * len(outs)
    outs = [
        pltpu.HBM(o.shape, o.dtype) if s is HBM else o for o, s in zip(outs, out_specs, strict=True)
    ]
    return pl.pallas_call(
        body,
        out_shape=tuple(outs) if many else outs[0],
        in_specs=list(specs),
        out_specs=tuple(out_specs) if many else out_specs[0],
        scratch_shapes=list(scratch),
        compiler_params=pltpu.CompilerParams(vmem_limit_bytes=moved + moved // 8 + held + SPARE),
        cost_estimate=pl.CostEstimate(flops=flops, bytes_accessed=moved, transcendentals=0),
    )(*ins)


def counted(scratch):
    return jnp.issubdtype(scratch.dtype, jnp.number)


def copies(pairs, sems):
    started = [pltpu.make_async_copy(a, b, sems.at[i]) for i, (a, b) in enumerate(pairs)]
    for copy in started:
        copy.start()
    return started


def pulling(body, pulled):
    def wrapped(*refs):
        buffers, sems = refs[-len(pulled) - 1 : -1], refs[-1]
        held = list(refs[: -len(pulled) - 1])
        started = copies([(held[i], b) for i, b in zip(pulled, buffers)], sems)
        for i, buffer in zip(pulled, buffers):
            held[i] = buffer
        for copy in started:
            copy.wait()
        body(*held)

    return wrapped


def unroll(steps):
    return steps if steps <= 8 else 1


def shape(dims, dtype=jnp.bfloat16):
    return jax.ShapeDtypeStruct(tuple(dims), dtype)


def mm(a, b, dims=(1, 0)):
    return lax.dot_general(
        a, b, (((dims[0],), (dims[1],)), ((), ())), preferred_element_type=jnp.float32
    )


def tile_of(tile_id, tiles_here):
    safe = jnp.maximum(tile_id, 0)
    owner = lax.div(safe, jnp.int32(tiles_here))
    return safe, owner, safe - owner * tiles_here


def side_of(owner, me, peers):
    half = lax.div(owner, jnp.int32(peers))
    mine = lax.div(me, jnp.int32(peers))
    return jnp.where(half == mine, 0, 1), owner - half * peers


def index_body(texts_here, ids_hbm, self_ref, text_hbm, out_ref, ids_ref, text_ref, sems):
    for copy in copies([(ids_hbm, ids_ref), (text_hbm, text_ref)], sems):
        copy.wait()
    tiles_here, entries = ids_ref.shape
    peers, _, lanes = out_ref.shape
    shards = 2 * peers
    width = lanes - 2 * LANES
    texts = texts_here * shards
    me = self_ref[0]
    row = lax.broadcasted_iota(jnp.int32, (peers, LANES), 0)
    near = jnp.full((peers, LANES), -1, jnp.int32)
    far = near
    for r in range(tiles_here):
        for k in range(entries):
            tile_id = ids_ref[r, k]
            _, owner, place = tile_of(tile_id, tiles_here)
            side, spot = side_of(owner, me, peers)
            wanted = (tile_id >= 0) & (owner != me)
            near = jnp.where(row == jnp.where(wanted & (side == 0), spot, -1), place, near)
            far = jnp.where(row == jnp.where(wanted & (side == 1), spot, -1), place, far)
    out_ref[:, :, width : width + LANES] = near.reshape(peers, 1, LANES)
    out_ref[:, :, width + LANES :] = far.reshape(peers, 1, LANES)
    tile_rows = text_ref.shape[1]
    lane = lax.broadcasted_iota(jnp.int32, (LANES, tile_rows), 1)
    sub = lax.broadcasted_iota(jnp.int32, (LANES, LANES), 0)
    diagonal = sub == lax.broadcasted_iota(jnp.int32, (LANES, LANES), 1)
    for c in range(width // LANES):
        slot = c * LANES + lax.broadcasted_iota(jnp.int32, (LANES, 1), 0)
        part = lax.div(slot, jnp.int32(shards))
        text = jnp.where(slot < texts, (slot - part * shards) * texts_here + part, -5)
        best = jnp.full((LANES, tile_rows), NO_NODE, jnp.int32)
        for j in range(tiles_here):
            node = (me * tiles_here + j) * tile_rows + lane
            best = jnp.where(text_ref[j : j + 1, :] == text, node, best)
        column = jnp.max(best.astype(jnp.float32), axis=1, keepdims=True)
        line = jnp.max(jnp.where(diagonal, column, float(NO_NODE)), axis=0, keepdims=True)
        out_ref[:, :, c * LANES : (c + 1) * LANES] = (
            jnp.broadcast_to(line, (peers, LANES)).astype(jnp.int32).reshape(peers, 1, LANES)
        )


def pack_body(asked_ref, cache_hbm, mate_hbm, out_hbm, tile_ref, in_sems, out_sems):
    _, _, tile_rows, _ = tile_ref.shape
    started = copies([(cache_hbm, tile_ref.at[0]), (mate_hbm, tile_ref.at[1])], in_sems)
    peers = out_hbm.shape[0]

    def slot(p, side):
        place = jnp.maximum(asked_ref[p, side], 0)
        target = out_hbm.at[p, pl.ds(side * tile_rows, tile_rows), :]
        return pltpu.make_async_copy(tile_ref.at[side, place], target, out_sems.at[side, p])

    for side in range(2):
        started[side].wait()
        lax.fori_loop(0, peers, lambda p, c: (slot(p, side).start(), c)[1], 0)
    for side in range(2):
        lax.fori_loop(0, peers, lambda p, c: (slot(p, side).wait(), c)[1], 0)


def mask_body(
    ids_ref, self_ref, got_ref, mate_ref, adj_ref, cache_ref, *refs
):
    outs, (kept_ref, pick_ref, own_ref, base_ref, sems) = refs[:4], refs[4:]
    tiles_here, entries, tile_rows, _ = adj_ref.shape
    peers, _, lanes = got_ref.shape
    width = lanes - 2 * LANES
    me = self_ref[0]
    both = jnp.maximum(got_ref[:, :, :width], mate_ref[:, :, :width])
    table = jnp.max(both.reshape(peers, width).astype(jnp.float32), axis=0, keepdims=True)
    place = lax.broadcasted_iota(jnp.int32, (tile_rows, width), 0).astype(jnp.float32)
    ones = jnp.ones((ROWS, width), jnp.bfloat16)
    sent = []

    def holds(tile_id):
        first = (tile_id * tile_rows).astype(jnp.float32)
        return jnp.where(table - first == place, 1.0, 0.0)

    for r in range(tiles_here):

        def one(k, total):
            tile_id = ids_ref[r, k]
            hot = holds(tile_id).astype(jnp.bfloat16)
            values = adj_ref[r, k]
            taken = mm(ones, hot, (1, 1))[0:1, :]
            keep = jnp.where(tile_id >= 0, 1.0, 0.0) * jnp.where(taken > 0.5, 0.0, 1.0)
            kept_ref[r, k] = (values.astype(jnp.float32) * keep).astype(jnp.bfloat16)
            return total + mm(values, hot)

        pick = lax.fori_loop(
            0, entries, one, jnp.zeros((tile_rows, width), jnp.float32), unroll=unroll(entries)
        )
        pick_ref[r] = pick.astype(jnp.bfloat16)
        hot = holds(me * tiles_here + r)
        own_ref[r] = hot.astype(jnp.bfloat16)
        fresh = jnp.max(hot, axis=1, keepdims=True)
        base_ref[r] = (cache_ref[r].astype(jnp.float32) * (1.0 - fresh)).astype(jnp.bfloat16)
        row = [(ref.at[r], out.at[r]) for ref, out in zip((kept_ref, pick_ref, own_ref, base_ref), outs)]
        sent = sent + copies(row, sems.at[r])
    for copy in sent:
        copy.wait()


def norm(values, gain):
    average = jnp.mean(values, axis=-1, keepdims=True)
    centred = values - average
    variance = jnp.mean(centred * centred, axis=-1, keepdims=True)
    return centred * lax.rsqrt(variance + NORM_EPS) * gain


def attend_body(
    seq, counts_ref, tokens_hbm, w_qkv_hbm, w_out_hbm, out_hbm,
    tokens_ref, w_qkv_ref, w_out_ref, out_ref, proj_ref, ctx_ref, in_sems, out_sems
):
    half = w_out_ref.shape[0]
    texts_here = tokens_ref.shape[0] // seq
    started = copies(
        [(tokens_hbm, tokens_ref)]
        + [(w_qkv_hbm.at[c], w_qkv_ref.at[c]) for c in range(3)]
        + [(w_out_hbm, w_out_ref)],
        in_sems,
    )
    started[0].wait()
    for c in range(3):
        started[1 + c].wait()
        proj_ref[:, c * half : (c + 1) * half] = mm(tokens_ref[...], w_qkv_ref[c]).astype(
            jnp.bfloat16
        )
    started[4].wait()
    sent = []
    left = lax.broadcasted_iota(jnp.int32, (seq, LANES), 1) < HEAD
    key_at = lax.broadcasted_iota(jnp.int32, (seq, seq), 1)
    for t in range(texts_here):
        rows = pl.ds(t * seq, seq)
        live = key_at < counts_ref[0, t]
        for pair in range(half // LANES):
            first = pair * LANES
            query = proj_ref[rows, first : first + LANES].astype(jnp.float32) * (HEAD**-0.5)
            key = proj_ref[rows, half + first : half + first + LANES]
            value = proj_ref[rows, 2 * half + first : 2 * half + first + LANES]
            sides = []
            for side in (left, jnp.logical_not(left)):
                scores = mm(jnp.where(side, query, 0.0).astype(jnp.bfloat16), key, (1, 1))
                scores = jnp.where(live, scores, MASKED)
                powers = jnp.exp(scores - jnp.max(scores, axis=-1, keepdims=True))
                total = jnp.sum(powers, axis=-1, keepdims=True)
                sides.append(mm((powers / total).astype(jnp.bfloat16), value))
            ctx_ref[rows, first : first + LANES] = jnp.where(left, sides[0], sides[1]).astype(
                jnp.bfloat16
            )
        out_ref[rows, :] = mm(ctx_ref[rows, :], w_out_ref[...]).astype(jnp.bfloat16)
        sent.append(pltpu.make_async_copy(out_ref.at[rows, :], out_hbm.at[rows, :], out_sems.at[t]))
        sent[-1].start()
    for copy in sent:
        copy.wait()


def inner_body(
    tokens_hbm, mine_hbm, other_hbm, up_hbm, down_hbm, gains_ref, first_ref, out_ref,
    inner_ref, tokens_ref, mine_ref, other_ref, up_ref, down_ref, sems
):
    started = copies(
        [
            (tokens_hbm, tokens_ref), (mine_hbm, mine_ref), (other_hbm, other_ref),
            (up_hbm, up_ref), (down_hbm, down_ref),
        ],
        sems,
    )
    for copy in started[:3]:
        copy.wait()
    added = mine_ref[...].astype(jnp.float32) + other_ref[...].astype(jnp.float32)
    first = norm(tokens_ref[...].astype(jnp.float32) + added, gains_ref[0:1, :])
    first_ref[...] = first.astype(jnp.bfloat16)
    started[3].wait()
    hidden_units = up_ref.shape[1]
    step = hidden_units // 4
    for c in range(4):
        cols = slice(c * step, (c + 1) * step)
        value = mm(first_ref[...], up_ref[:, cols])
        gate = jnp.tanh(ROOT * (value + CUBE * (value * value * value)))
        inner_ref[:, cols] = (0.5 * value * (1.0 + gate)).astype(jnp.bfloat16)
    started[4].wait()
    out_ref[...] = mm(inner_ref[...], down_ref[...]).astype(jnp.bfloat16)


def pool_body(seq, counts_ref, first_ref, mine_ref, other_ref, gains_ref, out_ref):
    shards = out_ref.shape[0]
    texts_here, width = first_ref.shape[0] // seq, first_ref.shape[1]
    for t in range(texts_here):
        rows = slice(t * seq, (t + 1) * seq)
        added = mine_ref[rows, :].astype(jnp.float32) + other_ref[rows, :].astype(jnp.float32)
        second = norm(first_ref[rows, :].astype(jnp.float32) + added, gains_ref[1:2, :])
        count = counts_ref[0, t]
        live = lax.broadcasted_iota(jnp.int32, (seq, 1), 0) < count
        total = jnp.sum(jnp.where(live, second, 0.0), axis=0, keepdims=True)
        pooled = (total / count.astype(jnp.float32)).astype(jnp.bfloat16).astype(jnp.float32)
        out_ref[:, :, t * width : (t + 1) * width] = jnp.broadcast_to(pooled, (shards, width)).reshape(
            shards, 1, width
        )


def pooled_rows(pooled_ref, width):
    shards, _, lanes = pooled_ref.shape
    parts = [
        pooled_ref[:, :, first : first + width].reshape(shards, width).astype(jnp.bfloat16)
        for first in range(0, lanes, width)
    ]
    return jnp.concatenate(parts, axis=0)


def gather_body(
    ids_hbm, self_ref, kept_hbm, cache_hbm, remote_ref, out_hbm,
    ids_ref, kept_ref, cache_ref, source_ref, out_ref, sems, out_sems
):
    started = copies([(ids_hbm, ids_ref), (cache_hbm, cache_ref), (kept_hbm, kept_ref)], sems)
    tiles_here, entries, tile_rows, _ = kept_ref.shape
    me = self_ref[0]
    started[0].wait()
    started[1].wait()

    def fetch(r, k):
        tile_id = ids_ref[r, k]
        _, owner, place = tile_of(tile_id, tiles_here)
        local = (owner == me) | (tile_id < 0)

        @pl.when(local)
        def _():
            source_ref[r % 2, k] = cache_ref[place]

        @pl.when(jnp.logical_not(local))
        def _():
            side, spot = side_of(owner, me, remote_ref.shape[0])
            first = pl.multiple_of(side * tile_rows, tile_rows)
            source_ref[r % 2, k] = remote_ref[spot, pl.ds(first, tile_rows), :]

    sent = []
    for r in range(tiles_here):
        lax.fori_loop(
            0, entries, lambda k, c: (fetch(r, k), c)[1], 0, unroll=unroll(entries)
        )
        if r == 0:
            started[2].wait()
        total = jnp.zeros(out_ref.shape[1:], jnp.float32)
        for k in range(entries):
            total = total + mm(kept_ref[r, k], source_ref[r % 2, k])
        out_ref[r] = total.astype(jnp.bfloat16)
        sent.append(pltpu.make_async_copy(out_ref.at[r], out_hbm.at[r], out_sems.at[r]))
        sent[-1].start()
    for copy in sent:
        copy.wait()


def forward_body(
    core_ref, mine_ref, other_ref, w_own_ref, w_other_ref, grad_ref, own_ref, base_ref, pick_ref,
    pooled_ref, node_ref, slope_ref, rows_ref
):
    half = mine_ref.shape[1]
    start = pl.multiple_of(core_ref[0] * half, LANES)
    far = pl.multiple_of((1 - core_ref[0]) * half, LANES)
    rows_ref[...] = pooled_rows(pooled_ref, rows_ref.shape[1])
    texts = rows_ref.shape[0]
    here = rows_ref[:, pl.ds(start, half)]
    w_own = w_own_ref[:, pl.ds(start, half)]
    w_other = w_other_ref[:, pl.ds(start, half)]
    moved = (mm(here, w_own) + mm(rows_ref[:, pl.ds(far, half)], w_other)).astype(jnp.bfloat16)
    hidden = (
        mm(mine_ref[...], w_own) + mm(other_ref[...], w_other) + mm(pick_ref[:, :texts], moved)
    )
    square = hidden * hidden
    gate = jnp.tanh(ROOT * hidden * (1.0 + CUBE * square))
    lifted = 0.5 * (1.0 + gate)
    slope = lifted + 0.5 * hidden * (1.0 - gate * gate) * (ROOT * (1.0 + 3.0 * CUBE * square))
    slope_ref[...] = (grad_ref[...].astype(jnp.float32) * slope).astype(jnp.bfloat16)
    fresh = mm(own_ref[:, :texts], here)
    node_ref[...] = (base_ref[...].astype(jnp.float32) + fresh + hidden * lifted).astype(
        jnp.bfloat16
    )


def chunk_body(
    per, texts_here, self_ref, core_ref, mine_ref, other_ref, part_ref, down_ref, pick_ref, own_ref,
    grad_ref, pooled_ref, keep_ref, give_ref, w_ref, text_ref, rows_ref, agg_ref
):
    kept, _, half = keep_ref.shape
    shards = 2 * kept
    deep = up_to(per, ROWS)
    text_rows = keep_ref.shape[1] - deep
    me = self_ref[0]
    own = pl.multiple_of(core_ref[0] * half, LANES)
    far = pl.multiple_of((1 - core_ref[0]) * half, LANES)
    rows_ref[...] = pooled_rows(pooled_ref, rows_ref.shape[1])
    here = rows_ref[:, pl.ds(own, half)]
    agg_ref[...] = (
        part_ref[...].astype(jnp.float32) + mm(pick_ref[:, : here.shape[0]], here)
    ).astype(jnp.bfloat16)
    columns = 2 * half
    text_ref[...] = mm(pick_ref[...], down_ref[...], (0, 0)) + mm(
        own_ref[...], grad_ref[...], (0, 0)
    )
    w_ref[pl.ds(own, half), :] = mm(mine_ref[...], agg_ref[...], (0, 0))
    w_ref[pl.ds(far, half), :] = mm(other_ref[...], agg_ref[...], (0, 0))
    w_ref[columns:, :] = jnp.zeros((w_ref.shape[0] - columns, half), jnp.float32)
    row = lax.broadcasted_iota(jnp.int32, (text_rows, half), 0)
    for q in range(shards):
        piece = w_ref[q * per : q * per + deep, :].astype(jnp.bfloat16)
        block = jnp.zeros((text_rows, half), jnp.float32)
        for i in range(texts_here):
            line = text_ref[i * shards + q : i * shards + q + 1, :]
            high = line.astype(jnp.bfloat16).astype(jnp.float32)
            block = jnp.where(row == i, high, block)
            block = jnp.where(row == text_rows // 2 + i, line - high, block)
        block = block.astype(jnp.bfloat16)
        step = q ^ me
        turned = step * 0
        reach = 1
        while reach < shards:
            turned = 2 * turned + ((step // reach) & 1)
            reach *= 2

        @pl.when(turned < kept)
        def _():
            keep_ref[turned, :deep, :] = piece
            keep_ref[turned, deep:, :] = block

        @pl.when(turned >= kept)
        def _():
            give_ref[turned - kept, :deep, :] = piece
            give_ref[turned - kept, deep:, :] = block


def backward_body(
    ids_ref, self_ref, core_ref, mine_ref, other_ref, w_own_ref, adj_ref, send_hbm, down_hbm,
    down_ref, send_ref, sems, slot_sems
):
    tiles_here, entries, tile_rows, _ = adj_ref.shape
    shards, _, half = send_hbm.shape
    me = self_ref[0]
    core = core_ref[0]
    own = pl.multiple_of(core * half, LANES)
    far = pl.multiple_of((1 - core) * half, LANES)
    down = mm(mine_ref[...], w_own_ref[:, pl.ds(own, half)], (1, 1)) + mm(
        other_ref[...], w_own_ref[:, pl.ds(far, half)], (1, 1)
    )
    down_ref[...] = down.astype(jnp.bfloat16)
    down_copy = pltpu.make_async_copy(down_ref, down_hbm, sems.at[0])
    down_copy.start()
    for r in range(tiles_here):
        rows = slice(r * tile_rows, (r + 1) * tile_rows)
        for first in range(0, entries, 6):
            group = range(first, min(first + 6, entries))
            side_by_side = jnp.concatenate([adj_ref[r, k] for k in group], axis=1)
            product = mm(side_by_side, down_ref[rows, :], (0, 0)).astype(jnp.bfloat16)
            for k in group:
                tile_id = ids_ref[r, k]
                _, owner, _ = tile_of(tile_id, tiles_here)
                slot = jnp.where((tile_id >= 0) & (owner != me), owner, shards)
                send_ref[slot] = product[(k - first) * tile_rows : (k - first + 1) * tile_rows]
    for copy in copies([(send_ref.at[q], send_hbm.at[q]) for q in range(shards)], slot_sems):
        copy.wait()
    down_copy.wait()


def fold(mine, theirs, deep):
    total = mine.astype(jnp.float32) + theirs.astype(jnp.float32)
    lines = (total.shape[0] - deep) // 2
    return total[:deep, :], total[deep : deep + lines, :] + total[deep + lines :, :]


def fold_body(deep, mine_ref, theirs_ref, keep_ref, give_ref):
    kept = keep_ref.shape[0]
    for s in range(2 * kept):
        w_sum, text = fold(mine_ref[s], theirs_ref[s], deep)
        high = text.astype(jnp.bfloat16).astype(jnp.float32)
        out_ref = (keep_ref if s < kept else give_ref).at[s % kept]
        out_ref[:deep, :] = w_sum.astype(jnp.bfloat16)
        out_ref[deep:, :] = jnp.concatenate([high, text - high], axis=0).astype(jnp.bfloat16)


def close_body(deep, mine_ref, theirs_ref, w_ref, text_ref):
    w_sum, text = fold(mine_ref[0], theirs_ref[0], deep)
    w_ref[...] = w_sum
    text_ref[...] = text[: text_ref.shape[0], :]


def local_body(ids_ref, self_ref, down_ref, adj_ref, grad_ref, local_ref):
    tiles_here, entries, _, _ = adj_ref.shape
    me = self_ref[0]
    local_ref[...] = grad_ref[...].astype(jnp.float32)
    for r in range(tiles_here):

        def one(k, carry):
            tile_id = ids_ref[r, k]
            _, owner, place = tile_of(tile_id, tiles_here)

            @pl.when((tile_id >= 0) & (owner == me))
            def _():
                local_ref[place] += mm(adj_ref[r, k], down_ref[r], (0, 0))

            return carry

        lax.fori_loop(0, entries, one, 0, unroll=unroll(entries))


def finish_body(self_ref, asked_ref, mate_ref, local_hbm, got_ref, node_ref, sum_ref, sems):
    local = pltpu.make_async_copy(local_hbm, sum_ref, sems.at[0])
    local.start()
    shards = got_ref.shape[0]
    me = self_ref[0]
    local.wait()

    def one(q, carry):
        side, spot = side_of(q, me, shards // 2)
        asked = jnp.where(side == 0, asked_ref[spot, 0], mate_ref[spot, 1])

        @pl.when(asked >= 0)
        def _():
            sum_ref[asked] += got_ref[q].astype(jnp.float32)

        return carry

    lax.fori_loop(0, shards, one, 0)
    node_ref[...] = sum_ref[...].astype(jnp.bfloat16)


def step(
    tokens, token_counts, w_qkv, w_out, w_up, w_down, ln_gains, cache, node_text, adj_tiles,
    adj_values, w_gnn, out_grad
):
    shards = lax.axis_size("graph")
    cores = lax.axis_size("mp")
    me = lax.axis_index("graph").astype(jnp.int32).reshape(1)
    core_at = lax.axis_index("mp")
    core = core_at.astype(jnp.int32).reshape(1)
    texts_here, seq, width = tokens.shape
    nodes_here, half = cache.shape
    tiles_here, entries, tile_rows = adj_values.shape[:3]
    texts = texts_here * shards
    slots = up_to(texts, LANES)
    per = width // shards
    deep = up_to(per, ROWS)
    count = texts_here * seq
    inner = w_up.shape[1]

    def swap(values):
        return lax.ppermute(values, "mp", [(i, cores - 1 - i) for i in range(cores)])

    def toward(values, reach):
        return lax.ppermute(values, "graph", [(i, i ^ reach) for i in range(shards)])

    peers = shards // 2

    def spread(values, groups=None):
        return lax.all_to_all(
            values, "graph", split_axis=0, concat_axis=0, tiled=True, axis_index_groups=groups
        )

    halves_of = [list(range(peers)), list(range(peers, shards))]

    cache_tiles = cache.reshape(tiles_here, tile_rows, half)
    mate_tiles = toward(cache_tiles, peers)
    index = call(
        functools.partial(index_body, texts_here),
        [shape((peers, 1, slots + 2 * LANES), jnp.int32)],
        [adj_tiles, me, node_text.reshape(tiles_here, tile_rows)],
        [HBM, SMEM, HBM],
        flops=1000,
        scratch=[
            pltpu.SMEM(adj_tiles.shape, jnp.int32),
            pltpu.VMEM((tiles_here, tile_rows), jnp.int32),
            pltpu.SemaphoreType.DMA((2,)),
        ],
    )
    got = spread(index, halves_of)
    mate_got = toward(got, peers)

    def places(table):
        return table[:, 0, slots:].reshape(peers, 2, LANES)[:, :, 0]

    asked = places(got)
    packed = call(
        pack_body,
        [shape((peers, 2 * tile_rows, half))],
        [asked, cache_tiles, mate_tiles],
        [SMEM, HBM, HBM],
        flops=1000,
        scratch=[
            pltpu.VMEM((2,) + cache_tiles.shape, jnp.bfloat16),
            pltpu.SemaphoreType.DMA((2,)),
            pltpu.SemaphoreType.DMA((2, peers)),
        ],
        out_specs=[HBM],
    )
    remote = spread(packed, halves_of)

    w_other = swap(w_gnn)

    flat_tokens = tokens.reshape(count, width)
    partial = call(
        functools.partial(attend_body, seq),
        [shape((count, width))],
        [token_counts, flat_tokens, jnp.transpose(w_qkv, (1, 0, 2)), w_out],
        [SMEM, HBM, HBM, HBM],
        flops=2 * count * (width * 3 * half + half * width + 2 * seq * half * 2),
        scratch=[
            pltpu.VMEM((count, width), jnp.bfloat16),
            pltpu.VMEM((3, width, half), jnp.bfloat16),
            pltpu.VMEM((half, width), jnp.bfloat16),
            pltpu.VMEM((count, width), jnp.bfloat16),
            pltpu.VMEM((count, 3 * half), jnp.bfloat16),
            pltpu.VMEM((count, half), jnp.bfloat16),
            pltpu.SemaphoreType.DMA((5,)),
            pltpu.SemaphoreType.DMA((texts_here,)),
        ],
        out_specs=[HBM],
    )
    first, mlp = call(
        inner_body,
        [shape((count, width)), shape((count, width))],
        [flat_tokens, partial, swap(partial), w_up, w_down, ln_gains],
        [HBM] * 5 + [VMEM],
        flops=4 * count * width * inner,
        scratch=[
            pltpu.VMEM((count, inner), jnp.bfloat16),
            pltpu.VMEM((count, width), jnp.bfloat16),
            pltpu.VMEM((count, width), jnp.bfloat16),
            pltpu.VMEM((count, width), jnp.bfloat16),
            pltpu.VMEM((width, inner), jnp.bfloat16),
            pltpu.VMEM((inner, width), jnp.bfloat16),
            pltpu.SemaphoreType.DMA((5,)),
        ],
    )
    pooled = call(
        functools.partial(pool_body, seq),
        [shape((shards, 1, texts_here * width), jnp.float32)],
        [token_counts, first, mlp, swap(mlp), ln_gains],
        [SMEM, VMEM, VMEM, VMEM, VMEM],
        flops=20 * count * width,
    )
    pooled = spread(pooled)

    kept, pick, own, base = call(
        mask_body,
        [
            shape(adj_values.shape),
            shape((tiles_here, tile_rows, slots)),
            shape((tiles_here, tile_rows, slots)),
            shape(cache_tiles.shape),
        ],
        [adj_tiles, me, got, mate_got, adj_values, cache_tiles],
        [SMEM, SMEM, VMEM, VMEM, VMEM, VMEM],
        flops=2 * adj_values.size * slots,
        scratch=[
            pltpu.VMEM(adj_values.shape, jnp.bfloat16),
            pltpu.VMEM((tiles_here, tile_rows, slots), jnp.bfloat16),
            pltpu.VMEM((tiles_here, tile_rows, slots), jnp.bfloat16),
            pltpu.VMEM(cache_tiles.shape, jnp.bfloat16),
            pltpu.SemaphoreType.DMA((tiles_here, 4)),
        ],
        out_specs=[HBM] * 4,
    )
    gathered = call(
        gather_body,
        [shape((tiles_here, tile_rows, half))],
        [adj_tiles, me, kept, cache_tiles, remote],
        [HBM, SMEM, HBM, HBM, VMEM],
        flops=2 * adj_values.size * half,
        scratch=[
            pltpu.SMEM(adj_tiles.shape, jnp.int32),
            pltpu.VMEM(kept.shape, jnp.bfloat16),
            pltpu.VMEM(cache_tiles.shape, jnp.bfloat16),
            pltpu.VMEM((2, entries, tile_rows, half), jnp.bfloat16),
            pltpu.VMEM((tiles_here, tile_rows, half), jnp.bfloat16),
            pltpu.SemaphoreType.DMA((3,)),
            pltpu.SemaphoreType.DMA((tiles_here,)),
        ],
        out_specs=[HBM],
    )
    gathered = gathered.reshape(nodes_here, half)
    picked = pick.reshape(nodes_here, slots)
    node_out, slope = call(
        forward_body,
        [shape((nodes_here, half)), shape((nodes_here, half))],
        [
            core, gathered, swap(gathered), w_gnn, w_other, out_grad,
            own.reshape(nodes_here, slots), base.reshape(nodes_here, half), picked, pooled,
        ],
        [SMEM] + [PULL] * 8 + [VMEM],
        flops=4 * nodes_here * half * half,
        scratch=[pltpu.VMEM((texts, width), jnp.bfloat16)],
    )
    grad_tiles = out_grad.reshape(tiles_here, tile_rows, half)
    slope_other = swap(slope)
    text_rows = up_to(2 * texts_here, 8)
    halves = (shards // 2, deep + text_rows, half)
    send, down = call(
        backward_body,
        [shape((shards, tile_rows, half)), shape((nodes_here, half))],
        [adj_tiles, me, core, slope, slope_other, w_gnn, adj_values],
        [SMEM, SMEM, SMEM] + [VMEM] * 4,
        flops=4 * nodes_here * half * half + 2 * adj_values.size * half,
        scratch=[
            pltpu.VMEM((nodes_here, half), jnp.bfloat16),
            pltpu.VMEM((shards + 1, tile_rows, half), jnp.bfloat16),
            pltpu.SemaphoreType.DMA((1,)),
            pltpu.SemaphoreType.DMA((shards,)),
        ],
        out_specs=[HBM] * 2,
    )
    returned = spread(send)
    keep, give = call(
        functools.partial(chunk_body, per, texts_here),
        [shape(halves), shape(halves)],
        [
            me, core, slope, slope_other, gathered, down, picked,
            own.reshape(nodes_here, slots), out_grad, pooled,
        ],
        [SMEM, SMEM] + [PULL] * 8,
        flops=4 * nodes_here * half * (half + slots),
        scratch=[
            pltpu.VMEM((width + ROWS, half), jnp.float32),
            pltpu.VMEM((slots, half), jnp.float32),
            pltpu.VMEM((texts, width), jnp.bfloat16),
            pltpu.VMEM((nodes_here, half), jnp.bfloat16),
        ],
    )
    local = call(
        local_body,
        [shape((tiles_here, tile_rows, half), jnp.float32)],
        [adj_tiles, me, down.reshape(tiles_here, tile_rows, half), adj_values, grad_tiles],
        [SMEM, SMEM] + [VMEM] * 3,
        flops=2 * adj_values.size * half,
    )
    reach = 1
    given = toward(give, reach)
    while 2 * reach < shards:
        part = (shards // (4 * reach), deep + text_rows, half)
        keep, give = call(
            functools.partial(fold_body, deep),
            [shape(part), shape(part)],
            [keep, given],
            [VMEM] * 2,
            flops=4 * math.prod(part),
        )
        reach = 2 * reach
        given = toward(give, reach)
    w_part, text_grad = call(
        functools.partial(close_body, deep),
        [shape((deep, half), jnp.float32), shape((texts_here, half), jnp.float32)],
        [keep, given],
        [VMEM] * 2,
        flops=1000,
    )
    node_grad = call(
        finish_body,
        [shape((tiles_here, tile_rows, half))],
        [me, asked, places(mate_got), local, returned],
        [SMEM, SMEM, SMEM, HBM, VMEM],
        flops=1000,
        scratch=[
            pltpu.VMEM((tiles_here, tile_rows, half), jnp.float32),
            pltpu.SemaphoreType.DMA((1,)),
        ],
    )
    return (node_out, w_part[:per].T, text_grad, node_grad.reshape(nodes_here, half))


def solution(mesh):
    placed = (
        P("graph", None, None),
        P("graph", None),
        P(None, None, "mp"),
        P("mp", None),
        P(None, "mp"),
        P("mp", None),
        P(),
        P("graph", "mp"),
        P("graph"),
        P("graph", None),
        P("graph", None, None, None),
        P("mp", None),
        P("graph", "mp"),
    )
    return jax.shard_map(
        step,
        mesh=mesh,
        in_specs=placed,
        out_specs=(P("graph", "mp"), P("mp", "graph"), P("graph", "mp"), P("graph", "mp")),
        check_vma=False,
    )
```

```python
import functools
import math

import jax
import jax.numpy as jnp
from jax import lax
from jax.experimental import pallas as pl
from jax.experimental.pallas import tpu as pltpu
from jax.sharding import PartitionSpec as P


HEAD = 64
LANES = 128
ROWS = 16
SPARE = 6 << 20
NORM_EPS = 1e-05
MASKED = -1e30
NO_NODE = -(1 << 20)
ROOT = 0.7978845608028654
CUBE = 0.044715

VMEM = pl.BlockSpec(memory_space=pltpu.VMEM)
HBM = pl.BlockSpec(memory_space=pltpu.HBM)
HELD = pl.BlockSpec(memory_space=pltpu.VMEM)
PULL = pl.BlockSpec(memory_space=pltpu.HBM)
SMEM = pl.BlockSpec(memory_space=pltpu.SMEM)


def up_to(value, unit):
    return (value + unit - 1) // unit * unit


def call(body, outs, ins, specs, flops, scratch=(), out_specs=None, aliases=None):
    moved = sum(a.size * a.dtype.itemsize for a in ins) + sum(
        o.size * o.dtype.itemsize for o in outs
    )
    many = len(outs) > 1
    ins = [
        pltpu.with_memory_space_constraint(a, pltpu.HBM) if s is HBM or s is PULL else a
        for a, s in zip(ins, specs, strict=True)
    ]
    ins = [
        pltpu.with_memory_space_constraint(a, pltpu.VMEM) if s is HELD else a
        for a, s in zip(ins, specs, strict=True)
    ]
    pulled = [i for i, s in enumerate(specs) if s is PULL]
    if pulled:
        body = pulling(body, pulled)
        scratch = list(scratch) + [pltpu.VMEM(ins[i].shape, ins[i].dtype) for i in pulled]
        scratch.append(pltpu.SemaphoreType.DMA((len(pulled),)))
    held = sum(math.prod(s.shape) * jnp.dtype(s.dtype).itemsize for s in scratch if counted(s))
    out_specs = out_specs or [VMEM] * len(outs)
    outs = [
        pltpu.HBM(o.shape, o.dtype) if s is HBM else o for o, s in zip(outs, out_specs, strict=True)
    ]
    return pl.pallas_call(
        body,
        out_shape=tuple(outs) if many else outs[0],
        in_specs=list(specs),
        out_specs=tuple(out_specs) if many else out_specs[0],
        scratch_shapes=list(scratch),
        input_output_aliases=aliases or {},
        compiler_params=pltpu.CompilerParams(vmem_limit_bytes=moved + moved // 8 + held + SPARE),
        cost_estimate=pl.CostEstimate(flops=flops, bytes_accessed=moved, transcendentals=0),
    )(*ins)


def counted(scratch):
    return jnp.issubdtype(scratch.dtype, jnp.number)


def copies(pairs, sems):
    started = [pltpu.make_async_copy(a, b, sems.at[i]) for i, (a, b) in enumerate(pairs)]
    for copy in started:
        copy.start()
    return started


def pulling(body, pulled):
    def wrapped(*refs):
        buffers, sems = refs[-len(pulled) - 1 : -1], refs[-1]
        held = list(refs[: -len(pulled) - 1])
        started = copies([(held[i], b) for i, b in zip(pulled, buffers)], sems)
        for i, buffer in zip(pulled, buffers):
            held[i] = buffer
        for copy in started:
            copy.wait()
        body(*held)

    return wrapped


def unroll(steps):
    return steps if steps <= 8 else 1


def shape(dims, dtype=jnp.bfloat16):
    return jax.ShapeDtypeStruct(tuple(dims), dtype)


def mm(a, b, dims=(1, 0)):
    return lax.dot_general(
        a, b, (((dims[0],), (dims[1],)), ((), ())), preferred_element_type=jnp.float32
    )


def tile_of(tile_id, tiles_here):
    safe = jnp.maximum(tile_id, 0)
    owner = lax.div(safe, jnp.int32(tiles_here))
    return safe, owner, safe - owner * tiles_here


def side_of(owner, me, peers):
    half = lax.div(owner, jnp.int32(peers))
    mine = lax.div(me, jnp.int32(peers))
    return jnp.where(half == mine, 0, 1), owner - half * peers


def index_body(texts_here, ids_hbm, self_ref, text_hbm, out_ref, ids_ref, text_ref, sems):
    for copy in copies([(ids_hbm, ids_ref), (text_hbm, text_ref)], sems):
        copy.wait()
    tiles_here, entries = ids_ref.shape
    peers, _, lanes = out_ref.shape
    shards = 2 * peers
    width = lanes - 2 * LANES
    texts = texts_here * shards
    me = self_ref[0]
    row = lax.broadcasted_iota(jnp.int32, (peers, LANES), 0)
    near = jnp.full((peers, LANES), -1, jnp.int32)
    far = near
    for r in range(tiles_here):
        for k in range(entries):
            tile_id = ids_ref[r, k]
            _, owner, place = tile_of(tile_id, tiles_here)
            side, spot = side_of(owner, me, peers)
            wanted = (tile_id >= 0) & (owner != me)
            near = jnp.where(row == jnp.where(wanted & (side == 0), spot, -1), place, near)
            far = jnp.where(row == jnp.where(wanted & (side == 1), spot, -1), place, far)
    out_ref[:, :, width : width + LANES] = near.reshape(peers, 1, LANES)
    out_ref[:, :, width + LANES :] = far.reshape(peers, 1, LANES)
    tile_rows = text_ref.shape[1]
    lane = lax.broadcasted_iota(jnp.int32, (LANES, tile_rows), 1)
    sub = lax.broadcasted_iota(jnp.int32, (LANES, LANES), 0)
    diagonal = sub == lax.broadcasted_iota(jnp.int32, (LANES, LANES), 1)
    for c in range(width // LANES):
        slot = c * LANES + lax.broadcasted_iota(jnp.int32, (LANES, 1), 0)
        part = lax.div(slot, jnp.int32(shards))
        text = jnp.where(slot < texts, (slot - part * shards) * texts_here + part, -5)
        best = jnp.full((LANES, tile_rows), NO_NODE, jnp.int32)
        for j in range(tiles_here):
            node = (me * tiles_here + j) * tile_rows + lane
            best = jnp.where(text_ref[j : j + 1, :] == text, node, best)
        column = jnp.max(best.astype(jnp.float32), axis=1, keepdims=True)
        line = jnp.max(jnp.where(diagonal, column, float(NO_NODE)), axis=0, keepdims=True)
        out_ref[:, :, c * LANES : (c + 1) * LANES] = (
            jnp.broadcast_to(line, (peers, LANES)).astype(jnp.int32).reshape(peers, 1, LANES)
        )


def pack_near_body(asked_ref, cache_hbm, out_hbm, tile_ref, in_sems, out_sems):
    copy = pltpu.make_async_copy(cache_hbm, tile_ref, in_sems.at[0])
    copy.start()
    copy.wait()
    place_tiles(0, asked_ref, tile_ref, out_hbm, out_sems)


def pack_far_body(asked_ref, mate_ref, near_hbm, out_hbm, out_sems):
    place_tiles(1, asked_ref, mate_ref, out_hbm, out_sems)


def place_tiles(side, asked_ref, tile_ref, out_hbm, out_sems):
    tile_rows = tile_ref.shape[1]
    peers = out_hbm.shape[0]

    def slot(p):
        place = jnp.maximum(asked_ref[p, side], 0)
        target = out_hbm.at[p, pl.ds(side * tile_rows, tile_rows), :]
        return pltpu.make_async_copy(tile_ref.at[place], target, out_sems.at[p])

    lax.fori_loop(0, peers, lambda p, c: (slot(p).start(), c)[1], 0)
    lax.fori_loop(0, peers, lambda p, c: (slot(p).wait(), c)[1], 0)


def mask_body(
    ids_ref, self_ref, got_ref, mate_ref, adj_ref, cache_ref, *refs
):
    outs, (kept_ref, pick_ref, own_ref, base_ref, sems) = refs[:4], refs[4:]
    tiles_here, entries, tile_rows, _ = adj_ref.shape
    peers, _, lanes = got_ref.shape
    width = lanes - 2 * LANES
    me = self_ref[0]
    both = jnp.maximum(got_ref[:, :, :width], mate_ref[:, :, :width])
    table = jnp.max(both.reshape(peers, width).astype(jnp.float32), axis=0, keepdims=True)
    place = lax.broadcasted_iota(jnp.int32, (tile_rows, width), 0).astype(jnp.float32)
    ones = jnp.ones((ROWS, width), jnp.bfloat16)
    sent = []

    def holds(tile_id):
        first = (tile_id * tile_rows).astype(jnp.float32)
        return jnp.where(table - first == place, 1.0, 0.0)

    for r in range(tiles_here):

        def one(k, total):
            tile_id = ids_ref[r, k]
            hot = holds(tile_id).astype(jnp.bfloat16)
            values = adj_ref[r, k]
            taken = mm(ones, hot, (1, 1))[0:1, :]
            keep = jnp.where(tile_id >= 0, 1.0, 0.0) * jnp.where(taken > 0.5, 0.0, 1.0)
            kept_ref[r, k] = (values.astype(jnp.float32) * keep).astype(jnp.bfloat16)
            return total + mm(values, hot)

        pick = lax.fori_loop(
            0, entries, one, jnp.zeros((tile_rows, width), jnp.float32), unroll=unroll(entries)
        )
        pick_ref[r] = pick.astype(jnp.bfloat16)
        hot = holds(me * tiles_here + r)
        own_ref[r] = hot.astype(jnp.bfloat16)
        fresh = jnp.max(hot, axis=1, keepdims=True)
        base_ref[r] = (cache_ref[r].astype(jnp.float32) * (1.0 - fresh)).astype(jnp.bfloat16)
        row = [(ref.at[r], out.at[r]) for ref, out in zip((kept_ref, pick_ref, own_ref, base_ref), outs)]
        sent = sent + copies(row, sems.at[r])
    for copy in sent:
        copy.wait()


def norm(values, gain):
    average = jnp.mean(values, axis=-1, keepdims=True)
    centred = values - average
    variance = jnp.mean(centred * centred, axis=-1, keepdims=True)
    return centred * lax.rsqrt(variance + NORM_EPS) * gain


def attend_body(
    seq, counts_ref, tokens_hbm, w_qkv_hbm, w_out_hbm, out_hbm,
    tokens_ref, w_qkv_ref, w_out_ref, out_ref, proj_ref, ctx_ref, in_sems, out_sems
):
    half = w_out_ref.shape[0]
    texts_here = tokens_ref.shape[0] // seq
    started = copies(
        [(tokens_hbm, tokens_ref)]
        + [(w_qkv_hbm.at[c], w_qkv_ref.at[c]) for c in range(3)]
        + [(w_out_hbm, w_out_ref)],
        in_sems,
    )
    started[0].wait()
    for c in range(3):
        started[1 + c].wait()
        proj_ref[:, c * half : (c + 1) * half] = mm(tokens_ref[...], w_qkv_ref[c]).astype(
            jnp.bfloat16
        )
    started[4].wait()
    sent = []
    left = lax.broadcasted_iota(jnp.int32, (seq, LANES), 1) < HEAD
    key_at = lax.broadcasted_iota(jnp.int32, (seq, seq), 1)
    for t in range(texts_here):
        rows = pl.ds(t * seq, seq)
        live = key_at < counts_ref[0, t]
        for pair in range(half // LANES):
            first = pair * LANES
            query = proj_ref[rows, first : first + LANES].astype(jnp.float32) * (HEAD**-0.5)
            key = proj_ref[rows, half + first : half + first + LANES]
            value = proj_ref[rows, 2 * half + first : 2 * half + first + LANES]
            sides = []
            for side in (left, jnp.logical_not(left)):
                scores = mm(jnp.where(side, query, 0.0).astype(jnp.bfloat16), key, (1, 1))
                scores = jnp.where(live, scores, MASKED)
                powers = jnp.exp(scores - jnp.max(scores, axis=-1, keepdims=True))
                total = jnp.sum(powers, axis=-1, keepdims=True)
                sides.append(mm((powers / total).astype(jnp.bfloat16), value))
            ctx_ref[rows, first : first + LANES] = jnp.where(left, sides[0], sides[1]).astype(
                jnp.bfloat16
            )
        out_ref[rows, :] = mm(ctx_ref[rows, :], w_out_ref[...]).astype(jnp.bfloat16)
        sent.append(pltpu.make_async_copy(out_ref.at[rows, :], out_hbm.at[rows, :], out_sems.at[t]))
        sent[-1].start()
    for copy in sent:
        copy.wait()


def inner_body(
    tokens_hbm, mine_hbm, other_hbm, up_hbm, down_hbm, gains_ref, first_ref, out_ref,
    inner_ref, tokens_ref, mine_ref, other_ref, up_ref, down_ref, sems
):
    started = copies(
        [
            (tokens_hbm, tokens_ref), (mine_hbm, mine_ref), (other_hbm, other_ref),
            (up_hbm, up_ref), (down_hbm, down_ref),
        ],
        sems,
    )
    for copy in started[:3]:
        copy.wait()
    added = mine_ref[...].astype(jnp.float32) + other_ref[...].astype(jnp.float32)
    first = norm(tokens_ref[...].astype(jnp.float32) + added, gains_ref[0:1, :])
    first_ref[...] = first.astype(jnp.bfloat16)
    started[3].wait()
    hidden_units = up_ref.shape[1]
    step = hidden_units // 4
    for c in range(4):
        cols = slice(c * step, (c + 1) * step)
        value = mm(first_ref[...], up_ref[:, cols])
        gate = jnp.tanh(ROOT * (value + CUBE * (value * value * value)))
        inner_ref[:, cols] = (0.5 * value * (1.0 + gate)).astype(jnp.bfloat16)
    started[4].wait()
    out_ref[...] = mm(inner_ref[...], down_ref[...]).astype(jnp.bfloat16)


def pool_body(seq, counts_ref, first_ref, mine_ref, other_ref, gains_ref, out_ref):
    texts_here, width = first_ref.shape[0] // seq, first_ref.shape[1]
    for t in range(texts_here):
        rows = slice(t * seq, (t + 1) * seq)
        added = mine_ref[rows, :].astype(jnp.float32) + other_ref[rows, :].astype(jnp.float32)
        second = norm(first_ref[rows, :].astype(jnp.float32) + added, gains_ref[1:2, :])
        count = counts_ref[0, t]
        live = lax.broadcasted_iota(jnp.int32, (seq, 1), 0) < count
        total = jnp.sum(jnp.where(live, second, 0.0), axis=0, keepdims=True)
        pooled = (total / count.astype(jnp.float32)).astype(jnp.bfloat16).astype(jnp.float32)
        out_ref[:, :, t * width : (t + 1) * width] = pooled.reshape(1, 1, width)


def pooled_rows(me, near_ref, far_ref, width):
    shards = 2 * near_ref.shape[0]
    parts = []
    for first in range(0, near_ref.shape[2], width):
        for ref in (near_ref, far_ref):
            part = ref[:, :, first : first + width].reshape(shards // 2, width)
            parts.append(part.astype(jnp.bfloat16))
    stacked = jnp.concatenate(parts, axis=0)
    texts = stacked.shape[0]
    row = lax.broadcasted_iota(jnp.int32, (texts, texts), 0)
    column = lax.broadcasted_iota(jnp.int32, (texts, texts), 1)
    place = column & (shards - 1)
    offset = jnp.zeros_like(place)
    reach = 1
    while reach < shards:
        offset = 2 * offset + (place & 1)
        place = lax.shift_right_logical(place, 1)
        reach *= 2
    source = column - (column & (shards - 1)) + (offset ^ me)
    order = jnp.where(row == source, 1.0, 0.0).astype(jnp.bfloat16)
    return mm(order, stacked).astype(jnp.bfloat16)


def gather_body(
    ids_hbm, self_ref, kept_hbm, cache_hbm, remote_ref, out_ref,
    ids_ref, kept_ref, cache_ref, source_ref, sems
):
    started = copies([(ids_hbm, ids_ref), (cache_hbm, cache_ref), (kept_hbm, kept_ref)], sems)
    tiles_here, entries, tile_rows, _ = kept_ref.shape
    me = self_ref[0]
    started[0].wait()
    started[1].wait()

    def fetch(r, k):
        tile_id = ids_ref[r, k]
        _, owner, place = tile_of(tile_id, tiles_here)
        local = (owner == me) | (tile_id < 0)

        @pl.when(local)
        def _():
            source_ref[r % 2, k] = cache_ref[place]

        @pl.when(jnp.logical_not(local))
        def _():
            side, spot = side_of(owner, me, remote_ref.shape[0])
            first = pl.multiple_of(side * tile_rows, tile_rows)
            source_ref[r % 2, k] = remote_ref[spot, pl.ds(first, tile_rows), :]

    for r in range(tiles_here):
        lax.fori_loop(
            0, entries, lambda k, c: (fetch(r, k), c)[1], 0, unroll=unroll(entries)
        )
        if r == 0:
            started[2].wait()
        total = jnp.zeros(out_ref.shape[1:], jnp.float32)
        for k in range(entries):
            total = total + mm(kept_ref[r, k], source_ref[r % 2, k])
        out_ref[r] = total.astype(jnp.bfloat16)


def forward_body(
    self_ref, core_ref, mine_ref, other_ref, w_own_ref, w_other_ref, grad_ref, own_ref, base_ref,
    pick_ref, near_ref, far_ref, node_hbm, slope_ref, agg_hbm, slope_hbm,
    rows_ref, node_ref, agg_ref, node_sems, agg_sems, slope_sems
):
    half = mine_ref.shape[1]
    start = pl.multiple_of(core_ref[0] * half, LANES)
    far = pl.multiple_of((1 - core_ref[0]) * half, LANES)
    rows_ref[...] = pooled_rows(self_ref[0], near_ref, far_ref, rows_ref.shape[1])
    texts = rows_ref.shape[0]
    here = rows_ref[:, pl.ds(start, half)]
    w_own = w_own_ref[:, pl.ds(start, half)]
    w_other = w_other_ref[:, pl.ds(start, half)]
    moved = (mm(here, w_own) + mm(rows_ref[:, pl.ds(far, half)], w_other)).astype(jnp.bfloat16)
    blocks = node_sems.shape[0]
    step = mine_ref.shape[0] // blocks
    sent = []
    for block in range(blocks):
        at = pl.ds(block * step, step)
        pick = pick_ref[at, :][:, :texts]
        hidden = mm(mine_ref[at, :], w_own) + mm(other_ref[at, :], w_other) + mm(pick, moved)
        square = hidden * hidden
        gate = jnp.tanh(ROOT * hidden * (1.0 + CUBE * square))
        lifted = 0.5 * (1.0 + gate)
        slope = lifted + 0.5 * hidden * (1.0 - gate * gate) * (ROOT * (1.0 + 3.0 * CUBE * square))
        slope_ref[at, :] = (grad_ref[at, :].astype(jnp.float32) * slope).astype(jnp.bfloat16)
        fresh = mm(own_ref[at, :][:, :texts], here)
        node_ref[at, :] = (base_ref[at, :].astype(jnp.float32) + fresh + hidden * lifted).astype(
            jnp.bfloat16
        )
        agg_ref[at, :] = (mine_ref[at, :].astype(jnp.float32) + mm(pick, here)).astype(jnp.bfloat16)
        sent += copies([(node_ref.at[at, :], node_hbm.at[at, :])], node_sems.at[pl.ds(block, 1)])
        sent += copies([(agg_ref.at[at, :], agg_hbm.at[at, :])], agg_sems.at[pl.ds(block, 1)])
        sent += copies([(slope_ref.at[at, :], slope_hbm.at[at, :])], slope_sems.at[pl.ds(block, 1)])
    for copy in sent:
        copy.wait()


def chunk_body(
    per, texts_here, self_ref, core_ref, mine_ref, other_ref, agg_ref, down_ref, pick_ref, own_ref,
    grad_ref, keep_ref, give_ref, w_ref, text_ref
):
    kept, _, half = keep_ref.shape
    shards = 2 * kept
    deep = up_to(per, ROWS)
    text_rows = keep_ref.shape[1] - deep
    me = self_ref[0]
    own = pl.multiple_of(core_ref[0] * half, LANES)
    far = pl.multiple_of((1 - core_ref[0]) * half, LANES)
    columns = 2 * half
    text_ref[...] = mm(pick_ref[...], down_ref[...], (0, 0)) + mm(
        own_ref[...], grad_ref[...], (0, 0)
    )
    w_ref[pl.ds(own, half), :] = mm(mine_ref[...], agg_ref[...], (0, 0))
    w_ref[pl.ds(far, half), :] = mm(other_ref[...], agg_ref[...], (0, 0))
    w_ref[columns:, :] = jnp.zeros((w_ref.shape[0] - columns, half), jnp.float32)
    row = lax.broadcasted_iota(jnp.int32, (text_rows, half), 0)
    for q in range(shards):
        piece = w_ref[q * per : q * per + deep, :].astype(jnp.bfloat16)
        block = jnp.zeros((text_rows, half), jnp.float32)
        for i in range(texts_here):
            line = text_ref[i * shards + q : i * shards + q + 1, :]
            high = line.astype(jnp.bfloat16).astype(jnp.float32)
            block = jnp.where(row == i, high, block)
            block = jnp.where(row == text_rows // 2 + i, line - high, block)
        block = block.astype(jnp.bfloat16)
        step = q ^ me
        turned = step * 0
        reach = 1
        while reach < shards:
            turned = 2 * turned + ((step // reach) & 1)
            reach *= 2

        @pl.when(turned < kept)
        def _():
            keep_ref[turned, :deep, :] = piece
            keep_ref[turned, deep:, :] = block

        @pl.when(turned >= kept)
        def _():
            give_ref[turned - kept, :deep, :] = piece
            give_ref[turned - kept, deep:, :] = block


def backward_body(
    ids_ref, self_ref, core_ref, mine_ref, other_ref, w_own_ref, adj_ref, send_hbm, down_hbm,
    down_ref, send_ref, sems, slot_sems
):
    tiles_here, entries, tile_rows, _ = adj_ref.shape
    shards, _, half = send_hbm.shape
    me = self_ref[0]
    core = core_ref[0]
    own = pl.multiple_of(core * half, LANES)
    far = pl.multiple_of((1 - core) * half, LANES)
    down = mm(mine_ref[...], w_own_ref[:, pl.ds(own, half)], (1, 1)) + mm(
        other_ref[...], w_own_ref[:, pl.ds(far, half)], (1, 1)
    )
    down_ref[...] = down.astype(jnp.bfloat16)
    down_copy = pltpu.make_async_copy(down_ref, down_hbm, sems.at[0])
    down_copy.start()
    for r in range(tiles_here):
        rows = slice(r * tile_rows, (r + 1) * tile_rows)
        for first in range(0, entries, 6):
            group = range(first, min(first + 6, entries))
            side_by_side = jnp.concatenate([adj_ref[r, k] for k in group], axis=1)
            product = mm(side_by_side, down_ref[rows, :], (0, 0)).astype(jnp.bfloat16)
            for k in group:
                tile_id = ids_ref[r, k]
                _, owner, _ = tile_of(tile_id, tiles_here)
                slot = jnp.where((tile_id >= 0) & (owner != me), owner, shards)
                send_ref[slot] = product[(k - first) * tile_rows : (k - first + 1) * tile_rows]
    for copy in copies([(send_ref.at[q], send_hbm.at[q]) for q in range(shards)], slot_sems):
        copy.wait()
    down_copy.wait()


def fold(mine, theirs, deep):
    total = mine.astype(jnp.float32) + theirs.astype(jnp.float32)
    lines = (total.shape[0] - deep) // 2
    return total[:deep, :], total[deep : deep + lines, :] + total[deep + lines :, :]


def fold_body(deep, mine_ref, theirs_ref, keep_ref, give_ref):
    kept = keep_ref.shape[0]
    for s in range(2 * kept):
        w_sum, text = fold(mine_ref[s], theirs_ref[s], deep)
        high = text.astype(jnp.bfloat16).astype(jnp.float32)
        out_ref = (keep_ref if s < kept else give_ref).at[s % kept]
        out_ref[:deep, :] = w_sum.astype(jnp.bfloat16)
        out_ref[deep:, :] = jnp.concatenate([high, text - high], axis=0).astype(jnp.bfloat16)


def close_body(deep, mine_ref, theirs_ref, w_ref, text_ref):
    w_sum, text = fold(mine_ref[0], theirs_ref[0], deep)
    w_ref[...] = w_sum
    text_ref[...] = text[: text_ref.shape[0], :]


def local_body(ids_ref, self_ref, down_ref, adj_ref, grad_ref, local_ref):
    tiles_here, entries, _, _ = adj_ref.shape
    me = self_ref[0]
    local_ref[...] = grad_ref[...].astype(jnp.float32)
    for r in range(tiles_here):

        def one(k, carry):
            tile_id = ids_ref[r, k]
            _, owner, place = tile_of(tile_id, tiles_here)

            @pl.when((tile_id >= 0) & (owner == me))
            def _():
                local_ref[place] += mm(adj_ref[r, k], down_ref[r], (0, 0))

            return carry

        lax.fori_loop(0, entries, one, 0, unroll=unroll(entries))


def finish_body(self_ref, asked_ref, mate_ref, local_hbm, got_ref, node_ref, sum_ref, sems):
    local = pltpu.make_async_copy(local_hbm, sum_ref, sems.at[0])
    local.start()
    shards = got_ref.shape[0]
    me = self_ref[0]
    local.wait()

    def one(q, carry):
        side, spot = side_of(q, me, shards // 2)
        asked = jnp.where(side == 0, asked_ref[spot, 0], mate_ref[spot, 1])

        @pl.when(asked >= 0)
        def _():
            sum_ref[asked] += got_ref[q].astype(jnp.float32)

        return carry

    lax.fori_loop(0, shards, one, 0)
    node_ref[...] = sum_ref[...].astype(jnp.bfloat16)


def step(
    tokens, token_counts, w_qkv, w_out, w_up, w_down, ln_gains, cache, node_text, adj_tiles,
    adj_values, w_gnn, out_grad
):
    shards = lax.axis_size("graph")
    cores = lax.axis_size("mp")
    me = lax.axis_index("graph").astype(jnp.int32).reshape(1)
    core_at = lax.axis_index("mp")
    core = core_at.astype(jnp.int32).reshape(1)
    texts_here, seq, width = tokens.shape
    nodes_here, half = cache.shape
    tiles_here, entries, tile_rows = adj_values.shape[:3]
    texts = texts_here * shards
    slots = up_to(texts, LANES)
    per = width // shards
    deep = up_to(per, ROWS)
    count = texts_here * seq
    inner = w_up.shape[1]

    def swap(values):
        return lax.ppermute(values, "mp", [(i, cores - 1 - i) for i in range(cores)])

    def toward(values, reach):
        return lax.ppermute(values, "graph", [(i, i ^ reach) for i in range(shards)])

    peers = shards // 2

    def spread(values, groups=None):
        return lax.all_to_all(
            values, "graph", split_axis=0, concat_axis=0, tiled=True, axis_index_groups=groups
        )

    halves_of = [list(range(peers)), list(range(peers, shards))]

    cache_tiles = cache.reshape(tiles_here, tile_rows, half)
    mate_tiles = toward(cache_tiles, peers)
    index = call(
        functools.partial(index_body, texts_here),
        [shape((peers, 1, slots + 2 * LANES), jnp.int32)],
        [adj_tiles, me, node_text.reshape(tiles_here, tile_rows)],
        [HBM, SMEM, HBM],
        flops=1000,
        scratch=[
            pltpu.SMEM(adj_tiles.shape, jnp.int32),
            pltpu.VMEM((tiles_here, tile_rows), jnp.int32),
            pltpu.SemaphoreType.DMA((2,)),
        ],
    )
    got = spread(index, halves_of)
    mate_got = toward(got, peers)

    def places(table):
        return table[:, 0, slots:].reshape(peers, 2, LANES)[:, :, 0]

    asked = places(got)
    packed = call(
        pack_near_body,
        [shape((peers, 2 * tile_rows, half))],
        [asked, cache_tiles],
        [SMEM, HBM],
        flops=1000,
        scratch=[
            pltpu.VMEM(cache_tiles.shape, jnp.bfloat16),
            pltpu.SemaphoreType.DMA((1,)),
            pltpu.SemaphoreType.DMA((peers,)),
        ],
        out_specs=[HBM],
    )
    packed = call(
        pack_far_body,
        [shape((peers, 2 * tile_rows, half))],
        [asked, mate_tiles, packed],
        [SMEM, VMEM, HBM],
        flops=1000,
        scratch=[pltpu.SemaphoreType.DMA((peers,))],
        out_specs=[HBM],
        aliases={2: 0},
    )
    remote = spread(packed, halves_of)

    w_other = swap(w_gnn)

    flat_tokens = tokens.reshape(count, width)
    partial = call(
        functools.partial(attend_body, seq),
        [shape((count, width))],
        [token_counts, flat_tokens, jnp.transpose(w_qkv, (1, 0, 2)), w_out],
        [SMEM, HBM, HBM, HBM],
        flops=2 * count * (width * 3 * half + half * width + 2 * seq * half * 2),
        scratch=[
            pltpu.VMEM((count, width), jnp.bfloat16),
            pltpu.VMEM((3, width, half), jnp.bfloat16),
            pltpu.VMEM((half, width), jnp.bfloat16),
            pltpu.VMEM((count, width), jnp.bfloat16),
            pltpu.VMEM((count, 3 * half), jnp.bfloat16),
            pltpu.VMEM((count, half), jnp.bfloat16),
            pltpu.SemaphoreType.DMA((5,)),
            pltpu.SemaphoreType.DMA((texts_here,)),
        ],
        out_specs=[HBM],
    )
    first, mlp = call(
        inner_body,
        [shape((count, width)), shape((count, width))],
        [flat_tokens, partial, swap(partial), w_up, w_down, ln_gains],
        [HBM] * 5 + [VMEM],
        flops=4 * count * width * inner,
        scratch=[
            pltpu.VMEM((count, inner), jnp.bfloat16),
            pltpu.VMEM((count, width), jnp.bfloat16),
            pltpu.VMEM((count, width), jnp.bfloat16),
            pltpu.VMEM((count, width), jnp.bfloat16),
            pltpu.VMEM((width, inner), jnp.bfloat16),
            pltpu.VMEM((inner, width), jnp.bfloat16),
            pltpu.SemaphoreType.DMA((5,)),
        ],
    )
    pooled = call(
        functools.partial(pool_body, seq),
        [shape((1, 1, texts_here * width), jnp.float32)],
        [token_counts, first, mlp, swap(mlp), ln_gains],
        [SMEM, VMEM, VMEM, VMEM, VMEM],
        flops=20 * count * width,
    )
    near = pooled
    reach = peers
    far = toward(near, reach)
    while reach > 1:
        reach = reach // 2
        near = jnp.concatenate([near, far], axis=0)
        far = toward(near, reach)

    kept, pick, own, base = call(
        mask_body,
        [
            shape(adj_values.shape),
            shape((tiles_here, tile_rows, slots)),
            shape((tiles_here, tile_rows, slots)),
            shape(cache_tiles.shape),
        ],
        [adj_tiles, me, got, mate_got, adj_values, cache_tiles],
        [SMEM, SMEM, VMEM, VMEM, VMEM, VMEM],
        flops=2 * adj_values.size * slots,
        scratch=[
            pltpu.VMEM(adj_values.shape, jnp.bfloat16),
            pltpu.VMEM((tiles_here, tile_rows, slots), jnp.bfloat16),
            pltpu.VMEM((tiles_here, tile_rows, slots), jnp.bfloat16),
            pltpu.VMEM(cache_tiles.shape, jnp.bfloat16),
            pltpu.SemaphoreType.DMA((tiles_here, 4)),
        ],
        out_specs=[HBM] * 4,
    )
    gathered = call(
        gather_body,
        [shape((tiles_here, tile_rows, half))],
        [adj_tiles, me, kept, cache_tiles, remote],
        [HBM, SMEM, HBM, HBM, VMEM],
        flops=2 * adj_values.size * half,
        scratch=[
            pltpu.SMEM(adj_tiles.shape, jnp.int32),
            pltpu.VMEM(kept.shape, jnp.bfloat16),
            pltpu.VMEM(cache_tiles.shape, jnp.bfloat16),
            pltpu.VMEM((2, entries, tile_rows, half), jnp.bfloat16),
            pltpu.SemaphoreType.DMA((3,)),
        ],
    )
    gathered = gathered.reshape(nodes_here, half)
    picked = pick.reshape(nodes_here, slots)
    node_out, slope, aggregate, slope_kept = call(
        forward_body,
        [shape((nodes_here, half))] * 4,
        [
            me, core, gathered, swap(gathered), w_gnn, w_other, out_grad,
            own.reshape(nodes_here, slots), base.reshape(nodes_here, half), picked, near, far,
        ],
        [SMEM, SMEM, HELD, HELD] + [VMEM] * 8,
        flops=4 * nodes_here * half * half,
        scratch=[
            pltpu.VMEM((texts, width), jnp.bfloat16),
            pltpu.VMEM((nodes_here, half), jnp.bfloat16),
            pltpu.VMEM((nodes_here, half), jnp.bfloat16),
            pltpu.SemaphoreType.DMA((tiles_here,)),
            pltpu.SemaphoreType.DMA((tiles_here,)),
            pltpu.SemaphoreType.DMA((tiles_here,)),
        ],
        out_specs=[HBM, VMEM, HBM, HBM],
    )
    grad_tiles = out_grad.reshape(tiles_here, tile_rows, half)
    slope_other = swap(slope)
    text_rows = up_to(2 * texts_here, 8)
    halves = (shards // 2, deep + text_rows, half)
    send, down = call(
        backward_body,
        [shape((shards, tile_rows, half)), shape((nodes_here, half))],
        [adj_tiles, me, core, slope, slope_other, w_gnn, adj_values],
        [SMEM, SMEM, SMEM] + [VMEM] * 4,
        flops=4 * nodes_here * half * half + 2 * adj_values.size * half,
        scratch=[
            pltpu.VMEM((nodes_here, half), jnp.bfloat16),
            pltpu.VMEM((shards + 1, tile_rows, half), jnp.bfloat16),
            pltpu.SemaphoreType.DMA((1,)),
            pltpu.SemaphoreType.DMA((shards,)),
        ],
        out_specs=[HBM] * 2,
    )
    returned = spread(send)
    keep, give = call(
        functools.partial(chunk_body, per, texts_here),
        [shape(halves), shape(halves)],
        [
            me, core, slope_kept, slope_other, aggregate, down, picked,
            own.reshape(nodes_here, slots), out_grad,
        ],
        [SMEM, SMEM] + [PULL] * 7,
        flops=4 * nodes_here * half * (half + slots),
        scratch=[
            pltpu.VMEM((width + ROWS, half), jnp.float32),
            pltpu.VMEM((slots, half), jnp.float32),
        ],
    )
    local = call(
        local_body,
        [shape((tiles_here, tile_rows, half), jnp.float32)],
        [adj_tiles, me, down.reshape(tiles_here, tile_rows, half), adj_values, grad_tiles],
        [SMEM, SMEM] + [VMEM] * 3,
        flops=2 * adj_values.size * half,
    )
    reach = 1
    given = toward(give, reach)
    while 2 * reach < shards:
        part = (shards // (4 * reach), deep + text_rows, half)
        keep, give = call(
            functools.partial(fold_body, deep),
            [shape(part), shape(part)],
            [keep, given],
            [VMEM] * 2,
            flops=4 * math.prod(part),
        )
        reach = 2 * reach
        given = toward(give, reach)
    w_part, text_grad = call(
        functools.partial(close_body, deep),
        [shape((deep, half), jnp.float32), shape((texts_here, half), jnp.float32)],
        [keep, given],
        [VMEM] * 2,
        flops=1000,
    )
    node_grad = call(
        finish_body,
        [shape((tiles_here, tile_rows, half))],
        [me, asked, places(mate_got), local, returned],
        [SMEM, SMEM, SMEM, HBM, VMEM],
        flops=1000,
        scratch=[
            pltpu.VMEM((tiles_here, tile_rows, half), jnp.float32),
            pltpu.SemaphoreType.DMA((1,)),
        ],
    )
    return (node_out, w_part[:per].T, text_grad, node_grad.reshape(nodes_here, half))


def solution(mesh):
    placed = (
        P("graph", None, None),
        P("graph", None),
        P(None, None, "mp"),
        P("mp", None),
        P(None, "mp"),
        P("mp", None),
        P(),
        P("graph", "mp"),
        P("graph"),
        P("graph", None),
        P("graph", None, None, None),
        P("mp", None),
        P("graph", "mp"),
    )
    return jax.shard_map(
        step,
        mesh=mesh,
        in_specs=placed,
        out_specs=(P("graph", "mp"), P("mp", "graph"), P("graph", "mp"), P("graph", "mp")),
        check_vma=False,
    )
```

```python
import functools
import math

import jax
import jax.numpy as jnp
from jax import lax
from jax.experimental import pallas as pl
from jax.experimental.pallas import tpu as pltpu
from jax.sharding import PartitionSpec as P


HEAD = 64
LANES = 128
ROWS = 16
SPARE = 6 << 20
NORM_EPS = 1e-05
MASKED = -1e30
NO_NODE = -(1 << 20)
ROOT = 0.7978845608028654
CUBE = 0.044715

VMEM = pl.BlockSpec(memory_space=pltpu.VMEM)
HBM = pl.BlockSpec(memory_space=pltpu.HBM)
HELD = pl.BlockSpec(memory_space=pltpu.VMEM)
PULL = pl.BlockSpec(memory_space=pltpu.HBM)
SMEM = pl.BlockSpec(memory_space=pltpu.SMEM)


def up_to(value, unit):
    return (value + unit - 1) // unit * unit


def call(body, outs, ins, specs, flops, scratch=(), out_specs=None, aliases=None):
    moved = sum(a.size * a.dtype.itemsize for a in ins) + sum(
        o.size * o.dtype.itemsize for o in outs
    )
    many = len(outs) > 1
    ins = [
        pltpu.with_memory_space_constraint(a, pltpu.HBM) if s is HBM or s is PULL else a
        for a, s in zip(ins, specs, strict=True)
    ]
    ins = [
        pltpu.with_memory_space_constraint(a, pltpu.VMEM) if s is HELD else a
        for a, s in zip(ins, specs, strict=True)
    ]
    pulled = [i for i, s in enumerate(specs) if s is PULL]
    if pulled:
        body = pulling(body, pulled)
        scratch = list(scratch) + [pltpu.VMEM(ins[i].shape, ins[i].dtype) for i in pulled]
        scratch.append(pltpu.SemaphoreType.DMA((len(pulled),)))
    held = sum(math.prod(s.shape) * jnp.dtype(s.dtype).itemsize for s in scratch if counted(s))
    out_specs = out_specs or [VMEM] * len(outs)
    outs = [
        pltpu.HBM(o.shape, o.dtype) if s is HBM else o for o, s in zip(outs, out_specs, strict=True)
    ]
    return pl.pallas_call(
        body,
        out_shape=tuple(outs) if many else outs[0],
        in_specs=list(specs),
        out_specs=tuple(out_specs) if many else out_specs[0],
        scratch_shapes=list(scratch),
        input_output_aliases=aliases or {},
        compiler_params=pltpu.CompilerParams(vmem_limit_bytes=moved + moved // 8 + held + SPARE),
        cost_estimate=pl.CostEstimate(flops=flops, bytes_accessed=moved, transcendentals=0),
    )(*ins)


def counted(scratch):
    return jnp.issubdtype(scratch.dtype, jnp.number)


def copies(pairs, sems):
    started = [pltpu.make_async_copy(a, b, sems.at[i]) for i, (a, b) in enumerate(pairs)]
    for copy in started:
        copy.start()
    return started


def pulling(body, pulled):
    def wrapped(*refs):
        buffers, sems = refs[-len(pulled) - 1 : -1], refs[-1]
        held = list(refs[: -len(pulled) - 1])
        started = copies([(held[i], b) for i, b in zip(pulled, buffers)], sems)
        for i, buffer in zip(pulled, buffers):
            held[i] = buffer
        for copy in started:
            copy.wait()
        body(*held)

    return wrapped


def unroll(steps):
    return steps if steps <= 8 else 1


def shape(dims, dtype=jnp.bfloat16):
    return jax.ShapeDtypeStruct(tuple(dims), dtype)


def mm(a, b, dims=(1, 0)):
    return lax.dot_general(
        a, b, (((dims[0],), (dims[1],)), ((), ())), preferred_element_type=jnp.float32
    )


def tile_of(tile_id, tiles_here):
    safe = jnp.maximum(tile_id, 0)
    owner = lax.div(safe, jnp.int32(tiles_here))
    return safe, owner, safe - owner * tiles_here


def side_of(owner, me, peers):
    half = lax.div(owner, jnp.int32(peers))
    mine = lax.div(me, jnp.int32(peers))
    return jnp.where(half == mine, 0, 1), owner - half * peers


def index_body(texts_here, ids_hbm, self_ref, text_hbm, out_ref, ids_ref, text_ref, sems):
    for copy in copies([(ids_hbm, ids_ref), (text_hbm, text_ref)], sems):
        copy.wait()
    tiles_here, entries = ids_ref.shape
    peers, _, lanes = out_ref.shape
    shards = 2 * peers
    width = lanes - 2 * LANES
    texts = texts_here * shards
    me = self_ref[0]
    row = lax.broadcasted_iota(jnp.int32, (peers, LANES), 0)
    near = jnp.full((peers, LANES), -1, jnp.int32)
    far = near
    for r in range(tiles_here):
        for k in range(entries):
            tile_id = ids_ref[r, k]
            _, owner, place = tile_of(tile_id, tiles_here)
            side, spot = side_of(owner, me, peers)
            wanted = (tile_id >= 0) & (owner != me)
            near = jnp.where(row == jnp.where(wanted & (side == 0), spot, -1), place, near)
            far = jnp.where(row == jnp.where(wanted & (side == 1), spot, -1), place, far)
    out_ref[:, :, width : width + LANES] = near.reshape(peers, 1, LANES)
    out_ref[:, :, width + LANES :] = far.reshape(peers, 1, LANES)
    tile_rows = text_ref.shape[1]
    lane = lax.broadcasted_iota(jnp.int32, (LANES, tile_rows), 1)
    sub = lax.broadcasted_iota(jnp.int32, (LANES, LANES), 0)
    diagonal = sub == lax.broadcasted_iota(jnp.int32, (LANES, LANES), 1)
    for c in range(width // LANES):
        slot = c * LANES + lax.broadcasted_iota(jnp.int32, (LANES, 1), 0)
        part = lax.div(slot, jnp.int32(shards))
        text = jnp.where(slot < texts, (slot - part * shards) * texts_here + part, -5)
        best = jnp.full((LANES, tile_rows), NO_NODE, jnp.int32)
        for j in range(tiles_here):
            node = (me * tiles_here + j) * tile_rows + lane
            best = jnp.where(text_ref[j : j + 1, :] == text, node, best)
        column = jnp.max(best.astype(jnp.float32), axis=1, keepdims=True)
        line = jnp.max(jnp.where(diagonal, column, float(NO_NODE)), axis=0, keepdims=True)
        out_ref[:, :, c * LANES : (c + 1) * LANES] = (
            jnp.broadcast_to(line, (peers, LANES)).astype(jnp.int32).reshape(peers, 1, LANES)
        )


def pack_near_body(asked_ref, cache_hbm, out_hbm, tile_ref, in_sems, out_sems):
    copy = pltpu.make_async_copy(cache_hbm, tile_ref, in_sems.at[0])
    copy.start()
    copy.wait()
    place_tiles(0, asked_ref, tile_ref, out_hbm, out_sems)


def pack_far_body(asked_ref, mate_ref, near_hbm, out_hbm, out_sems):
    place_tiles(1, asked_ref, mate_ref, out_hbm, out_sems)


def place_tiles(side, asked_ref, tile_ref, out_hbm, out_sems):
    tile_rows = tile_ref.shape[1]
    peers = out_hbm.shape[0]

    def slot(p):
        place = jnp.maximum(asked_ref[p, side], 0)
        target = out_hbm.at[p, pl.ds(side * tile_rows, tile_rows), :]
        return pltpu.make_async_copy(tile_ref.at[place], target, out_sems.at[p])

    lax.fori_loop(0, peers, lambda p, c: (slot(p).start(), c)[1], 0)
    lax.fori_loop(0, peers, lambda p, c: (slot(p).wait(), c)[1], 0)


def mask_body(
    ids_ref, self_ref, got_ref, mate_ref, adj_ref, cache_ref, *refs
):
    outs, (kept_ref, pick_ref, own_ref, base_ref, sems) = refs[:4], refs[4:]
    tiles_here, entries, tile_rows, _ = adj_ref.shape
    peers, _, lanes = got_ref.shape
    width = lanes - 2 * LANES
    me = self_ref[0]
    both = jnp.maximum(got_ref[:, :, :width], mate_ref[:, :, :width])
    table = jnp.max(both.reshape(peers, width).astype(jnp.float32), axis=0, keepdims=True)
    place = lax.broadcasted_iota(jnp.int32, (tile_rows, width), 0).astype(jnp.float32)
    ones = jnp.ones((ROWS, width), jnp.bfloat16)
    sent = []

    def holds(tile_id):
        first = (tile_id * tile_rows).astype(jnp.float32)
        return jnp.where(table - first == place, 1.0, 0.0)

    for r in range(tiles_here):

        def one(k, total):
            tile_id = ids_ref[r, k]
            hot = holds(tile_id).astype(jnp.bfloat16)
            values = adj_ref[r, k]
            taken = mm(ones, hot, (1, 1))[0:1, :]
            keep = jnp.where(tile_id >= 0, 1.0, 0.0) * jnp.where(taken > 0.5, 0.0, 1.0)
            kept_ref[r, k] = (values.astype(jnp.float32) * keep).astype(jnp.bfloat16)
            return total + mm(values, hot)

        pick = lax.fori_loop(
            0, entries, one, jnp.zeros((tile_rows, width), jnp.float32), unroll=unroll(entries)
        )
        pick_ref[r] = pick.astype(jnp.bfloat16)
        hot = holds(me * tiles_here + r)
        own_ref[r] = hot.astype(jnp.bfloat16)
        fresh = jnp.max(hot, axis=1, keepdims=True)
        base_ref[r] = (cache_ref[r].astype(jnp.float32) * (1.0 - fresh)).astype(jnp.bfloat16)
        row = [(ref.at[r], out.at[r]) for ref, out in zip((kept_ref, pick_ref, own_ref, base_ref), outs)]
        sent = sent + copies(row, sems.at[r])
    for copy in sent:
        copy.wait()


def norm(values, gain):
    average = jnp.mean(values, axis=-1, keepdims=True)
    centred = values - average
    variance = jnp.mean(centred * centred, axis=-1, keepdims=True)
    return centred * lax.rsqrt(variance + NORM_EPS) * gain


def attend_body(
    seq, counts_ref, tokens_hbm, w_qkv_hbm, w_out_hbm, out_hbm,
    tokens_ref, w_qkv_ref, w_out_ref, out_ref, proj_ref, ctx_ref, in_sems, out_sems
):
    half = w_out_ref.shape[0]
    texts_here = tokens_ref.shape[0] // seq
    started = copies(
        [(tokens_hbm, tokens_ref)]
        + [(w_qkv_hbm.at[c], w_qkv_ref.at[c]) for c in range(3)]
        + [(w_out_hbm, w_out_ref)],
        in_sems,
    )
    started[0].wait()
    for c in range(3):
        started[1 + c].wait()
        proj_ref[:, c * half : (c + 1) * half] = mm(tokens_ref[...], w_qkv_ref[c]).astype(
            jnp.bfloat16
        )
    started[4].wait()
    sent = []
    left = lax.broadcasted_iota(jnp.int32, (seq, LANES), 1) < HEAD
    key_at = lax.broadcasted_iota(jnp.int32, (seq, seq), 1)
    for t in range(texts_here):
        rows = pl.ds(t * seq, seq)
        live = key_at < counts_ref[0, t]
        for pair in range(half // LANES):
            first = pair * LANES
            query = proj_ref[rows, first : first + LANES].astype(jnp.float32) * (HEAD**-0.5)
            key = proj_ref[rows, half + first : half + first + LANES]
            value = proj_ref[rows, 2 * half + first : 2 * half + first + LANES]
            sides = []
            for side in (left, jnp.logical_not(left)):
                scores = mm(jnp.where(side, query, 0.0).astype(jnp.bfloat16), key, (1, 1))
                scores = jnp.where(live, scores, MASKED)
                powers = jnp.exp(scores - jnp.max(scores, axis=-1, keepdims=True))
                total = jnp.sum(powers, axis=-1, keepdims=True)
                sides.append(mm((powers / total).astype(jnp.bfloat16), value))
            ctx_ref[rows, first : first + LANES] = jnp.where(left, sides[0], sides[1]).astype(
                jnp.bfloat16
            )
        out_ref[rows, :] = mm(ctx_ref[rows, :], w_out_ref[...]).astype(jnp.bfloat16)
        sent.append(pltpu.make_async_copy(out_ref.at[rows, :], out_hbm.at[rows, :], out_sems.at[t]))
        sent[-1].start()
    for copy in sent:
        copy.wait()


def inner_body(
    tokens_ref, mine_hbm, other_ref, up_hbm, down_hbm, gains_ref, first_ref, out_ref,
    inner_ref, mine_ref, up_ref, down_ref, sems
):
    started = copies([(mine_hbm, mine_ref), (up_hbm, up_ref), (down_hbm, down_ref)], sems)
    started[0].wait()
    added = mine_ref[...].astype(jnp.float32) + other_ref[...].astype(jnp.float32)
    first = norm(tokens_ref[...].astype(jnp.float32) + added, gains_ref[0:1, :])
    first_ref[...] = first.astype(jnp.bfloat16)
    started[1].wait()
    hidden_units = up_ref.shape[1]
    step = hidden_units // 4
    for c in range(4):
        cols = slice(c * step, (c + 1) * step)
        value = mm(first_ref[...], up_ref[:, cols])
        gate = jnp.tanh(ROOT * (value + CUBE * (value * value * value)))
        inner_ref[:, cols] = (0.5 * value * (1.0 + gate)).astype(jnp.bfloat16)
    started[2].wait()
    out_ref[...] = mm(inner_ref[...], down_ref[...]).astype(jnp.bfloat16)


def pool_body(seq, counts_ref, first_ref, mine_ref, other_ref, gains_ref, out_ref):
    texts_here, width = first_ref.shape[0] // seq, first_ref.shape[1]
    for t in range(texts_here):
        rows = slice(t * seq, (t + 1) * seq)
        added = mine_ref[rows, :].astype(jnp.float32) + other_ref[rows, :].astype(jnp.float32)
        second = norm(first_ref[rows, :].astype(jnp.float32) + added, gains_ref[1:2, :])
        count = counts_ref[0, t]
        live = lax.broadcasted_iota(jnp.int32, (seq, 1), 0) < count
        total = jnp.sum(jnp.where(live, second, 0.0), axis=0, keepdims=True)
        pooled = (total / count.astype(jnp.float32)).astype(jnp.bfloat16).astype(jnp.float32)
        out_ref[:, :, t * width : (t + 1) * width] = pooled.reshape(1, 1, width)


def pooled_rows(me, near_ref, far_ref, width):
    shards = 2 * near_ref.shape[0]
    parts = []
    for first in range(0, near_ref.shape[2], width):
        for ref in (near_ref, far_ref):
            part = ref[:, :, first : first + width].reshape(shards // 2, width)
            parts.append(part.astype(jnp.bfloat16))
    stacked = jnp.concatenate(parts, axis=0)
    texts = stacked.shape[0]
    row = lax.broadcasted_iota(jnp.int32, (texts, texts), 0)
    column = lax.broadcasted_iota(jnp.int32, (texts, texts), 1)
    place = column & (shards - 1)
    offset = jnp.zeros_like(place)
    reach = 1
    while reach < shards:
        offset = 2 * offset + (place & 1)
        place = lax.shift_right_logical(place, 1)
        reach *= 2
    source = column - (column & (shards - 1)) + (offset ^ me)
    order = jnp.where(row == source, 1.0, 0.0).astype(jnp.bfloat16)
    return mm(order, stacked).astype(jnp.bfloat16)


def gather_body(
    row_from, ids_hbm, self_ref, kept_hbm, cache_hbm, remote_ref, out_ref,
    ids_ref, kept_ref, cache_ref, source_ref, sems
):
    rows, entries, tile_rows, _ = kept_ref.shape
    started = copies(
        [(ids_hbm, ids_ref), (cache_hbm, cache_ref), (kept_hbm.at[pl.ds(row_from, rows)], kept_ref)],
        sems,
    )
    tiles_here = cache_ref.shape[0]
    me = self_ref[0]
    started[0].wait()
    started[1].wait()

    def fetch(r, k):
        tile_id = ids_ref[row_from + r, k]
        _, owner, place = tile_of(tile_id, tiles_here)
        local = (owner == me) | (tile_id < 0)

        @pl.when(local)
        def _():
            source_ref[r, k] = cache_ref[place]

        @pl.when(jnp.logical_not(local))
        def _():
            side, spot = side_of(owner, me, remote_ref.shape[0])
            first = pl.multiple_of(side * tile_rows, tile_rows)
            source_ref[r, k] = remote_ref[spot, pl.ds(first, tile_rows), :]

    for r in range(rows):
        lax.fori_loop(
            0, entries, lambda k, c: (fetch(r, k), c)[1], 0, unroll=unroll(entries)
        )
        if r == 0:
            started[2].wait()
        total = jnp.zeros(out_ref.shape[1:], jnp.float32)
        for k in range(entries):
            total = total + mm(kept_ref[r, k], source_ref[r, k])
        out_ref[r] = total.astype(jnp.bfloat16)


def forward_body(
    self_ref, core_ref, top_ref, bottom_ref, far_top_ref, far_bottom_ref, w_own_ref, w_other_ref,
    grad_ref, own_ref, base_hbm, pick_ref, near_ref, far_ref, node_hbm, slope_ref, agg_hbm, slope_hbm,
    rows_ref, node_ref, agg_ref, base_ref, node_sems, agg_sems, slope_sems, base_sems
):
    based = copies([(base_hbm, base_ref)], base_sems)
    half = top_ref.shape[1]
    start = pl.multiple_of(core_ref[0] * half, LANES)
    far = pl.multiple_of((1 - core_ref[0]) * half, LANES)
    rows_ref[...] = pooled_rows(self_ref[0], near_ref, far_ref, rows_ref.shape[1])
    texts = rows_ref.shape[0]
    here = rows_ref[:, pl.ds(start, half)]
    w_own = w_own_ref[:, pl.ds(start, half)]
    w_other = w_other_ref[:, pl.ds(start, half)]
    moved = (mm(here, w_own) + mm(rows_ref[:, pl.ds(far, half)], w_other)).astype(jnp.bfloat16)
    blocks = node_sems.shape[0]
    step = grad_ref.shape[0] // blocks
    sent = []
    for block in range(blocks):
        at = pl.ds(block * step, step)
        mine_ref, other_ref = (
            (top_ref, far_top_ref) if 2 * block < blocks else (bottom_ref, far_bottom_ref)
        )
        within = pl.ds((2 * block % blocks) * step // 2, step)
        pick = pick_ref[at, :][:, :texts]
        hidden = (
            mm(mine_ref[within, :], w_own) + mm(other_ref[within, :], w_other) + mm(pick, moved)
        )
        square = hidden * hidden
        gate = jnp.tanh(ROOT * hidden * (1.0 + CUBE * square))
        lifted = 0.5 * (1.0 + gate)
        slope = lifted + 0.5 * hidden * (1.0 - gate * gate) * (ROOT * (1.0 + 3.0 * CUBE * square))
        slope_ref[at, :] = (grad_ref[at, :].astype(jnp.float32) * slope).astype(jnp.bfloat16)
        fresh = mm(own_ref[at, :][:, :texts], here)
        for copy in based:
            copy.wait()
        based = []
        node_ref[at, :] = (base_ref[at, :].astype(jnp.float32) + fresh + hidden * lifted).astype(
            jnp.bfloat16
        )
        agg_ref[at, :] = (mine_ref[within, :].astype(jnp.float32) + mm(pick, here)).astype(jnp.bfloat16)
        sent += copies([(node_ref.at[at, :], node_hbm.at[at, :])], node_sems.at[pl.ds(block, 1)])
        sent += copies([(agg_ref.at[at, :], agg_hbm.at[at, :])], agg_sems.at[pl.ds(block, 1)])
        sent += copies([(slope_ref.at[at, :], slope_hbm.at[at, :])], slope_sems.at[pl.ds(block, 1)])
    for copy in sent:
        copy.wait()


def chunk_body(
    per, texts_here, self_ref, core_ref, mine_ref, other_ref, agg_ref, down_ref, pick_ref, own_ref,
    grad_ref, keep_ref, give_ref, w_ref, text_ref
):
    kept, _, half = keep_ref.shape
    shards = 2 * kept
    deep = up_to(per, ROWS)
    text_rows = keep_ref.shape[1] - deep
    me = self_ref[0]
    own = pl.multiple_of(core_ref[0] * half, LANES)
    far = pl.multiple_of((1 - core_ref[0]) * half, LANES)
    columns = 2 * half
    text_ref[...] = mm(pick_ref[...], down_ref[...], (0, 0)) + mm(
        own_ref[...], grad_ref[...], (0, 0)
    )
    w_ref[pl.ds(own, half), :] = mm(mine_ref[...], agg_ref[...], (0, 0))
    w_ref[pl.ds(far, half), :] = mm(other_ref[...], agg_ref[...], (0, 0))
    w_ref[columns:, :] = jnp.zeros((w_ref.shape[0] - columns, half), jnp.float32)
    row = lax.broadcasted_iota(jnp.int32, (text_rows, half), 0)
    for q in range(shards):
        piece = w_ref[q * per : q * per + deep, :].astype(jnp.bfloat16)
        block = jnp.zeros((text_rows, half), jnp.float32)
        for i in range(texts_here):
            line = text_ref[i * shards + q : i * shards + q + 1, :]
            high = line.astype(jnp.bfloat16).astype(jnp.float32)
            block = jnp.where(row == i, high, block)
            block = jnp.where(row == text_rows // 2 + i, line - high, block)
        block = block.astype(jnp.bfloat16)
        step = q ^ me
        turned = step * 0
        reach = 1
        while reach < shards:
            turned = 2 * turned + ((step // reach) & 1)
            reach *= 2

        @pl.when(turned < kept)
        def _():
            keep_ref[turned, :deep, :] = piece
            keep_ref[turned, deep:, :] = block

        @pl.when(turned >= kept)
        def _():
            give_ref[turned - kept, :deep, :] = piece
            give_ref[turned - kept, deep:, :] = block


def backward_body(
    ids_ref, self_ref, core_ref, mine_ref, other_ref, w_own_ref, adj_ref, send_hbm, down_hbm,
    down_ref, send_ref, sems, slot_sems
):
    tiles_here, entries, tile_rows, _ = adj_ref.shape
    shards, _, half = send_hbm.shape
    me = self_ref[0]
    core = core_ref[0]
    own = pl.multiple_of(core * half, LANES)
    far = pl.multiple_of((1 - core) * half, LANES)
    down = mm(mine_ref[...], w_own_ref[:, pl.ds(own, half)], (1, 1)) + mm(
        other_ref[...], w_own_ref[:, pl.ds(far, half)], (1, 1)
    )
    down_ref[...] = down.astype(jnp.bfloat16)
    down_copy = pltpu.make_async_copy(down_ref, down_hbm, sems.at[0])
    down_copy.start()

    def slot_of(r, k):
        tile_id = ids_ref[r, k]
        _, owner, _ = tile_of(tile_id, tiles_here)
        away = (tile_id >= 0) & (owner != me)
        return away, jnp.where(away, owner, shards)

    def slot_copy(slot):
        return pltpu.make_async_copy(send_ref.at[slot], send_hbm.at[slot], slot_sems.at[slot])

    def each_away(r, act):
        def one(k, carry):
            away, slot = slot_of(r, k)

            @pl.when(away)
            def _():
                act(slot_copy(slot))

            return carry

        lax.fori_loop(0, entries, one, 0)

    for r in range(tiles_here):
        rows = slice(r * tile_rows, (r + 1) * tile_rows)
        for first in range(0, entries, 6):
            group = range(first, min(first + 6, entries))
            side_by_side = jnp.concatenate([adj_ref[r, k] for k in group], axis=1)
            product = mm(side_by_side, down_ref[rows, :], (0, 0)).astype(jnp.bfloat16)
            for k in group:
                _, slot = slot_of(r, k)
                send_ref[slot] = product[(k - first) * tile_rows : (k - first + 1) * tile_rows]
        each_away(r, lambda copy: copy.start())
    for r in range(tiles_here):
        each_away(r, lambda copy: copy.wait())
    down_copy.wait()


def fold(mine, theirs, deep):
    total = mine.astype(jnp.float32) + theirs.astype(jnp.float32)
    lines = (total.shape[0] - deep) // 2
    return total[:deep, :], total[deep : deep + lines, :] + total[deep + lines :, :]


def fold_body(deep, mine_ref, theirs_ref, keep_ref, give_ref):
    kept = keep_ref.shape[0]
    for s in range(2 * kept):
        w_sum, text = fold(mine_ref[s], theirs_ref[s], deep)
        high = text.astype(jnp.bfloat16).astype(jnp.float32)
        out_ref = (keep_ref if s < kept else give_ref).at[s % kept]
        out_ref[:deep, :] = w_sum.astype(jnp.bfloat16)
        out_ref[deep:, :] = jnp.concatenate([high, text - high], axis=0).astype(jnp.bfloat16)


def close_body(deep, mine_ref, theirs_ref, w_ref, text_ref):
    w_sum, text = fold(mine_ref[0], theirs_ref[0], deep)
    w_ref[...] = w_sum
    text_ref[...] = text[: text_ref.shape[0], :]


def local_body(ids_ref, self_ref, down_ref, adj_ref, grad_ref, local_ref):
    tiles_here, entries, _, _ = adj_ref.shape
    me = self_ref[0]
    local_ref[...] = grad_ref[...].astype(jnp.float32)
    for r in range(tiles_here):

        def one(k, carry):
            tile_id = ids_ref[r, k]
            _, owner, place = tile_of(tile_id, tiles_here)

            @pl.when((tile_id >= 0) & (owner == me))
            def _():
                local_ref[place] += mm(adj_ref[r, k], down_ref[r], (0, 0))

            return carry

        lax.fori_loop(0, entries, one, 0, unroll=unroll(entries))


def finish_body(
    self_ref, asked_ref, mate_ref, local_hbm, got_ref, node_hbm, sum_ref, local_ref, node_ref, sems, out_sems
):
    tiles_here = sum_ref.shape[0]
    started = copies([(local_hbm.at[j], local_ref.at[j]) for j in range(tiles_here)], sems)
    shards = got_ref.shape[0]
    me = self_ref[0]
    sum_ref[...] = jnp.zeros_like(sum_ref)

    def one(q, carry):
        side, spot = side_of(q, me, shards // 2)
        asked = jnp.where(side == 0, asked_ref[spot, 0], mate_ref[spot, 1])

        @pl.when(asked >= 0)
        def _():
            sum_ref[asked] += got_ref[q].astype(jnp.float32)

        return carry

    lax.fori_loop(0, shards, one, 0)
    sent = []
    for j in range(tiles_here):
        started[j].wait()
        node_ref[j] = (sum_ref[j] + local_ref[j]).astype(jnp.bfloat16)
        sent += copies([(node_ref.at[j], node_hbm.at[j])], out_sems.at[pl.ds(j, 1)])
    for copy in sent:
        copy.wait()


def step(
    tokens, token_counts, w_qkv, w_out, w_up, w_down, ln_gains, cache, node_text, adj_tiles,
    adj_values, w_gnn, out_grad
):
    shards = lax.axis_size("graph")
    cores = lax.axis_size("mp")
    me = lax.axis_index("graph").astype(jnp.int32).reshape(1)
    core_at = lax.axis_index("mp")
    core = core_at.astype(jnp.int32).reshape(1)
    texts_here, seq, width = tokens.shape
    nodes_here, half = cache.shape
    tiles_here, entries, tile_rows = adj_values.shape[:3]
    texts = texts_here * shards
    slots = up_to(texts, LANES)
    per = width // shards
    deep = up_to(per, ROWS)
    count = texts_here * seq
    inner = w_up.shape[1]

    def swap(values):
        return lax.ppermute(values, "mp", [(i, cores - 1 - i) for i in range(cores)])

    def toward(values, reach):
        return lax.ppermute(values, "graph", [(i, i ^ reach) for i in range(shards)])

    peers = shards // 2

    def spread(values, groups=None):
        return lax.all_to_all(
            values, "graph", split_axis=0, concat_axis=0, tiled=True, axis_index_groups=groups
        )

    halves_of = [list(range(peers)), list(range(peers, shards))]

    cache_tiles = cache.reshape(tiles_here, tile_rows, half)
    mate_tiles = toward(cache_tiles, peers)
    index = call(
        functools.partial(index_body, texts_here),
        [shape((peers, 1, slots + 2 * LANES), jnp.int32)],
        [adj_tiles, me, node_text.reshape(tiles_here, tile_rows)],
        [HBM, SMEM, HBM],
        flops=1000,
        scratch=[
            pltpu.SMEM(adj_tiles.shape, jnp.int32),
            pltpu.VMEM((tiles_here, tile_rows), jnp.int32),
            pltpu.SemaphoreType.DMA((2,)),
        ],
    )
    got = spread(index, halves_of)
    mate_got = toward(got, peers)

    def places(table):
        return table[:, 0, slots:].reshape(peers, 2, LANES)[:, :, 0]

    asked = places(got)
    packed = call(
        pack_near_body,
        [shape((peers, 2 * tile_rows, half))],
        [asked, cache_tiles],
        [SMEM, HBM],
        flops=1000,
        scratch=[
            pltpu.VMEM(cache_tiles.shape, jnp.bfloat16),
            pltpu.SemaphoreType.DMA((1,)),
            pltpu.SemaphoreType.DMA((peers,)),
        ],
        out_specs=[HBM],
    )
    packed = call(
        pack_far_body,
        [shape((peers, 2 * tile_rows, half))],
        [asked, mate_tiles, packed],
        [SMEM, VMEM, HBM],
        flops=1000,
        scratch=[pltpu.SemaphoreType.DMA((peers,))],
        out_specs=[HBM],
        aliases={2: 0},
    )
    remote = spread(packed, halves_of)

    w_other = swap(w_gnn)

    flat_tokens = tokens.reshape(count, width)
    partial = call(
        functools.partial(attend_body, seq),
        [shape((count, width))],
        [token_counts, flat_tokens, jnp.transpose(w_qkv, (1, 0, 2)), w_out],
        [SMEM, HBM, HBM, HBM],
        flops=2 * count * (width * 3 * half + half * width + 2 * seq * half * 2),
        scratch=[
            pltpu.VMEM((count, width), jnp.bfloat16),
            pltpu.VMEM((3, width, half), jnp.bfloat16),
            pltpu.VMEM((half, width), jnp.bfloat16),
            pltpu.VMEM((count, width), jnp.bfloat16),
            pltpu.VMEM((count, 3 * half), jnp.bfloat16),
            pltpu.VMEM((count, half), jnp.bfloat16),
            pltpu.SemaphoreType.DMA((5,)),
            pltpu.SemaphoreType.DMA((texts_here,)),
        ],
        out_specs=[HBM],
    )
    first, mlp = call(
        inner_body,
        [shape((count, width)), shape((count, width))],
        [flat_tokens, partial, swap(partial), w_up, w_down, ln_gains],
        [VMEM, HBM, VMEM, HBM, HBM, VMEM],
        flops=4 * count * width * inner,
        scratch=[
            pltpu.VMEM((count, inner), jnp.bfloat16),
            pltpu.VMEM((count, width), jnp.bfloat16),
            pltpu.VMEM((width, inner), jnp.bfloat16),
            pltpu.VMEM((inner, width), jnp.bfloat16),
            pltpu.SemaphoreType.DMA((3,)),
        ],
    )
    pooled = call(
        functools.partial(pool_body, seq),
        [shape((1, 1, texts_here * width), jnp.float32)],
        [token_counts, first, mlp, swap(mlp), ln_gains],
        [SMEM, VMEM, VMEM, VMEM, VMEM],
        flops=20 * count * width,
    )
    near = pooled
    reach = peers
    far = toward(near, reach)
    while reach > 1:
        reach = reach // 2
        near = jnp.concatenate([near, far], axis=0)
        far = toward(near, reach)

    kept, pick, own, base = call(
        mask_body,
        [
            shape(adj_values.shape),
            shape((tiles_here, tile_rows, slots)),
            shape((tiles_here, tile_rows, slots)),
            shape(cache_tiles.shape),
        ],
        [adj_tiles, me, got, mate_got, adj_values, cache_tiles],
        [SMEM, SMEM, VMEM, VMEM, VMEM, VMEM],
        flops=2 * adj_values.size * slots,
        scratch=[
            pltpu.VMEM(adj_values.shape, jnp.bfloat16),
            pltpu.VMEM((tiles_here, tile_rows, slots), jnp.bfloat16),
            pltpu.VMEM((tiles_here, tile_rows, slots), jnp.bfloat16),
            pltpu.VMEM(cache_tiles.shape, jnp.bfloat16),
            pltpu.SemaphoreType.DMA((tiles_here, 4)),
        ],
        out_specs=[HBM] * 4,
    )
    rows = tiles_here // 2

    def gather(row_from):
        part = call(
            functools.partial(gather_body, row_from),
            [shape((rows, tile_rows, half))],
            [adj_tiles, me, kept, cache_tiles, remote],
            [HBM, SMEM, HBM, HBM, VMEM],
            flops=adj_values.size * half,
            scratch=[
                pltpu.SMEM(adj_tiles.shape, jnp.int32),
                pltpu.VMEM((rows,) + kept.shape[1:], jnp.bfloat16),
                pltpu.VMEM(cache_tiles.shape, jnp.bfloat16),
                pltpu.VMEM((rows, entries, tile_rows, half), jnp.bfloat16),
                pltpu.SemaphoreType.DMA((3,)),
            ],
        )
        return part.reshape(rows * tile_rows, half)

    top, bottom = gather(0), gather(rows)
    picked = pick.reshape(nodes_here, slots)
    node_out, slope, aggregate, slope_kept = call(
        forward_body,
        [shape((nodes_here, half))] * 4,
        [
            me, core, top, bottom, swap(top), swap(bottom), w_gnn, w_other,
            out_grad,
            own.reshape(nodes_here, slots), base.reshape(nodes_here, half), picked, near, far,
        ],
        [SMEM, SMEM] + [HELD] * 4 + [VMEM] * 4 + [HBM] + [VMEM] * 3,
        flops=4 * nodes_here * half * half,
        scratch=[
            pltpu.VMEM((texts, width), jnp.bfloat16),
            pltpu.VMEM((nodes_here, half), jnp.bfloat16),
            pltpu.VMEM((nodes_here, half), jnp.bfloat16),
            pltpu.VMEM((nodes_here, half), jnp.bfloat16),
            pltpu.SemaphoreType.DMA((tiles_here,)),
            pltpu.SemaphoreType.DMA((tiles_here,)),
            pltpu.SemaphoreType.DMA((tiles_here,)),
            pltpu.SemaphoreType.DMA((1,)),
        ],
        out_specs=[HBM, VMEM, HBM, HBM],
    )
    grad_tiles = out_grad.reshape(tiles_here, tile_rows, half)
    slope_other = swap(slope)
    text_rows = up_to(2 * texts_here, 8)
    halves = (shards // 2, deep + text_rows, half)
    send, down = call(
        backward_body,
        [shape((shards, tile_rows, half)), shape((nodes_here, half))],
        [adj_tiles, me, core, slope, slope_other, w_gnn, adj_values],
        [SMEM, SMEM, SMEM] + [VMEM] * 4,
        flops=4 * nodes_here * half * half + 2 * adj_values.size * half,
        scratch=[
            pltpu.VMEM((nodes_here, half), jnp.bfloat16),
            pltpu.VMEM((shards + 1, tile_rows, half), jnp.bfloat16),
            pltpu.SemaphoreType.DMA((1,)),
            pltpu.SemaphoreType.DMA((shards,)),
        ],
        out_specs=[HBM] * 2,
    )
    returned = spread(send)
    keep, give = call(
        functools.partial(chunk_body, per, texts_here),
        [shape(halves), shape(halves)],
        [
            me, core, slope_kept, slope_other, aggregate, down, picked,
            own.reshape(nodes_here, slots), out_grad,
        ],
        [SMEM, SMEM] + [PULL] * 7,
        flops=4 * nodes_here * half * (half + slots),
        scratch=[
            pltpu.VMEM((width + ROWS, half), jnp.float32),
            pltpu.VMEM((slots, half), jnp.float32),
        ],
    )
    local = call(
        local_body,
        [shape((tiles_here, tile_rows, half), jnp.float32)],
        [adj_tiles, me, down.reshape(tiles_here, tile_rows, half), adj_values, grad_tiles],
        [SMEM, SMEM] + [VMEM] * 3,
        flops=2 * adj_values.size * half,
    )
    reach = 1
    given = toward(give, reach)
    while 2 * reach < shards:
        part = (shards // (4 * reach), deep + text_rows, half)
        keep, give = call(
            functools.partial(fold_body, deep),
            [shape(part), shape(part)],
            [keep, given],
            [VMEM] * 2,
            flops=4 * math.prod(part),
        )
        reach = 2 * reach
        given = toward(give, reach)
    w_part, text_grad = call(
        functools.partial(close_body, deep),
        [shape((deep, half), jnp.float32), shape((texts_here, half), jnp.float32)],
        [keep, given],
        [VMEM] * 2,
        flops=1000,
    )
    node_grad = call(
        finish_body,
        [shape((tiles_here, tile_rows, half))],
        [me, asked, places(mate_got), local, returned],
        [SMEM, SMEM, SMEM, HBM, VMEM],
        flops=1000,
        scratch=[
            pltpu.VMEM((tiles_here, tile_rows, half), jnp.float32),
            pltpu.VMEM((tiles_here, tile_rows, half), jnp.float32),
            pltpu.VMEM((tiles_here, tile_rows, half), jnp.bfloat16),
            pltpu.SemaphoreType.DMA((tiles_here,)),
            pltpu.SemaphoreType.DMA((tiles_here,)),
        ],
        out_specs=[HBM],
    )
    return (node_out, w_part[:per].T, text_grad, node_grad.reshape(nodes_here, half))


def solution(mesh):
    placed = (
        P("graph", None, None),
        P("graph", None),
        P(None, None, "mp"),
        P("mp", None),
        P(None, "mp"),
        P("mp", None),
        P(),
        P("graph", "mp"),
        P("graph"),
        P("graph", None),
        P("graph", None, None, None),
        P("mp", None),
        P("graph", "mp"),
    )
    return jax.shard_map(
        step,
        mesh=mesh,
        in_specs=placed,
        out_specs=(P("graph", "mp"), P("mp", "graph"), P("graph", "mp"), P("graph", "mp")),
        check_vma=False,
    )
```

```python
import functools
import math

import jax
import jax.numpy as jnp
from jax import lax
from jax.experimental import pallas as pl
from jax.experimental.pallas import tpu as pltpu
from jax.sharding import PartitionSpec as P


HEAD = 64
LANES = 128
ROWS = 16
SPARE = 6 << 20
NORM_EPS = 1e-05
MASKED = -1e30
NO_NODE = -(1 << 20)
ROOT = 0.7978845608028654
CUBE = 0.044715


VMEM = pl.BlockSpec(memory_space=pltpu.VMEM)
HBM = pl.BlockSpec(memory_space=pltpu.HBM)
HELD = pl.BlockSpec(memory_space=pltpu.VMEM)
PULL = pl.BlockSpec(memory_space=pltpu.HBM)
SMEM = pl.BlockSpec(memory_space=pltpu.SMEM)


def up_to(value, unit):
    return (value + unit - 1) // unit * unit


def call(body, outs, ins, specs, flops, scratch=(), out_specs=None, aliases=None):
    moved = sum(a.size * a.dtype.itemsize for a in ins) + sum(
        o.size * o.dtype.itemsize for o in outs
    )
    many = len(outs) > 1
    ins = [
        pltpu.with_memory_space_constraint(a, pltpu.HBM) if s is HBM or s is PULL else a
        for a, s in zip(ins, specs, strict=True)
    ]
    ins = [
        pltpu.with_memory_space_constraint(a, pltpu.VMEM) if s is HELD else a
        for a, s in zip(ins, specs, strict=True)
    ]
    pulled = [i for i, s in enumerate(specs) if s is PULL]
    if pulled:
        body = pulling(body, pulled)
        scratch = list(scratch) + [pltpu.VMEM(ins[i].shape, ins[i].dtype) for i in pulled]
        scratch.append(pltpu.SemaphoreType.DMA((len(pulled),)))
    held = sum(math.prod(s.shape) * jnp.dtype(s.dtype).itemsize for s in scratch if counted(s))
    out_specs = out_specs or [VMEM] * len(outs)
    outs = [
        pltpu.HBM(o.shape, o.dtype) if s is HBM else o for o, s in zip(outs, out_specs, strict=True)
    ]
    return pl.pallas_call(
        body,
        out_shape=tuple(outs) if many else outs[0],
        in_specs=list(specs),
        out_specs=tuple(out_specs) if many else out_specs[0],
        scratch_shapes=list(scratch),
        input_output_aliases=aliases or {},
        compiler_params=pltpu.CompilerParams(vmem_limit_bytes=moved + moved // 8 + held + SPARE),
        cost_estimate=pl.CostEstimate(flops=flops, bytes_accessed=moved, transcendentals=0),
    )(*ins)


def counted(scratch):
    return jnp.issubdtype(scratch.dtype, jnp.number)


def copies(pairs, sems):
    started = [pltpu.make_async_copy(a, b, sems.at[i]) for i, (a, b) in enumerate(pairs)]
    for copy in started:
        copy.start()
    return started


def pulling(body, pulled):
    def wrapped(*refs):
        buffers, sems = refs[-len(pulled) - 1 : -1], refs[-1]
        held = list(refs[: -len(pulled) - 1])
        started = copies([(held[i], b) for i, b in zip(pulled, buffers)], sems)
        for i, buffer in zip(pulled, buffers):
            held[i] = buffer
        for copy in started:
            copy.wait()
        body(*held)

    return wrapped


def unroll(steps):
    return steps if steps <= 8 else 1


def shape(dims, dtype=jnp.bfloat16):
    return jax.ShapeDtypeStruct(tuple(dims), dtype)


def mm(a, b, dims=(1, 0)):
    return lax.dot_general(
        a, b, (((dims[0],), (dims[1],)), ((), ())), preferred_element_type=jnp.float32
    )


def tile_of(tile_id, tiles_here):
    safe = jnp.maximum(tile_id, 0)
    owner = lax.div(safe, jnp.int32(tiles_here))
    return safe, owner, safe - owner * tiles_here


def side_of(owner, me, peers):
    half = lax.div(owner, jnp.int32(peers))
    mine = lax.div(me, jnp.int32(peers))
    return jnp.where(half == mine, 0, 1), owner - half * peers


def index_body(texts_here, ids_hbm, self_ref, text_hbm, out_ref, ids_ref, text_ref, sems):
    for copy in copies([(ids_hbm, ids_ref), (text_hbm, text_ref)], sems):
        copy.wait()
    tiles_here, entries = ids_ref.shape
    peers, _, lanes = out_ref.shape
    shards = 2 * peers
    width = lanes - 2 * LANES
    texts = texts_here * shards
    me = self_ref[0]
    row = lax.broadcasted_iota(jnp.int32, (peers, LANES), 0)
    near = jnp.full((peers, LANES), -1, jnp.int32)
    far = near
    for r in range(tiles_here):
        for k in range(entries):
            tile_id = ids_ref[r, k]
            _, owner, place = tile_of(tile_id, tiles_here)
            side, spot = side_of(owner, me, peers)
            wanted = (tile_id >= 0) & (owner != me)
            near = jnp.where(row == jnp.where(wanted & (side == 0), spot, -1), place, near)
            far = jnp.where(row == jnp.where(wanted & (side == 1), spot, -1), place, far)
    out_ref[:, :, width : width + LANES] = near.reshape(peers, 1, LANES)
    out_ref[:, :, width + LANES :] = far.reshape(peers, 1, LANES)
    tile_rows = text_ref.shape[1]
    lane = lax.broadcasted_iota(jnp.int32, (LANES, tile_rows), 1)
    sub = lax.broadcasted_iota(jnp.int32, (LANES, LANES), 0)
    diagonal = sub == lax.broadcasted_iota(jnp.int32, (LANES, LANES), 1)
    for c in range(width // LANES):
        slot = c * LANES + lax.broadcasted_iota(jnp.int32, (LANES, 1), 0)
        part = lax.div(slot, jnp.int32(shards))
        text = jnp.where(slot < texts, (slot - part * shards) * texts_here + part, -5)
        best = jnp.full((LANES, tile_rows), NO_NODE, jnp.int32)
        for j in range(tiles_here):
            node = (me * tiles_here + j) * tile_rows + lane
            best = jnp.where(text_ref[j : j + 1, :] == text, node, best)
        column = jnp.max(best.astype(jnp.float32), axis=1, keepdims=True)
        line = jnp.max(jnp.where(diagonal, column, float(NO_NODE)), axis=0, keepdims=True)
        out_ref[:, :, c * LANES : (c + 1) * LANES] = (
            jnp.broadcast_to(line, (peers, LANES)).astype(jnp.int32).reshape(peers, 1, LANES)
        )


def pack_near_body(asked_ref, cache_hbm, out_hbm, tile_ref, in_sems, out_sems):
    copy = pltpu.make_async_copy(cache_hbm, tile_ref, in_sems.at[0])
    copy.start()
    copy.wait()
    place_tiles(0, asked_ref, tile_ref, out_hbm, out_sems)


def pack_far_body(asked_ref, mate_ref, near_hbm, out_hbm, out_sems):
    place_tiles(1, asked_ref, mate_ref, out_hbm, out_sems)


def place_tiles(side, asked_ref, tile_ref, out_hbm, out_sems):
    tile_rows = tile_ref.shape[1]
    peers = out_hbm.shape[0]

    def slot(p):
        place = jnp.maximum(asked_ref[p, side], 0)
        target = out_hbm.at[p, pl.ds(side * tile_rows, tile_rows), :]
        return pltpu.make_async_copy(tile_ref.at[place], target, out_sems.at[p])

    lax.fori_loop(0, peers, lambda p, c: (slot(p).start(), c)[1], 0)
    lax.fori_loop(0, peers, lambda p, c: (slot(p).wait(), c)[1], 0)


def mask_body(
    ids_ref, self_ref, got_ref, mate_ref, adj_ref, cache_ref, *refs
):
    outs, (kept_ref, pick_ref, own_ref, base_ref, sems) = refs[:4], refs[4:]
    tiles_here, entries, tile_rows, _ = adj_ref.shape
    peers, _, lanes = got_ref.shape
    width = lanes - 2 * LANES
    me = self_ref[0]
    both = jnp.maximum(got_ref[:, :, :width], mate_ref[:, :, :width])
    table = jnp.max(both.reshape(peers, width).astype(jnp.float32), axis=0, keepdims=True)
    place = lax.broadcasted_iota(jnp.int32, (tile_rows, width), 0).astype(jnp.float32)
    ones = jnp.ones((ROWS, width), jnp.bfloat16)
    sent = []

    def holds(tile_id):
        first = (tile_id * tile_rows).astype(jnp.float32)
        return jnp.where(table - first == place, 1.0, 0.0)

    for r in range(tiles_here):

        def one(k, total):
            tile_id = ids_ref[r, k]
            hot = holds(tile_id).astype(jnp.bfloat16)
            values = adj_ref[r, k]
            taken = mm(ones, hot, (1, 1))[0:1, :]
            keep = jnp.where(tile_id >= 0, 1.0, 0.0) * jnp.where(taken > 0.5, 0.0, 1.0)
            kept_ref[r, k] = (values.astype(jnp.float32) * keep).astype(jnp.bfloat16)
            return total + mm(values, hot)

        pick = lax.fori_loop(
            0, entries, one, jnp.zeros((tile_rows, width), jnp.float32), unroll=unroll(entries)
        )
        pick_ref[r] = pick.astype(jnp.bfloat16)
        hot = holds(me * tiles_here + r)
        own_ref[r] = hot.astype(jnp.bfloat16)
        fresh = jnp.max(hot, axis=1, keepdims=True)
        base_ref[r] = (cache_ref[r].astype(jnp.float32) * (1.0 - fresh)).astype(jnp.bfloat16)
        row = [(ref.at[r], out.at[r]) for ref, out in zip((kept_ref, pick_ref, own_ref, base_ref), outs)]
        sent = sent + copies(row, sems.at[r])
    for copy in sent:
        copy.wait()


def norm(values, gain):
    average = jnp.mean(values, axis=-1, keepdims=True)
    centred = values - average
    variance = jnp.mean(centred * centred, axis=-1, keepdims=True)
    return centred * lax.rsqrt(variance + NORM_EPS) * gain


def attend_body(
    seq, counts_ref, tokens_hbm, w_qkv_hbm, w_out_hbm, out_hbm,
    tokens_ref, w_qkv_ref, w_out_ref, out_ref, proj_ref, ctx_ref, in_sems, out_sems
):
    half = w_out_ref.shape[0]
    texts_here = tokens_ref.shape[0] // seq
    started = copies(
        [(tokens_hbm, tokens_ref)]
        + [(w_qkv_hbm.at[c], w_qkv_ref.at[c]) for c in range(3)]
        + [(w_out_hbm, w_out_ref)],
        in_sems,
    )
    started[0].wait()
    for c in range(3):
        started[1 + c].wait()
        proj_ref[:, c * half : (c + 1) * half] = mm(tokens_ref[...], w_qkv_ref[c]).astype(
            jnp.bfloat16
        )
    started[4].wait()
    sent = []
    left = lax.broadcasted_iota(jnp.int32, (seq, LANES), 1) < HEAD
    key_at = lax.broadcasted_iota(jnp.int32, (seq, seq), 1)
    for t in range(texts_here):
        rows = pl.ds(t * seq, seq)
        live = key_at < counts_ref[0, t]
        for pair in range(half // LANES):
            first = pair * LANES
            query = proj_ref[rows, first : first + LANES].astype(jnp.float32) * (HEAD**-0.5)
            key = proj_ref[rows, half + first : half + first + LANES]
            value = proj_ref[rows, 2 * half + first : 2 * half + first + LANES]
            sides = []
            for side in (left, jnp.logical_not(left)):
                scores = mm(jnp.where(side, query, 0.0).astype(jnp.bfloat16), key, (1, 1))
                scores = jnp.where(live, scores, MASKED)
                powers = jnp.exp(scores - jnp.max(scores, axis=-1, keepdims=True))
                total = jnp.sum(powers, axis=-1, keepdims=True)
                sides.append(mm((powers / total).astype(jnp.bfloat16), value))
            ctx_ref[rows, first : first + LANES] = jnp.where(left, sides[0], sides[1]).astype(
                jnp.bfloat16
            )
        out_ref[rows, :] = mm(ctx_ref[rows, :], w_out_ref[...]).astype(jnp.bfloat16)
        sent.append(pltpu.make_async_copy(out_ref.at[rows, :], out_hbm.at[rows, :], out_sems.at[t]))
        sent[-1].start()
    for copy in sent:
        copy.wait()


def inner_body(
    tokens_ref, mine_hbm, other_ref, up_hbm, down_hbm, gains_ref, first_ref, out_ref,
    inner_ref, mine_ref, up_ref, down_ref, sems
):
    started = copies([(mine_hbm, mine_ref), (up_hbm, up_ref), (down_hbm, down_ref)], sems)
    started[0].wait()
    added = mine_ref[...].astype(jnp.float32) + other_ref[...].astype(jnp.float32)
    first = norm(tokens_ref[...].astype(jnp.float32) + added, gains_ref[0:1, :])
    first_ref[...] = first.astype(jnp.bfloat16)
    started[1].wait()
    hidden_units = up_ref.shape[1]
    step = hidden_units // 4
    for c in range(4):
        cols = slice(c * step, (c + 1) * step)
        value = mm(first_ref[...], up_ref[:, cols])
        gate = jnp.tanh(ROOT * (value + CUBE * (value * value * value)))
        inner_ref[:, cols] = (0.5 * value * (1.0 + gate)).astype(jnp.bfloat16)
    started[2].wait()
    out_ref[...] = mm(inner_ref[...], down_ref[...]).astype(jnp.bfloat16)


def pool_body(seq, counts_ref, first_ref, mine_ref, other_ref, gains_ref, out_ref):
    texts_here, width = first_ref.shape[0] // seq, first_ref.shape[1]
    for t in range(texts_here):
        rows = slice(t * seq, (t + 1) * seq)
        added = mine_ref[rows, :].astype(jnp.float32) + other_ref[rows, :].astype(jnp.float32)
        second = norm(first_ref[rows, :].astype(jnp.float32) + added, gains_ref[1:2, :])
        count = counts_ref[0, t]
        live = lax.broadcasted_iota(jnp.int32, (seq, 1), 0) < count
        total = jnp.sum(jnp.where(live, second, 0.0), axis=0, keepdims=True)
        pooled = (total / count.astype(jnp.float32)).astype(jnp.bfloat16).astype(jnp.float32)
        out_ref[:, :, t * width : (t + 1) * width] = pooled.reshape(1, 1, width)


def digits(shards):
    high, found = shards.bit_length() - 1, []
    while high > 0:
        low = max(high - 2, 0)
        found.append((low, high - low))
        high = low
    return found


def pooled_rows(me, pieces, width):
    shards = sum(piece.shape[0] for piece in pieces)
    parts = []
    for first in range(0, pieces[0].shape[2], width):
        for ref in pieces:
            part = ref[:, :, first : first + width].reshape(ref.shape[0], width)
            parts.append(part.astype(jnp.bfloat16))
    stacked = jnp.concatenate(parts, axis=0)
    texts = stacked.shape[0]
    row = lax.broadcasted_iota(jnp.int32, (texts, texts), 0)
    column = lax.broadcasted_iota(jnp.int32, (texts, texts), 1)
    place = column & (shards - 1)
    offset = jnp.zeros_like(place)
    for low, count in digits(shards):
        offset = offset + ((place & ((1 << count) - 1)) << low)
        place = lax.shift_right_logical(place, count)
    source = column - (column & (shards - 1)) + (offset ^ me)
    order = jnp.where(row == source, 1.0, 0.0).astype(jnp.bfloat16)
    return mm(order, stacked).astype(jnp.bfloat16)


def gather_body(
    row_from, ids_hbm, self_ref, kept_hbm, cache_hbm, remote_ref, out_ref,
    ids_ref, kept_ref, cache_ref, source_ref, sems
):
    rows, entries, tile_rows, _ = kept_ref.shape
    started = copies(
        [(ids_hbm, ids_ref), (cache_hbm, cache_ref), (kept_hbm.at[pl.ds(row_from, rows)], kept_ref)],
        sems,
    )
    tiles_here = cache_ref.shape[0]
    me = self_ref[0]
    started[0].wait()
    started[1].wait()

    def fetch(r, k):
        tile_id = ids_ref[row_from + r, k]
        _, owner, place = tile_of(tile_id, tiles_here)
        local = (owner == me) | (tile_id < 0)

        @pl.when(local)
        def _():
            source_ref[r, k] = cache_ref[place]

        @pl.when(jnp.logical_not(local))
        def _():
            side, spot = side_of(owner, me, remote_ref.shape[0])
            first = pl.multiple_of(side * tile_rows, tile_rows)
            source_ref[r, k] = remote_ref[spot, pl.ds(first, tile_rows), :]

    for r in range(rows):
        lax.fori_loop(
            0, entries, lambda k, c: (fetch(r, k), c)[1], 0, unroll=unroll(entries)
        )
        if r == 0:
            started[2].wait()
        total = jnp.zeros(out_ref.shape[1:], jnp.float32)
        for k in range(entries):
            total = total + mm(kept_ref[r, k], source_ref[r, k])
        out_ref[r] = total.astype(jnp.bfloat16)


def forward_body(
    self_ref, core_ref, top_ref, bottom_ref, far_top_ref, far_bottom_ref, w_own_ref, w_other_ref,
    grad_ref, own_ref, base_hbm, pick_ref, *refs
):
    (
        *pieces, node_hbm, slope_ref, agg_hbm, slope_hbm,
        rows_ref, node_ref, agg_ref, base_ref, node_sems, agg_sems, slope_sems, base_sems
    ) = refs
    based = copies([(base_hbm, base_ref)], base_sems)
    half = top_ref.shape[1]
    start = pl.multiple_of(core_ref[0] * half, LANES)
    far = pl.multiple_of((1 - core_ref[0]) * half, LANES)
    rows_ref[...] = pooled_rows(self_ref[0], pieces, rows_ref.shape[1])
    texts = rows_ref.shape[0]
    here = rows_ref[:, pl.ds(start, half)]
    w_own = w_own_ref[:, pl.ds(start, half)]
    w_other = w_other_ref[:, pl.ds(start, half)]
    moved = (mm(here, w_own) + mm(rows_ref[:, pl.ds(far, half)], w_other)).astype(jnp.bfloat16)
    blocks = node_sems.shape[0]
    step = grad_ref.shape[0] // blocks
    sent = []
    for block in range(blocks):
        at = pl.ds(block * step, step)
        mine_ref, other_ref = (
            (top_ref, far_top_ref) if 2 * block < blocks else (bottom_ref, far_bottom_ref)
        )
        within = pl.ds((2 * block % blocks) * step // 2, step)
        pick = pick_ref[at, :][:, :texts]
        hidden = (
            mm(mine_ref[within, :], w_own) + mm(other_ref[within, :], w_other) + mm(pick, moved)
        )
        square = hidden * hidden
        gate = jnp.tanh(ROOT * hidden * (1.0 + CUBE * square))
        lifted = 0.5 * (1.0 + gate)
        slope = lifted + 0.5 * hidden * (1.0 - gate * gate) * (ROOT * (1.0 + 3.0 * CUBE * square))
        slope_ref[at, :] = (grad_ref[at, :].astype(jnp.float32) * slope).astype(jnp.bfloat16)
        fresh = mm(own_ref[at, :][:, :texts], here)
        for copy in based:
            copy.wait()
        based = []
        node_ref[at, :] = (base_ref[at, :].astype(jnp.float32) + fresh + hidden * lifted).astype(
            jnp.bfloat16
        )
        agg_ref[at, :] = (mine_ref[within, :].astype(jnp.float32) + mm(pick, here)).astype(jnp.bfloat16)
        sent += copies([(node_ref.at[at, :], node_hbm.at[at, :])], node_sems.at[pl.ds(block, 1)])
        sent += copies([(agg_ref.at[at, :], agg_hbm.at[at, :])], agg_sems.at[pl.ds(block, 1)])
        sent += copies([(slope_ref.at[at, :], slope_hbm.at[at, :])], slope_sems.at[pl.ds(block, 1)])
    for copy in sent:
        copy.wait()


def chunk_body(
    per, texts_here, self_ref, core_ref, mine_ref, other_ref, agg_ref, down_ref, pick_ref, own_ref,
    grad_ref, keep_ref, give_ref, w_ref, text_ref
):
    kept, _, half = keep_ref.shape
    shards = 2 * kept
    deep = up_to(per, ROWS)
    text_rows = keep_ref.shape[1] - deep
    me = self_ref[0]
    own = pl.multiple_of(core_ref[0] * half, LANES)
    far = pl.multiple_of((1 - core_ref[0]) * half, LANES)
    columns = 2 * half
    text_ref[...] = mm(pick_ref[...], down_ref[...], (0, 0)) + mm(
        own_ref[...], grad_ref[...], (0, 0)
    )
    w_ref[pl.ds(own, half), :] = mm(mine_ref[...], agg_ref[...], (0, 0))
    w_ref[pl.ds(far, half), :] = mm(other_ref[...], agg_ref[...], (0, 0))
    w_ref[columns:, :] = jnp.zeros((w_ref.shape[0] - columns, half), jnp.float32)
    row = lax.broadcasted_iota(jnp.int32, (text_rows, half), 0)
    for q in range(shards):
        piece = w_ref[q * per : q * per + deep, :].astype(jnp.bfloat16)
        block = jnp.zeros((text_rows, half), jnp.float32)
        for i in range(texts_here):
            line = text_ref[i * shards + q : i * shards + q + 1, :]
            high = line.astype(jnp.bfloat16).astype(jnp.float32)
            block = jnp.where(row == i, high, block)
            block = jnp.where(row == text_rows // 2 + i, line - high, block)
        block = block.astype(jnp.bfloat16)
        step = q ^ me
        turned = step * 0
        reach = 1
        while reach < shards:
            turned = 2 * turned + ((step // reach) & 1)
            reach *= 2

        @pl.when(turned < kept)
        def _():
            keep_ref[turned, :deep, :] = piece
            keep_ref[turned, deep:, :] = block

        @pl.when(turned >= kept)
        def _():
            give_ref[turned - kept, :deep, :] = piece
            give_ref[turned - kept, deep:, :] = block


def backward_body(
    ids_ref, self_ref, core_ref, mine_ref, other_ref, w_own_ref, adj_ref, send_hbm, down_hbm,
    down_ref, send_ref, sems, slot_sems
):
    tiles_here, entries, tile_rows, _ = adj_ref.shape
    shards, _, half = send_hbm.shape
    me = self_ref[0]
    core = core_ref[0]
    own = pl.multiple_of(core * half, LANES)
    far = pl.multiple_of((1 - core) * half, LANES)
    down = mm(mine_ref[...], w_own_ref[:, pl.ds(own, half)], (1, 1)) + mm(
        other_ref[...], w_own_ref[:, pl.ds(far, half)], (1, 1)
    )
    down_ref[...] = down.astype(jnp.bfloat16)
    down_copy = pltpu.make_async_copy(down_ref, down_hbm, sems.at[0])
    down_copy.start()
    for r in range(tiles_here):
        rows = slice(r * tile_rows, (r + 1) * tile_rows)
        for first in range(0, entries, 6):
            group = range(first, min(first + 6, entries))
            side_by_side = jnp.concatenate([adj_ref[r, k] for k in group], axis=1)
            product = mm(side_by_side, down_ref[rows, :], (0, 0)).astype(jnp.bfloat16)
            for k in group:
                tile_id = ids_ref[r, k]
                _, owner, _ = tile_of(tile_id, tiles_here)
                slot = jnp.where((tile_id >= 0) & (owner != me), owner, shards)
                send_ref[slot] = product[(k - first) * tile_rows : (k - first + 1) * tile_rows]
    for copy in copies([(send_ref.at[q], send_hbm.at[q]) for q in range(shards)], slot_sems):
        copy.wait()
    down_copy.wait()


def fold(mine, theirs, deep):
    total = mine.astype(jnp.float32) + theirs.astype(jnp.float32)
    lines = (total.shape[0] - deep) // 2
    return total[:deep, :], total[deep : deep + lines, :] + total[deep + lines :, :]


def fold_body(deep, mine_ref, theirs_ref, keep_ref, give_ref):
    kept = keep_ref.shape[0]
    for s in range(2 * kept):
        w_sum, text = fold(mine_ref[s], theirs_ref[s], deep)
        high = text.astype(jnp.bfloat16).astype(jnp.float32)
        out_ref = (keep_ref if s < kept else give_ref).at[s % kept]
        out_ref[:deep, :] = w_sum.astype(jnp.bfloat16)
        out_ref[deep:, :] = jnp.concatenate([high, text - high], axis=0).astype(jnp.bfloat16)


def close_body(deep, mine_ref, theirs_ref, w_ref, text_ref):
    w_sum, text = fold(mine_ref[0], theirs_ref[0], deep)
    w_ref[...] = w_sum
    text_ref[...] = text[: text_ref.shape[0], :]


def local_body(ids_ref, self_ref, down_ref, adj_ref, grad_ref, local_ref):
    tiles_here, entries, _, _ = adj_ref.shape
    me = self_ref[0]
    local_ref[...] = grad_ref[...].astype(jnp.float32)
    for r in range(tiles_here):

        def one(k, carry):
            tile_id = ids_ref[r, k]
            _, owner, place = tile_of(tile_id, tiles_here)

            @pl.when((tile_id >= 0) & (owner == me))
            def _():
                local_ref[place] += mm(adj_ref[r, k], down_ref[r], (0, 0))

            return carry

        lax.fori_loop(0, entries, one, 0, unroll=unroll(entries))


def finish_body(
    self_ref, asked_ref, mate_ref, local_hbm, got_ref, node_hbm, sum_ref, local_ref, node_ref, sems, out_sems
):
    tiles_here = sum_ref.shape[0]
    started = copies([(local_hbm.at[j], local_ref.at[j]) for j in range(tiles_here)], sems)
    shards = got_ref.shape[0]
    me = self_ref[0]
    sum_ref[...] = jnp.zeros_like(sum_ref)

    def one(q, carry):
        side, spot = side_of(q, me, shards // 2)
        asked = jnp.where(side == 0, asked_ref[spot, 0], mate_ref[spot, 1])

        @pl.when(asked >= 0)
        def _():
            sum_ref[asked] += got_ref[q].astype(jnp.float32)

        return carry

    lax.fori_loop(0, shards, one, 0)
    sent = []
    for j in range(tiles_here):
        started[j].wait()
        node_ref[j] = (sum_ref[j] + local_ref[j]).astype(jnp.bfloat16)
        sent += copies([(node_ref.at[j], node_hbm.at[j])], out_sems.at[pl.ds(j, 1)])
    for copy in sent:
        copy.wait()


def step(
    tokens, token_counts, w_qkv, w_out, w_up, w_down, ln_gains, cache, node_text, adj_tiles,
    adj_values, w_gnn, out_grad
):
    shards = lax.axis_size("graph")
    cores = lax.axis_size("mp")
    me = lax.axis_index("graph").astype(jnp.int32).reshape(1)
    core_at = lax.axis_index("mp")
    core = core_at.astype(jnp.int32).reshape(1)
    texts_here, seq, width = tokens.shape
    nodes_here, half = cache.shape
    tiles_here, entries, tile_rows = adj_values.shape[:3]
    texts = texts_here * shards
    slots = up_to(texts, LANES)
    per = width // shards
    deep = up_to(per, ROWS)
    count = texts_here * seq
    inner = w_up.shape[1]

    def swap(values):
        return lax.ppermute(values, "mp", [(i, cores - 1 - i) for i in range(cores)])

    def toward(values, reach):
        return lax.ppermute(values, "graph", [(i, i ^ reach) for i in range(shards)])

    peers = shards // 2

    def spread(values, groups=None):
        return lax.all_to_all(
            values, "graph", split_axis=0, concat_axis=0, tiled=True, axis_index_groups=groups
        )

    halves_of = [list(range(peers)), list(range(peers, shards))]

    cache_tiles = cache.reshape(tiles_here, tile_rows, half)
    mate_tiles = toward(cache_tiles, peers)
    index = call(
        functools.partial(index_body, texts_here),
        [shape((peers, 1, slots + 2 * LANES), jnp.int32)],
        [adj_tiles, me, node_text.reshape(tiles_here, tile_rows)],
        [HBM, SMEM, HBM],
        flops=1000,
        scratch=[
            pltpu.SMEM(adj_tiles.shape, jnp.int32),
            pltpu.VMEM((tiles_here, tile_rows), jnp.int32),
            pltpu.SemaphoreType.DMA((2,)),
        ],
    )
    got = spread(index, halves_of)
    mate_got = toward(got, peers)

    def places(table):
        return table[:, 0, slots:].reshape(peers, 2, LANES)[:, :, 0]

    asked = places(got)
    packed = call(
        pack_near_body,
        [shape((peers, 2 * tile_rows, half))],
        [asked, cache_tiles],
        [SMEM, HBM],
        flops=1000,
        scratch=[
            pltpu.VMEM(cache_tiles.shape, jnp.bfloat16),
            pltpu.SemaphoreType.DMA((1,)),
            pltpu.SemaphoreType.DMA((peers,)),
        ],
        out_specs=[HBM],
    )
    packed = call(
        pack_far_body,
        [shape((peers, 2 * tile_rows, half))],
        [asked, mate_tiles, packed],
        [SMEM, VMEM, HBM],
        flops=1000,
        scratch=[pltpu.SemaphoreType.DMA((peers,))],
        out_specs=[HBM],
        aliases={2: 0},
    )
    remote = spread(packed, halves_of)

    w_other = swap(w_gnn)

    flat_tokens = tokens.reshape(count, width)
    partial = call(
        functools.partial(attend_body, seq),
        [shape((count, width))],
        [token_counts, flat_tokens, jnp.transpose(w_qkv, (1, 0, 2)), w_out],
        [SMEM, HBM, HBM, HBM],
        flops=2 * count * (width * 3 * half + half * width + 2 * seq * half * 2),
        scratch=[
            pltpu.VMEM((count, width), jnp.bfloat16),
            pltpu.VMEM((3, width, half), jnp.bfloat16),
            pltpu.VMEM((half, width), jnp.bfloat16),
            pltpu.VMEM((count, width), jnp.bfloat16),
            pltpu.VMEM((count, 3 * half), jnp.bfloat16),
            pltpu.VMEM((count, half), jnp.bfloat16),
            pltpu.SemaphoreType.DMA((5,)),
            pltpu.SemaphoreType.DMA((texts_here,)),
        ],
        out_specs=[HBM],
    )
    first, mlp = call(
        inner_body,
        [shape((count, width)), shape((count, width))],
        [flat_tokens, partial, swap(partial), w_up, w_down, ln_gains],
        [VMEM, HBM, VMEM, HBM, HBM, VMEM],
        flops=4 * count * width * inner,
        scratch=[
            pltpu.VMEM((count, inner), jnp.bfloat16),
            pltpu.VMEM((count, width), jnp.bfloat16),
            pltpu.VMEM((width, inner), jnp.bfloat16),
            pltpu.VMEM((inner, width), jnp.bfloat16),
            pltpu.SemaphoreType.DMA((3,)),
        ],
    )
    pooled = call(
        functools.partial(pool_body, seq),
        [shape((1, 1, texts_here * width), jnp.float32)],
        [token_counts, first, mlp, swap(mlp), ln_gains],
        [SMEM, VMEM, VMEM, VMEM, VMEM],
        flops=20 * count * width,
    )
    pieces = [pooled]
    for low, bits in digits(shards):
        state = pieces[0] if len(pieces) == 1 else jnp.concatenate(pieces, axis=0)
        pieces = [state]
        for c in range(1, 1 << bits):
            pieces.append(toward(state, c << low))

    kept, pick, own, base = call(
        mask_body,
        [
            shape(adj_values.shape),
            shape((tiles_here, tile_rows, slots)),
            shape((tiles_here, tile_rows, slots)),
            shape(cache_tiles.shape),
        ],
        [adj_tiles, me, got, mate_got, adj_values, cache_tiles],
        [SMEM, SMEM, VMEM, VMEM, VMEM, VMEM],
        flops=2 * adj_values.size * slots,
        scratch=[
            pltpu.VMEM(adj_values.shape, jnp.bfloat16),
            pltpu.VMEM((tiles_here, tile_rows, slots), jnp.bfloat16),
            pltpu.VMEM((tiles_here, tile_rows, slots), jnp.bfloat16),
            pltpu.VMEM(cache_tiles.shape, jnp.bfloat16),
            pltpu.SemaphoreType.DMA((tiles_here, 4)),
        ],
        out_specs=[HBM] * 4,
    )
    rows = tiles_here // 2

    def gather(row_from):
        part = call(
            functools.partial(gather_body, row_from),
            [shape((rows, tile_rows, half))],
            [adj_tiles, me, kept, cache_tiles, remote],
            [HBM, SMEM, HBM, HBM, VMEM],
            flops=adj_values.size * half,
            scratch=[
                pltpu.SMEM(adj_tiles.shape, jnp.int32),
                pltpu.VMEM((rows,) + kept.shape[1:], jnp.bfloat16),
                pltpu.VMEM(cache_tiles.shape, jnp.bfloat16),
                pltpu.VMEM((rows, entries, tile_rows, half), jnp.bfloat16),
                pltpu.SemaphoreType.DMA((3,)),
            ],
        )
        return part.reshape(rows * tile_rows, half)

    top, bottom = gather(0), gather(rows)
    picked = pick.reshape(nodes_here, slots)
    node_out, slope, aggregate, slope_kept = call(
        forward_body,
        [shape((nodes_here, half))] * 4,
        [
            me, core, top, bottom, swap(top), swap(bottom), w_gnn, w_other,
            out_grad,
            own.reshape(nodes_here, slots), base.reshape(nodes_here, half), picked, *pieces,
        ],
        [SMEM, SMEM] + [HELD] * 4 + [VMEM] * 4 + [HBM] + [VMEM] * (1 + len(pieces)),
        flops=4 * nodes_here * half * half,
        scratch=[
            pltpu.VMEM((texts, width), jnp.bfloat16),
            pltpu.VMEM((nodes_here, half), jnp.bfloat16),
            pltpu.VMEM((nodes_here, half), jnp.bfloat16),
            pltpu.VMEM((nodes_here, half), jnp.bfloat16),
            pltpu.SemaphoreType.DMA((tiles_here,)),
            pltpu.SemaphoreType.DMA((tiles_here,)),
            pltpu.SemaphoreType.DMA((tiles_here,)),
            pltpu.SemaphoreType.DMA((1,)),
        ],
        out_specs=[HBM, VMEM, HBM, HBM],
    )
    grad_tiles = out_grad.reshape(tiles_here, tile_rows, half)
    slope_other = swap(slope)
    text_rows = up_to(2 * texts_here, 8)
    halves = (shards // 2, deep + text_rows, half)
    send, down = call(
        backward_body,
        [shape((shards, tile_rows, half)), shape((nodes_here, half))],
        [adj_tiles, me, core, slope, slope_other, w_gnn, adj_values],
        [SMEM, SMEM, SMEM] + [VMEM] * 4,
        flops=4 * nodes_here * half * half + 2 * adj_values.size * half,
        scratch=[
            pltpu.VMEM((nodes_here, half), jnp.bfloat16),
            pltpu.VMEM((shards + 1, tile_rows, half), jnp.bfloat16),
            pltpu.SemaphoreType.DMA((1,)),
            pltpu.SemaphoreType.DMA((shards,)),
        ],
        out_specs=[HBM] * 2,
    )
    returned = spread(send)
    keep, give = call(
        functools.partial(chunk_body, per, texts_here),
        [shape(halves), shape(halves)],
        [
            me, core, slope_kept, slope_other, aggregate, down, picked,
            own.reshape(nodes_here, slots), out_grad,
        ],
        [SMEM, SMEM] + [PULL] * 7,
        flops=4 * nodes_here * half * (half + slots),
        scratch=[
            pltpu.VMEM((width + ROWS, half), jnp.float32),
            pltpu.VMEM((slots, half), jnp.float32),
        ],
    )
    local = call(
        local_body,
        [shape((tiles_here, tile_rows, half), jnp.float32)],
        [adj_tiles, me, down.reshape(tiles_here, tile_rows, half), adj_values, grad_tiles],
        [SMEM, SMEM] + [VMEM] * 3,
        flops=2 * adj_values.size * half,
    )
    reach = 1
    given = toward(give, reach)
    while 2 * reach < shards:
        part = (shards // (4 * reach), deep + text_rows, half)
        keep, give = call(
            functools.partial(fold_body, deep),
            [shape(part), shape(part)],
            [keep, given],
            [VMEM] * 2,
            flops=4 * math.prod(part),
        )
        reach = 2 * reach
        given = toward(give, reach)
    w_part, text_grad = call(
        functools.partial(close_body, deep),
        [shape((deep, half), jnp.float32), shape((texts_here, half), jnp.float32)],
        [keep, given],
        [VMEM] * 2,
        flops=1000,
    )
    node_grad = call(
        finish_body,
        [shape((tiles_here, tile_rows, half))],
        [me, asked, places(mate_got), local, returned],
        [SMEM, SMEM, SMEM, HBM, VMEM],
        flops=1000,
        scratch=[
            pltpu.VMEM((tiles_here, tile_rows, half), jnp.float32),
            pltpu.VMEM((tiles_here, tile_rows, half), jnp.float32),
            pltpu.VMEM((tiles_here, tile_rows, half), jnp.bfloat16),
            pltpu.SemaphoreType.DMA((tiles_here,)),
            pltpu.SemaphoreType.DMA((tiles_here,)),
        ],
        out_specs=[HBM],
    )
    return (node_out, w_part[:per].T, text_grad, node_grad.reshape(nodes_here, half))


def solution(mesh):
    placed = (
        P("graph", None, None),
        P("graph", None),
        P(None, None, "mp"),
        P("mp", None),
        P(None, "mp"),
        P("mp", None),
        P(),
        P("graph", "mp"),
        P("graph"),
        P("graph", None),
        P("graph", None, None, None),
        P("mp", None),
        P("graph", "mp"),
    )
    return jax.shard_map(
        step,
        mesh=mesh,
        in_specs=placed,
        out_specs=(P("graph", "mp"), P("mp", "graph"), P("graph", "mp"), P("graph", "mp")),
        check_vma=False,
    )
```

```python
import functools
import math

import jax
import jax.numpy as jnp
from jax import lax
from jax.experimental import pallas as pl
from jax.experimental.pallas import tpu as pltpu
from jax.sharding import PartitionSpec as P


HEAD = 64
LANES = 128
ROWS = 16
SPARE = 6 << 20
NORM_EPS = 1e-05
MASKED = -1e30
NO_NODE = -(1 << 20)
ROOT = 0.7978845608028654
CUBE = 0.044715


VMEM = pl.BlockSpec(memory_space=pltpu.VMEM)
HBM = pl.BlockSpec(memory_space=pltpu.HBM)
HELD = pl.BlockSpec(memory_space=pltpu.VMEM)
PULL = pl.BlockSpec(memory_space=pltpu.HBM)
SMEM = pl.BlockSpec(memory_space=pltpu.SMEM)


def up_to(value, unit):
    return (value + unit - 1) // unit * unit


def call(body, outs, ins, specs, flops, scratch=(), out_specs=None, aliases=None):
    moved = sum(a.size * a.dtype.itemsize for a in ins) + sum(
        o.size * o.dtype.itemsize for o in outs
    )
    many = len(outs) > 1
    ins = [
        pltpu.with_memory_space_constraint(a, pltpu.HBM) if s is HBM or s is PULL else a
        for a, s in zip(ins, specs, strict=True)
    ]
    ins = [
        pltpu.with_memory_space_constraint(a, pltpu.VMEM) if s is HELD else a
        for a, s in zip(ins, specs, strict=True)
    ]
    pulled = [i for i, s in enumerate(specs) if s is PULL]
    if pulled:
        body = pulling(body, pulled)
        scratch = list(scratch) + [pltpu.VMEM(ins[i].shape, ins[i].dtype) for i in pulled]
        scratch.append(pltpu.SemaphoreType.DMA((len(pulled),)))
    held = sum(math.prod(s.shape) * jnp.dtype(s.dtype).itemsize for s in scratch if counted(s))
    out_specs = out_specs or [VMEM] * len(outs)
    outs = [
        pltpu.HBM(o.shape, o.dtype) if s is HBM else o for o, s in zip(outs, out_specs, strict=True)
    ]
    return pl.pallas_call(
        body,
        out_shape=tuple(outs) if many else outs[0],
        in_specs=list(specs),
        out_specs=tuple(out_specs) if many else out_specs[0],
        scratch_shapes=list(scratch),
        input_output_aliases=aliases or {},
        compiler_params=pltpu.CompilerParams(vmem_limit_bytes=moved + moved // 8 + held + SPARE),
        cost_estimate=pl.CostEstimate(flops=flops, bytes_accessed=moved, transcendentals=0),
    )(*ins)


def counted(scratch):
    return jnp.issubdtype(scratch.dtype, jnp.number)


def copies(pairs, sems):
    started = [pltpu.make_async_copy(a, b, sems.at[i]) for i, (a, b) in enumerate(pairs)]
    for copy in started:
        copy.start()
    return started


def pulling(body, pulled):
    def wrapped(*refs):
        buffers, sems = refs[-len(pulled) - 1 : -1], refs[-1]
        held = list(refs[: -len(pulled) - 1])
        started = copies([(held[i], b) for i, b in zip(pulled, buffers)], sems)
        for i, buffer in zip(pulled, buffers):
            held[i] = buffer
        for copy in started:
            copy.wait()
        body(*held)

    return wrapped


def unroll(steps):
    return steps if steps <= 8 else 1


def shape(dims, dtype=jnp.bfloat16):
    return jax.ShapeDtypeStruct(tuple(dims), dtype)


def mm(a, b, dims=(1, 0)):
    return lax.dot_general(
        a, b, (((dims[0],), (dims[1],)), ((), ())), preferred_element_type=jnp.float32
    )


def tile_of(tile_id, tiles_here):
    safe = jnp.maximum(tile_id, 0)
    owner = lax.div(safe, jnp.int32(tiles_here))
    return safe, owner, safe - owner * tiles_here


def side_of(owner, me, peers):
    half = lax.div(owner, jnp.int32(peers))
    mine = lax.div(me, jnp.int32(peers))
    return jnp.where(half == mine, 0, 1), owner - half * peers


def index_body(texts_here, ids_hbm, self_ref, text_hbm, out_ref, ids_ref, text_ref, sems):
    for copy in copies([(ids_hbm, ids_ref), (text_hbm, text_ref)], sems):
        copy.wait()
    tiles_here, entries = ids_ref.shape
    peers, _, lanes = out_ref.shape
    shards = 2 * peers
    width = lanes - 2 * LANES
    texts = texts_here * shards
    me = self_ref[0]
    row = lax.broadcasted_iota(jnp.int32, (peers, LANES), 0)
    near = jnp.full((peers, LANES), -1, jnp.int32)
    far = near
    for r in range(tiles_here):
        for k in range(entries):
            tile_id = ids_ref[r, k]
            _, owner, place = tile_of(tile_id, tiles_here)
            side, spot = side_of(owner, me, peers)
            wanted = (tile_id >= 0) & (owner != me)
            near = jnp.where(row == jnp.where(wanted & (side == 0), spot, -1), place, near)
            far = jnp.where(row == jnp.where(wanted & (side == 1), spot, -1), place, far)
    out_ref[:, :, width : width + LANES] = near.reshape(peers, 1, LANES)
    out_ref[:, :, width + LANES :] = far.reshape(peers, 1, LANES)
    tile_rows = text_ref.shape[1]
    lane = lax.broadcasted_iota(jnp.int32, (LANES, tile_rows), 1)
    sub = lax.broadcasted_iota(jnp.int32, (LANES, LANES), 0)
    diagonal = sub == lax.broadcasted_iota(jnp.int32, (LANES, LANES), 1)
    for c in range(width // LANES):
        slot = c * LANES + lax.broadcasted_iota(jnp.int32, (LANES, 1), 0)
        part = lax.div(slot, jnp.int32(shards))
        text = jnp.where(slot < texts, (slot - part * shards) * texts_here + part, -5)
        best = jnp.full((LANES, tile_rows), NO_NODE, jnp.int32)
        for j in range(tiles_here):
            node = (me * tiles_here + j) * tile_rows + lane
            best = jnp.where(text_ref[j : j + 1, :] == text, node, best)
        column = jnp.max(best.astype(jnp.float32), axis=1, keepdims=True)
        line = jnp.max(jnp.where(diagonal, column, float(NO_NODE)), axis=0, keepdims=True)
        out_ref[:, :, c * LANES : (c + 1) * LANES] = (
            jnp.broadcast_to(line, (peers, LANES)).astype(jnp.int32).reshape(peers, 1, LANES)
        )


def pack_near_body(asked_ref, cache_hbm, out_hbm, tile_ref, in_sems, out_sems):
    copy = pltpu.make_async_copy(cache_hbm, tile_ref, in_sems.at[0])
    copy.start()
    copy.wait()
    place_tiles(0, asked_ref, tile_ref, out_hbm, out_sems)


def pack_far_body(asked_ref, mate_ref, near_hbm, out_hbm, out_sems):
    place_tiles(1, asked_ref, mate_ref, out_hbm, out_sems)


def place_tiles(side, asked_ref, tile_ref, out_hbm, out_sems):
    tile_rows = tile_ref.shape[1]
    peers = out_hbm.shape[0]

    def slot(p):
        place = jnp.maximum(asked_ref[p, side], 0)
        target = out_hbm.at[p, pl.ds(side * tile_rows, tile_rows), :]
        return pltpu.make_async_copy(tile_ref.at[place], target, out_sems.at[p])

    lax.fori_loop(0, peers, lambda p, c: (slot(p).start(), c)[1], 0)
    lax.fori_loop(0, peers, lambda p, c: (slot(p).wait(), c)[1], 0)


def mask_body(
    ids_ref, self_ref, got_ref, mate_ref, adj_ref, cache_ref, *refs
):
    outs, (kept_ref, pick_ref, own_ref, base_ref, sems) = refs[:4], refs[4:]
    tiles_here, entries, tile_rows, _ = adj_ref.shape
    peers, _, lanes = got_ref.shape
    width = lanes - 2 * LANES
    me = self_ref[0]
    both = jnp.maximum(got_ref[:, :, :width], mate_ref[:, :, :width])
    table = jnp.max(both.reshape(peers, width).astype(jnp.float32), axis=0, keepdims=True)
    place = lax.broadcasted_iota(jnp.int32, (tile_rows, width), 0).astype(jnp.float32)
    ones = jnp.ones((ROWS, width), jnp.bfloat16)
    sent = []

    def holds(tile_id):
        first = (tile_id * tile_rows).astype(jnp.float32)
        return jnp.where(table - first == place, 1.0, 0.0)

    for r in range(tiles_here):

        def one(k, total):
            tile_id = ids_ref[r, k]
            hot = holds(tile_id).astype(jnp.bfloat16)
            values = adj_ref[r, k]
            taken = mm(ones, hot, (1, 1))[0:1, :]
            keep = jnp.where(tile_id >= 0, 1.0, 0.0) * jnp.where(taken > 0.5, 0.0, 1.0)
            kept_ref[r, k] = (values.astype(jnp.float32) * keep).astype(jnp.bfloat16)
            return total + mm(values, hot)

        pick = lax.fori_loop(
            0, entries, one, jnp.zeros((tile_rows, width), jnp.float32), unroll=unroll(entries)
        )
        pick_ref[r] = pick.astype(jnp.bfloat16)
        hot = holds(me * tiles_here + r)
        own_ref[r] = hot.astype(jnp.bfloat16)
        fresh = jnp.max(hot, axis=1, keepdims=True)
        base_ref[r] = (cache_ref[r].astype(jnp.float32) * (1.0 - fresh)).astype(jnp.bfloat16)
        row = [(ref.at[r], out.at[r]) for ref, out in zip((kept_ref, pick_ref, own_ref, base_ref), outs)]
        sent = sent + copies(row, sems.at[r])
    for copy in sent:
        copy.wait()


def norm(values, gain):
    average = jnp.mean(values, axis=-1, keepdims=True)
    centred = values - average
    variance = jnp.mean(centred * centred, axis=-1, keepdims=True)
    return centred * lax.rsqrt(variance + NORM_EPS) * gain


def attend_body(
    seq, counts_ref, tokens_hbm, w_qkv_hbm, w_out_hbm, out_hbm,
    tokens_ref, w_qkv_ref, w_out_ref, out_ref, proj_ref, ctx_ref, in_sems, out_sems
):
    half = w_out_ref.shape[0]
    texts_here = tokens_ref.shape[0] // seq
    started = copies(
        [(tokens_hbm, tokens_ref)]
        + [(w_qkv_hbm.at[c], w_qkv_ref.at[c]) for c in range(3)]
        + [(w_out_hbm, w_out_ref)],
        in_sems,
    )
    started[0].wait()
    for c in range(3):
        started[1 + c].wait()
        proj_ref[:, c * half : (c + 1) * half] = mm(tokens_ref[...], w_qkv_ref[c]).astype(
            jnp.bfloat16
        )
    started[4].wait()
    sent = []
    left = lax.broadcasted_iota(jnp.int32, (seq, LANES), 1) < HEAD
    key_at = lax.broadcasted_iota(jnp.int32, (seq, seq), 1)
    for t in range(texts_here):
        rows = pl.ds(t * seq, seq)
        live = key_at < counts_ref[0, t]
        for pair in range(half // LANES):
            first = pair * LANES
            query = proj_ref[rows, first : first + LANES].astype(jnp.float32) * (HEAD**-0.5)
            key = proj_ref[rows, half + first : half + first + LANES]
            value = proj_ref[rows, 2 * half + first : 2 * half + first + LANES]
            sides = []
            for side in (left, jnp.logical_not(left)):
                scores = mm(jnp.where(side, query, 0.0).astype(jnp.bfloat16), key, (1, 1))
                scores = jnp.where(live, scores, MASKED)
                powers = jnp.exp(scores - jnp.max(scores, axis=-1, keepdims=True))
                total = jnp.sum(powers, axis=-1, keepdims=True)
                sides.append(mm((powers / total).astype(jnp.bfloat16), value))
            ctx_ref[rows, first : first + LANES] = jnp.where(left, sides[0], sides[1]).astype(
                jnp.bfloat16
            )
        out_ref[rows, :] = mm(ctx_ref[rows, :], w_out_ref[...]).astype(jnp.bfloat16)
        sent.append(pltpu.make_async_copy(out_ref.at[rows, :], out_hbm.at[rows, :], out_sems.at[t]))
        sent[-1].start()
    for copy in sent:
        copy.wait()


def inner_body(
    tokens_ref, mine_hbm, other_ref, up_hbm, down_hbm, gains_ref, first_ref, out_ref,
    inner_ref, mine_ref, up_ref, down_ref, sems
):
    started = copies([(mine_hbm, mine_ref), (up_hbm, up_ref), (down_hbm, down_ref)], sems)
    started[0].wait()
    added = mine_ref[...].astype(jnp.float32) + other_ref[...].astype(jnp.float32)
    first = norm(tokens_ref[...].astype(jnp.float32) + added, gains_ref[0:1, :])
    first_ref[...] = first.astype(jnp.bfloat16)
    started[1].wait()
    hidden_units = up_ref.shape[1]
    step = hidden_units // 4
    for c in range(4):
        cols = slice(c * step, (c + 1) * step)
        value = mm(first_ref[...], up_ref[:, cols])
        gate = jnp.tanh(ROOT * (value + CUBE * (value * value * value)))
        inner_ref[:, cols] = (0.5 * value * (1.0 + gate)).astype(jnp.bfloat16)
    started[2].wait()
    out_ref[...] = mm(inner_ref[...], down_ref[...]).astype(jnp.bfloat16)


def pool_body(seq, counts_ref, first_ref, mine_ref, other_ref, gains_ref, out_ref):
    texts_here, width = first_ref.shape[0] // seq, first_ref.shape[1]
    for t in range(texts_here):
        rows = slice(t * seq, (t + 1) * seq)
        added = mine_ref[rows, :].astype(jnp.float32) + other_ref[rows, :].astype(jnp.float32)
        second = norm(first_ref[rows, :].astype(jnp.float32) + added, gains_ref[1:2, :])
        count = counts_ref[0, t]
        live = lax.broadcasted_iota(jnp.int32, (seq, 1), 0) < count
        total = jnp.sum(jnp.where(live, second, 0.0), axis=0, keepdims=True)
        pooled = (total / count.astype(jnp.float32)).astype(jnp.bfloat16).astype(jnp.float32)
        out_ref[:, :, t * width : (t + 1) * width] = pooled.reshape(1, 1, width)


def digits(shards):
    high, found = shards.bit_length() - 1, []
    while high > 0:
        low = max(high - 2, 0)
        found.append((low, high - low))
        high = low
    return found


def rising(shards):
    total = shards.bit_length() - 1
    return [(low, min(2, total - low)) for low in range(0, total, 2)]


def pooled_rows(me, pieces, width):
    shards = sum(piece.shape[0] for piece in pieces)
    parts = []
    for first in range(0, pieces[0].shape[2], width):
        for ref in pieces:
            part = ref[:, :, first : first + width].reshape(ref.shape[0], width)
            parts.append(part.astype(jnp.bfloat16))
    stacked = jnp.concatenate(parts, axis=0)
    texts = stacked.shape[0]
    row = lax.broadcasted_iota(jnp.int32, (texts, texts), 0)
    column = lax.broadcasted_iota(jnp.int32, (texts, texts), 1)
    place = column & (shards - 1)
    offset = jnp.zeros_like(place)
    for low, count in digits(shards):
        offset = offset + ((place & ((1 << count) - 1)) << low)
        place = lax.shift_right_logical(place, count)
    source = column - (column & (shards - 1)) + (offset ^ me)
    order = jnp.where(row == source, 1.0, 0.0).astype(jnp.bfloat16)
    return mm(order, stacked).astype(jnp.bfloat16)


def gather_body(
    row_from, ids_hbm, self_ref, kept_hbm, cache_hbm, remote_ref, out_ref,
    ids_ref, kept_ref, cache_ref, source_ref, sems
):
    rows, entries, tile_rows, _ = kept_ref.shape
    started = copies(
        [(ids_hbm, ids_ref), (cache_hbm, cache_ref), (kept_hbm.at[pl.ds(row_from, rows)], kept_ref)],
        sems,
    )
    tiles_here = cache_ref.shape[0]
    me = self_ref[0]
    started[0].wait()
    started[1].wait()

    def fetch(r, k):
        tile_id = ids_ref[row_from + r, k]
        _, owner, place = tile_of(tile_id, tiles_here)
        local = (owner == me) | (tile_id < 0)

        @pl.when(local)
        def _():
            source_ref[r, k] = cache_ref[place]

        @pl.when(jnp.logical_not(local))
        def _():
            side, spot = side_of(owner, me, remote_ref.shape[0])
            first = pl.multiple_of(side * tile_rows, tile_rows)
            source_ref[r, k] = remote_ref[spot, pl.ds(first, tile_rows), :]

    for r in range(rows):
        lax.fori_loop(
            0, entries, lambda k, c: (fetch(r, k), c)[1], 0, unroll=unroll(entries)
        )
        if r == 0:
            started[2].wait()
        total = jnp.zeros(out_ref.shape[1:], jnp.float32)
        for k in range(entries):
            total = total + mm(kept_ref[r, k], source_ref[r, k])
        out_ref[r] = total.astype(jnp.bfloat16)


def forward_body(
    self_ref, core_ref, top_ref, bottom_ref, far_top_ref, far_bottom_ref, w_own_ref, w_other_ref,
    grad_ref, own_ref, base_hbm, pick_ref, *refs
):
    (
        *pieces, node_hbm, slope_ref, agg_hbm, slope_hbm,
        rows_ref, node_ref, agg_ref, base_ref, node_sems, agg_sems, slope_sems, base_sems
    ) = refs
    based = copies([(base_hbm, base_ref)], base_sems)
    half = top_ref.shape[1]
    start = pl.multiple_of(core_ref[0] * half, LANES)
    far = pl.multiple_of((1 - core_ref[0]) * half, LANES)
    rows_ref[...] = pooled_rows(self_ref[0], pieces, rows_ref.shape[1])
    texts = rows_ref.shape[0]
    here = rows_ref[:, pl.ds(start, half)]
    w_own = w_own_ref[:, pl.ds(start, half)]
    w_other = w_other_ref[:, pl.ds(start, half)]
    moved = (mm(here, w_own) + mm(rows_ref[:, pl.ds(far, half)], w_other)).astype(jnp.bfloat16)
    blocks = node_sems.shape[0]
    step = grad_ref.shape[0] // blocks
    sent = []
    for block in range(blocks):
        at = pl.ds(block * step, step)
        mine_ref, other_ref = (
            (top_ref, far_top_ref) if 2 * block < blocks else (bottom_ref, far_bottom_ref)
        )
        within = pl.ds((2 * block % blocks) * step // 2, step)
        pick = pick_ref[at, :][:, :texts]
        hidden = (
            mm(mine_ref[within, :], w_own) + mm(other_ref[within, :], w_other) + mm(pick, moved)
        )
        square = hidden * hidden
        gate = jnp.tanh(ROOT * hidden * (1.0 + CUBE * square))
        lifted = 0.5 * (1.0 + gate)
        slope = lifted + 0.5 * hidden * (1.0 - gate * gate) * (ROOT * (1.0 + 3.0 * CUBE * square))
        slope_ref[at, :] = (grad_ref[at, :].astype(jnp.float32) * slope).astype(jnp.bfloat16)
        fresh = mm(own_ref[at, :][:, :texts], here)
        for copy in based:
            copy.wait()
        based = []
        node_ref[at, :] = (base_ref[at, :].astype(jnp.float32) + fresh + hidden * lifted).astype(
            jnp.bfloat16
        )
        agg_ref[at, :] = (mine_ref[within, :].astype(jnp.float32) + mm(pick, here)).astype(jnp.bfloat16)
        sent += copies([(node_ref.at[at, :], node_hbm.at[at, :])], node_sems.at[pl.ds(block, 1)])
        sent += copies([(agg_ref.at[at, :], agg_hbm.at[at, :])], agg_sems.at[pl.ds(block, 1)])
        sent += copies([(slope_ref.at[at, :], slope_hbm.at[at, :])], slope_sems.at[pl.ds(block, 1)])
    for copy in sent:
        copy.wait()


def chunk_body(
    per, texts_here, self_ref, core_ref, mine_ref, other_ref, agg_ref, down_ref, pick_ref, own_ref,
    grad_ref, *refs
):
    *part_refs, w_ref, text_ref, all_ref = refs
    shards, rows_each, half = all_ref.shape
    ways, kept = len(part_refs), shards // len(part_refs)
    deep = up_to(per, ROWS)
    text_rows = rows_each - deep
    me = self_ref[0]
    own = pl.multiple_of(core_ref[0] * half, LANES)
    far = pl.multiple_of((1 - core_ref[0]) * half, LANES)
    columns = 2 * half
    text_ref[...] = mm(pick_ref[...], down_ref[...], (0, 0)) + mm(
        own_ref[...], grad_ref[...], (0, 0)
    )
    w_ref[pl.ds(own, half), :] = mm(mine_ref[...], agg_ref[...], (0, 0))
    w_ref[pl.ds(far, half), :] = mm(other_ref[...], agg_ref[...], (0, 0))
    w_ref[columns:, :] = jnp.zeros((w_ref.shape[0] - columns, half), jnp.float32)
    row = lax.broadcasted_iota(jnp.int32, (text_rows, half), 0)
    for q in range(shards):
        piece = w_ref[q * per : q * per + deep, :].astype(jnp.bfloat16)
        block = jnp.zeros((text_rows, half), jnp.float32)
        for i in range(texts_here):
            line = text_ref[i * shards + q : i * shards + q + 1, :]
            high = line.astype(jnp.bfloat16).astype(jnp.float32)
            block = jnp.where(row == i, high, block)
            block = jnp.where(row == text_rows // 2 + i, line - high, block)
        step = q ^ me
        spot = (step & (ways - 1)) * kept + lax.shift_right_logical(step, ways.bit_length() - 1)
        all_ref[spot, :deep, :] = piece
        all_ref[spot, deep:, :] = block.astype(jnp.bfloat16)
    for c in range(ways):
        part_refs[c][...] = all_ref[c * kept : (c + 1) * kept]


def backward_body(
    ids_ref, self_ref, core_ref, mine_ref, other_ref, w_own_ref, adj_ref, send_hbm, down_hbm,
    down_ref, send_ref, sems, slot_sems
):
    tiles_here, entries, tile_rows, _ = adj_ref.shape
    shards, _, half = send_hbm.shape
    me = self_ref[0]
    core = core_ref[0]
    own = pl.multiple_of(core * half, LANES)
    far = pl.multiple_of((1 - core) * half, LANES)
    down = mm(mine_ref[...], w_own_ref[:, pl.ds(own, half)], (1, 1)) + mm(
        other_ref[...], w_own_ref[:, pl.ds(far, half)], (1, 1)
    )
    down_ref[...] = down.astype(jnp.bfloat16)
    down_copy = pltpu.make_async_copy(down_ref, down_hbm, sems.at[0])
    down_copy.start()
    for r in range(tiles_here):
        rows = slice(r * tile_rows, (r + 1) * tile_rows)
        for first in range(0, entries, 6):
            group = range(first, min(first + 6, entries))
            side_by_side = jnp.concatenate([adj_ref[r, k] for k in group], axis=1)
            product = mm(side_by_side, down_ref[rows, :], (0, 0)).astype(jnp.bfloat16)
            for k in group:
                tile_id = ids_ref[r, k]
                _, owner, _ = tile_of(tile_id, tiles_here)
                slot = jnp.where((tile_id >= 0) & (owner != me), owner, shards)
                send_ref[slot] = product[(k - first) * tile_rows : (k - first + 1) * tile_rows]
    for copy in copies([(send_ref.at[q], send_hbm.at[q]) for q in range(shards)], slot_sems):
        copy.wait()
    down_copy.wait()


def fold(refs, s, deep):
    total = sum(ref[s].astype(jnp.float32) for ref in refs)
    lines = (total.shape[0] - deep) // 2
    return total[:deep, :], total[deep : deep + lines, :] + total[deep + lines :, :]


def fold_body(deep, taken, *refs):
    in_refs, out_refs = refs[:taken], refs[taken:]
    ways = len(out_refs)
    for s in range(in_refs[0].shape[0]):
        w_sum, text = fold(in_refs, s, deep)
        high = text.astype(jnp.bfloat16).astype(jnp.float32)
        out_ref = out_refs[s % ways].at[s // ways]
        out_ref[:deep, :] = w_sum.astype(jnp.bfloat16)
        out_ref[deep:, :] = jnp.concatenate([high, text - high], axis=0).astype(jnp.bfloat16)


def close_body(deep, taken, *refs):
    w_ref, text_ref = refs[taken:]
    w_sum, text = fold(refs[:taken], 0, deep)
    w_ref[...] = w_sum
    text_ref[...] = text[: text_ref.shape[0], :]


def local_body(ids_ref, self_ref, down_ref, adj_ref, grad_ref, local_ref):
    tiles_here, entries, _, _ = adj_ref.shape
    me = self_ref[0]
    local_ref[...] = grad_ref[...].astype(jnp.float32)
    for r in range(tiles_here):

        def one(k, carry):
            tile_id = ids_ref[r, k]
            _, owner, place = tile_of(tile_id, tiles_here)

            @pl.when((tile_id >= 0) & (owner == me))
            def _():
                local_ref[place] += mm(adj_ref[r, k], down_ref[r], (0, 0))

            return carry

        lax.fori_loop(0, entries, one, 0, unroll=unroll(entries))


def finish_body(
    self_ref, asked_ref, mate_ref, local_hbm, got_ref, node_hbm, sum_ref, local_ref, node_ref, sems, out_sems
):
    tiles_here = sum_ref.shape[0]
    started = copies([(local_hbm.at[j], local_ref.at[j]) for j in range(tiles_here)], sems)
    shards = got_ref.shape[0]
    me = self_ref[0]
    sum_ref[...] = jnp.zeros_like(sum_ref)

    def one(q, carry):
        side, spot = side_of(q, me, shards // 2)
        asked = jnp.where(side == 0, asked_ref[spot, 0], mate_ref[spot, 1])

        @pl.when(asked >= 0)
        def _():
            sum_ref[asked] += got_ref[q].astype(jnp.float32)

        return carry

    lax.fori_loop(0, shards, one, 0)
    sent = []
    for j in range(tiles_here):
        started[j].wait()
        node_ref[j] = (sum_ref[j] + local_ref[j]).astype(jnp.bfloat16)
        sent += copies([(node_ref.at[j], node_hbm.at[j])], out_sems.at[pl.ds(j, 1)])
    for copy in sent:
        copy.wait()


def step(
    tokens, token_counts, w_qkv, w_out, w_up, w_down, ln_gains, cache, node_text, adj_tiles,
    adj_values, w_gnn, out_grad
):
    shards = lax.axis_size("graph")
    cores = lax.axis_size("mp")
    me = lax.axis_index("graph").astype(jnp.int32).reshape(1)
    core_at = lax.axis_index("mp")
    core = core_at.astype(jnp.int32).reshape(1)
    texts_here, seq, width = tokens.shape
    nodes_here, half = cache.shape
    tiles_here, entries, tile_rows = adj_values.shape[:3]
    texts = texts_here * shards
    slots = up_to(texts, LANES)
    per = width // shards
    deep = up_to(per, ROWS)
    count = texts_here * seq
    inner = w_up.shape[1]

    def swap(values):
        return lax.ppermute(values, "mp", [(i, cores - 1 - i) for i in range(cores)])

    def toward(values, reach):
        return lax.ppermute(values, "graph", [(i, i ^ reach) for i in range(shards)])

    peers = shards // 2

    def spread(values, groups=None):
        return lax.all_to_all(
            values, "graph", split_axis=0, concat_axis=0, tiled=True, axis_index_groups=groups
        )

    halves_of = [list(range(peers)), list(range(peers, shards))]

    cache_tiles = cache.reshape(tiles_here, tile_rows, half)
    mate_tiles = toward(cache_tiles, peers)
    index = call(
        functools.partial(index_body, texts_here),
        [shape((peers, 1, slots + 2 * LANES), jnp.int32)],
        [adj_tiles, me, node_text.reshape(tiles_here, tile_rows)],
        [HBM, SMEM, HBM],
        flops=1000,
        scratch=[
            pltpu.SMEM(adj_tiles.shape, jnp.int32),
            pltpu.VMEM((tiles_here, tile_rows), jnp.int32),
            pltpu.SemaphoreType.DMA((2,)),
        ],
    )
    got = spread(index, halves_of)
    mate_got = toward(got, peers)

    def places(table):
        return table[:, 0, slots:].reshape(peers, 2, LANES)[:, :, 0]

    asked = places(got)
    packed = call(
        pack_near_body,
        [shape((peers, 2 * tile_rows, half))],
        [asked, cache_tiles],
        [SMEM, HBM],
        flops=1000,
        scratch=[
            pltpu.VMEM(cache_tiles.shape, jnp.bfloat16),
            pltpu.SemaphoreType.DMA((1,)),
            pltpu.SemaphoreType.DMA((peers,)),
        ],
        out_specs=[HBM],
    )
    packed = call(
        pack_far_body,
        [shape((peers, 2 * tile_rows, half))],
        [asked, mate_tiles, packed],
        [SMEM, VMEM, HBM],
        flops=1000,
        scratch=[pltpu.SemaphoreType.DMA((peers,))],
        out_specs=[HBM],
        aliases={2: 0},
    )
    remote = spread(packed, halves_of)

    w_other = swap(w_gnn)

    flat_tokens = tokens.reshape(count, width)
    partial = call(
        functools.partial(attend_body, seq),
        [shape((count, width))],
        [token_counts, flat_tokens, jnp.transpose(w_qkv, (1, 0, 2)), w_out],
        [SMEM, HBM, HBM, HBM],
        flops=2 * count * (width * 3 * half + half * width + 2 * seq * half * 2),
        scratch=[
            pltpu.VMEM((count, width), jnp.bfloat16),
            pltpu.VMEM((3, width, half), jnp.bfloat16),
            pltpu.VMEM((half, width), jnp.bfloat16),
            pltpu.VMEM((count, width), jnp.bfloat16),
            pltpu.VMEM((count, 3 * half), jnp.bfloat16),
            pltpu.VMEM((count, half), jnp.bfloat16),
            pltpu.SemaphoreType.DMA((5,)),
            pltpu.SemaphoreType.DMA((texts_here,)),
        ],
        out_specs=[HBM],
    )
    first, mlp = call(
        inner_body,
        [shape((count, width)), shape((count, width))],
        [flat_tokens, partial, swap(partial), w_up, w_down, ln_gains],
        [VMEM, HBM, VMEM, HBM, HBM, VMEM],
        flops=4 * count * width * inner,
        scratch=[
            pltpu.VMEM((count, inner), jnp.bfloat16),
            pltpu.VMEM((count, width), jnp.bfloat16),
            pltpu.VMEM((width, inner), jnp.bfloat16),
            pltpu.VMEM((inner, width), jnp.bfloat16),
            pltpu.SemaphoreType.DMA((3,)),
        ],
    )
    pooled = call(
        functools.partial(pool_body, seq),
        [shape((1, 1, texts_here * width), jnp.float32)],
        [token_counts, first, mlp, swap(mlp), ln_gains],
        [SMEM, VMEM, VMEM, VMEM, VMEM],
        flops=20 * count * width,
    )
    pieces = [pooled]
    for low, bits in digits(shards):
        state = pieces[0] if len(pieces) == 1 else jnp.concatenate(pieces, axis=0)
        pieces = [state]
        for c in range(1, 1 << bits):
            pieces.append(toward(state, c << low))

    kept, pick, own, base = call(
        mask_body,
        [
            shape(adj_values.shape),
            shape((tiles_here, tile_rows, slots)),
            shape((tiles_here, tile_rows, slots)),
            shape(cache_tiles.shape),
        ],
        [adj_tiles, me, got, mate_got, adj_values, cache_tiles],
        [SMEM, SMEM, VMEM, VMEM, VMEM, VMEM],
        flops=2 * adj_values.size * slots,
        scratch=[
            pltpu.VMEM(adj_values.shape, jnp.bfloat16),
            pltpu.VMEM((tiles_here, tile_rows, slots), jnp.bfloat16),
            pltpu.VMEM((tiles_here, tile_rows, slots), jnp.bfloat16),
            pltpu.VMEM(cache_tiles.shape, jnp.bfloat16),
            pltpu.SemaphoreType.DMA((tiles_here, 4)),
        ],
        out_specs=[HBM] * 4,
    )
    rows = tiles_here // 2

    def gather(row_from):
        part = call(
            functools.partial(gather_body, row_from),
            [shape((rows, tile_rows, half))],
            [adj_tiles, me, kept, cache_tiles, remote],
            [HBM, SMEM, HBM, HBM, VMEM],
            flops=adj_values.size * half,
            scratch=[
                pltpu.SMEM(adj_tiles.shape, jnp.int32),
                pltpu.VMEM((rows,) + kept.shape[1:], jnp.bfloat16),
                pltpu.VMEM(cache_tiles.shape, jnp.bfloat16),
                pltpu.VMEM((rows, entries, tile_rows, half), jnp.bfloat16),
                pltpu.SemaphoreType.DMA((3,)),
            ],
        )
        return part.reshape(rows * tile_rows, half)

    top, bottom = gather(0), gather(rows)
    picked = pick.reshape(nodes_here, slots)
    node_out, slope, aggregate, slope_kept = call(
        forward_body,
        [shape((nodes_here, half))] * 4,
        [
            me, core, top, bottom, swap(top), swap(bottom), w_gnn, w_other,
            out_grad,
            own.reshape(nodes_here, slots), base.reshape(nodes_here, half), picked, *pieces,
        ],
        [SMEM, SMEM] + [HELD] * 4 + [VMEM] * 4 + [HBM] + [VMEM] * (1 + len(pieces)),
        flops=4 * nodes_here * half * half,
        scratch=[
            pltpu.VMEM((texts, width), jnp.bfloat16),
            pltpu.VMEM((nodes_here, half), jnp.bfloat16),
            pltpu.VMEM((nodes_here, half), jnp.bfloat16),
            pltpu.VMEM((nodes_here, half), jnp.bfloat16),
            pltpu.SemaphoreType.DMA((tiles_here,)),
            pltpu.SemaphoreType.DMA((tiles_here,)),
            pltpu.SemaphoreType.DMA((tiles_here,)),
            pltpu.SemaphoreType.DMA((1,)),
        ],
        out_specs=[HBM, VMEM, HBM, HBM],
    )
    grad_tiles = out_grad.reshape(tiles_here, tile_rows, half)
    slope_other = swap(slope)
    text_rows = up_to(2 * texts_here, 8)
    bits = [(low, count) for low, count in rising(shards)]
    ways = 1 << bits[0][1]
    portion = (shards // ways, deep + text_rows, half)
    send, down = call(
        backward_body,
        [shape((shards, tile_rows, half)), shape((nodes_here, half))],
        [adj_tiles, me, core, slope, slope_other, w_gnn, adj_values],
        [SMEM, SMEM, SMEM] + [VMEM] * 4,
        flops=4 * nodes_here * half * half + 2 * adj_values.size * half,
        scratch=[
            pltpu.VMEM((nodes_here, half), jnp.bfloat16),
            pltpu.VMEM((shards + 1, tile_rows, half), jnp.bfloat16),
            pltpu.SemaphoreType.DMA((1,)),
            pltpu.SemaphoreType.DMA((shards,)),
        ],
        out_specs=[HBM] * 2,
    )
    returned = spread(send)
    parts = call(
        functools.partial(chunk_body, per, texts_here),
        [shape(portion)] * ways,
        [
            me, core, slope_kept, slope_other, aggregate, down, picked,
            own.reshape(nodes_here, slots), out_grad,
        ],
        [SMEM, SMEM] + [PULL] * 7,
        flops=4 * nodes_here * half * (half + slots),
        scratch=[
            pltpu.VMEM((width + ROWS, half), jnp.float32),
            pltpu.VMEM((slots, half), jnp.float32),
            pltpu.VMEM((shards, deep + text_rows, half), jnp.bfloat16),
        ],
    )
    local = call(
        local_body,
        [shape((tiles_here, tile_rows, half), jnp.float32)],
        [adj_tiles, me, down.reshape(tiles_here, tile_rows, half), adj_values, grad_tiles],
        [SMEM, SMEM] + [VMEM] * 3,
        flops=2 * adj_values.size * half,
    )
    for turn, (low, _) in enumerate(bits):
        arrived = [parts[0]]
        for c in range(1, len(parts)):
            arrived.append(toward(parts[c], c << low))
        if turn + 1 < len(bits):
            ways = 1 << bits[turn + 1][1]
            portion = (portion[0] // ways,) + portion[1:]
            parts = call(
                functools.partial(fold_body, deep, len(arrived)),
                [shape(portion)] * ways,
                arrived,
                [VMEM] * len(arrived),
                flops=4 * math.prod(portion),
            )
    w_part, text_grad = call(
        functools.partial(close_body, deep, len(arrived)),
        [shape((deep, half), jnp.float32), shape((texts_here, half), jnp.float32)],
        arrived,
        [VMEM] * len(arrived),
        flops=1000,
    )
    node_grad = call(
        finish_body,
        [shape((tiles_here, tile_rows, half))],
        [me, asked, places(mate_got), local, returned],
        [SMEM, SMEM, SMEM, HBM, VMEM],
        flops=1000,
        scratch=[
            pltpu.VMEM((tiles_here, tile_rows, half), jnp.float32),
            pltpu.VMEM((tiles_here, tile_rows, half), jnp.float32),
            pltpu.VMEM((tiles_here, tile_rows, half), jnp.bfloat16),
            pltpu.SemaphoreType.DMA((tiles_here,)),
            pltpu.SemaphoreType.DMA((tiles_here,)),
        ],
        out_specs=[HBM],
    )
    return (node_out, w_part[:per].T, text_grad, node_grad.reshape(nodes_here, half))


def solution(mesh):
    placed = (
        P("graph", None, None),
        P("graph", None),
        P(None, None, "mp"),
        P("mp", None),
        P(None, "mp"),
        P("mp", None),
        P(),
        P("graph", "mp"),
        P("graph"),
        P("graph", None),
        P("graph", None, None, None),
        P("mp", None),
        P("graph", "mp"),
    )
    return jax.shard_map(
        step,
        mesh=mesh,
        in_specs=placed,
        out_specs=(P("graph", "mp"), P("mp", "graph"), P("graph", "mp"), P("graph", "mp")),
        check_vma=False,
    )
```
